8 devices in a mesh: dp: 1 (over z), my: 2 (over y), mx: 4 (over x, core).
Axes of the slice: x: 2, y: 2, z: 1, core: 2. Of those that a mesh axis runs over, the one named last changes fastest.
Arguments:
- tokens: bfloat16 [64, 256, 4096], P('dp', None, 'my')
- ln_scale: bfloat16 [4096], P('my')
- w_in: bfloat16 [4096, 28672], P('my', 'mx')
- mlp_bias: bfloat16 [16384], P('mx')
- q_scale: bfloat16 [256], replicated
- k_scale: bfloat16 [256], replicated
- w_out: bfloat16 [20480, 4096], P('mx', 'my')
- attn_out_bias: bfloat16 [4096], P('my')
- mlp_out_bias: bfloat16 [4096], P('my')
Outputs:
- output: bfloat16 [64, 256, 4096], P('dp', None, 'my')
All inputs are finite; a program needn't handle non-finite values.
Results may differ from the reference program's by a relative error of at most 0.011843.
Values are sent between devices in bfloat16 or wider.
A program may use at most 1 GiB of HBM per device.

```python
import jax
import jax.numpy as jnp
from jax import lax

BATCH = 64
SEQ = 256
D = 4096
HEADS = 16
HEAD = 256
FF = 16384
BLOCKS = 4

HEADS_BLK = HEADS // BLOCKS
FF_BLK = FF // BLOCKS
QKV_BLK = HEADS_BLK * HEAD
IN_BLK = 3 * QKV_BLK + FF_BLK


def block_columns(pieces):
    per_block = [one_piece.reshape(D, BLOCKS, one_piece.shape[1] // BLOCKS) for one_piece in pieces]
    return jnp.concatenate(per_block, axis=2).reshape(D, -1)


def block_rows(pieces):
    per_block = [one_piece.reshape(BLOCKS, one_piece.shape[0] // BLOCKS, D) for one_piece in pieces]
    return jnp.concatenate(per_block, axis=1).reshape(-1, D)


def setup_inputs(seed: int = 0, part: int = 0) -> dict:
    root_key = jax.random.key(seed)
    shared_keys = jax.random.split(root_key, 12)
    part_keys = jax.random.split(jax.random.fold_in(root_key, part), 4)
    width_grid = jnp.linspace(-1.0, 1.0, D)
    mean_amp = jax.random.uniform(part_keys[0], (), jnp.float32, minval=0.6, maxval=1.2)
    scale_amp = jax.random.uniform(part_keys[1], (), jnp.float32, minval=0.3, maxval=0.6)
    row_offset = 0.3 * jax.random.normal(part_keys[2], (BATCH, SEQ, 1), jnp.float32)
    base_noise = jax.random.normal(part_keys[3], (BATCH, SEQ, D), jnp.float32)
    tokens = base_noise * jnp.exp(scale_amp * width_grid) + mean_amp * width_grid + row_offset
    in_gain = D ** -0.5
    w_query = jax.random.normal(shared_keys[0], (D, HEADS * HEAD), jnp.float32) * in_gain
    w_key = jax.random.normal(shared_keys[1], (D, HEADS * HEAD), jnp.float32) * in_gain
    w_value = jax.random.normal(shared_keys[2], (D, HEADS * HEAD), jnp.float32) * in_gain
    w_up = jax.random.normal(shared_keys[3], (D, FF), jnp.float32) * in_gain
    w_attn_out = jax.random.normal(shared_keys[4], (HEADS * HEAD, D), jnp.float32) * (HEADS * HEAD) ** -0.5
    w_down = jax.random.normal(shared_keys[5], (FF, D), jnp.float32) * FF ** -0.5
    return {
        'tokens': tokens.astype(jnp.bfloat16),
        'ln_scale': jax.random.uniform(shared_keys[6], (D,), jnp.float32, minval=0.5, maxval=1.5).astype(jnp.bfloat16),
        'w_in': block_columns([w_query, w_key, w_value, w_up]).astype(jnp.bfloat16),
        'mlp_bias': (0.5 * jax.random.normal(shared_keys[7], (FF,), jnp.float32)).astype(jnp.bfloat16),
        'q_scale': jax.random.uniform(shared_keys[8], (HEAD,), jnp.float32, minval=1.2, maxval=2.0).astype(jnp.bfloat16),
        'k_scale': jax.random.uniform(shared_keys[9], (HEAD,), jnp.float32, minval=1.2, maxval=2.0).astype(jnp.bfloat16),
        'w_out': block_rows([w_attn_out, w_down]).astype(jnp.bfloat16),
        'attn_out_bias': (0.3 * jax.random.normal(shared_keys[10], (D,), jnp.float32)).astype(jnp.bfloat16),
        'mlp_out_bias': (0.3 * jax.random.normal(shared_keys[11], (D,), jnp.float32)).astype(jnp.bfloat16),
    }


def norm_last(features, gain_vec):
    centered = features - jnp.mean(features, axis=-1, keepdims=True)
    variance = jnp.mean(jnp.square(centered), axis=-1, keepdims=True)
    return centered * lax.rsqrt(variance + 1e-6) * gain_vec.astype(jnp.float32)


def reference(tokens, ln_scale, w_in, mlp_bias, q_scale, k_scale, w_out, attn_out_bias, mlp_out_bias):
    out_bias = attn_out_bias.astype(jnp.float32) + mlp_out_bias.astype(jnp.float32)
    unit_bias = mlp_bias.reshape(BLOCKS, FF_BLK).astype(jnp.float32)

    def one_image(image_row):
        tok_f32 = image_row.astype(jnp.float32)
        normed = norm_last(tok_f32, ln_scale).astype(jnp.bfloat16)
        projected = jnp.dot(normed, w_in, preferred_element_type=jnp.float32).astype(jnp.bfloat16)
        projected = projected.reshape(SEQ, BLOCKS, IN_BLK)
        head_shape = (SEQ, HEADS, HEAD)
        queries = norm_last(projected[:, :, :QKV_BLK].reshape(head_shape).astype(jnp.float32), q_scale).astype(jnp.bfloat16)
        keys_n = norm_last(projected[:, :, QKV_BLK:2 * QKV_BLK].reshape(head_shape).astype(jnp.float32), k_scale).astype(jnp.bfloat16)
        values = projected[:, :, 2 * QKV_BLK:3 * QKV_BLK].reshape(head_shape)
        logits = jnp.einsum('qhd,khd->hqk', queries.astype(jnp.float32), keys_n.astype(jnp.float32)) * HEAD ** -0.5
        attn_prob = jax.nn.softmax(logits, axis=-1).astype(jnp.bfloat16)
        mixed = jnp.einsum('hqk,khd->qhd', attn_prob.astype(jnp.float32), values.astype(jnp.float32)).astype(jnp.bfloat16)
        mlp_act = jax.nn.gelu(projected[:, :, 3 * QKV_BLK:].astype(jnp.float32) + unit_bias, approximate=False).astype(jnp.bfloat16)
        joined = jnp.concatenate([mixed.reshape(SEQ, BLOCKS, QKV_BLK), mlp_act], axis=2).reshape(SEQ, -1)
        out_f32 = jnp.dot(joined, w_out, preferred_element_type=jnp.float32)
        return (out_f32 + out_bias + tok_f32).astype(jnp.bfloat16)

    return lax.map(one_image, tokens)
```

```python
import functools

import jax
import jax.numpy as jnp
from jax import lax
from jax.experimental import pallas as pl
from jax.experimental.pallas import tpu as pltpu
from jax.sharding import PartitionSpec as P

MESH = pl.DeviceIdType.MESH
F32, BF16 = jnp.float32, jnp.bfloat16

SEQ, DH, WID = 256, 256, 2048
IMGS, GROUPS = 32, 8
M = IMGS // GROUPS * SEQ
HALF = M // 2
ROWS = IMGS * SEQ
TN = 512
QKV = 1024
UNITS = 4096
NJ = 7
NR = 5
NN = WID // TN
T1, T2 = 2 * NJ, 2 * NN
TT = T1 + T2
JB = NR * TN
EPS = 1e-6


def in_col(j, side):
    mlp = (j + 1) // 4
    at = (1 - mlp) * (QKV * j + (QKV // 2) * side) + mlp * (3 * QKV + (UNITS // 2) * side + TN * (j - 3))
    return pl.multiple_of(at, TN)


def out_row(r, side):
    mlp = (r + 3) // 4
    at = (1 - mlp) * (QKV // 2) * side + mlp * (QKV + (UNITS // 2) * side + TN * (r - 1))
    return pl.multiple_of(at, TN)


def tile(n):
    return pl.ds(pl.multiple_of(n * TN, TN), TN)


def rows_of(g):
    return pl.ds(pl.multiple_of(g * M, M), M)


def kernel(tok, lns, w_in, mb, qs, ks, w_out, ob,
           out, toth, wb, wc, wd, w2b, w2c, w2d, py, po, ry, s1, rx,
           z, joined, qk, vv, wbuf, ptile, sv, lbuf, sc, ub, gains,
           wsem, psem, vsem, lsem, csem,
           t_s, t_r, w_s, w_r, w2_s, w2_r, y_s, y_r, x_s, x_r, o_s, o_r, m_s, m_r):
    y = lax.axis_index("my")
    mi = lax.axis_index("mx")
    x, c = mi // 2, mi % 2
    dev_y = {"my": 1 - y, "mx": mi}
    dev_x = {"my": y, "mx": 2 * (1 - x) + c}
    dev_c = {"my": y, "mx": 2 * x + 1 - c}

    barrier = pltpu.get_barrier_semaphore()
    for dev in (dev_y, dev_x, dev_c):
        pl.semaphore_signal(barrier, inc=1, device_id=dev, device_id_type=MESH)
    pl.semaphore_wait(barrier, 3)

    def remote(src, dst, ss, rs, dev):
        return pltpu.make_async_remote_copy(src_ref=src, dst_ref=dst, send_sem=ss, recv_sem=rs, device_id=dev, device_id_type=MESH)

    def half_rows(g):
        return pl.ds(pl.multiple_of(g * M + x * HALF, HALF), HALF)

    def t_dir(g):
        src = tok.at[pl.ds(pl.multiple_of(c * ROWS + g * M + x * HALF, HALF), HALF)]
        return remote(src, toth.at[half_rows(g)], t_s.at[0, g], t_r.at[0, g], dev_y)

    def t_rel(g):
        return remote(toth.at[half_rows(g)], toth.at[half_rows(g)], t_s.at[1, g], t_r.at[1, g], dev_x)

    def w_c(j):
        return remote(w_in.at[:, pl.ds(in_col(j, 1 - y), TN)], wc.at[:, tile(j)], w_s.at[0, j], w_r.at[0, j], dev_y)

    def w_b(j):
        return remote(w_in.at[:, pl.ds(in_col(j, y), TN)], wb.at[:, tile(j)], w_s.at[1, j], w_r.at[1, j], dev_c)

    def w_d(j):
        return remote(wc.at[:, tile(j)], wd.at[:, tile(j)], w_s.at[2, j], w_r.at[2, j], dev_c)

    def w2_c(r):
        return remote(w_out.at[pl.ds(out_row(r, 1 - y), TN)], w2c.at[tile(r)], w2_s.at[0, r], w2_r.at[0, r], dev_y)

    def w2_b(r):
        return remote(w_out.at[pl.ds(out_row(r, y), TN)], w2b.at[tile(r)], w2_s.at[1, r], w2_r.at[1, r], dev_c)

    def w2_d(r):
        return remote(w2c.at[tile(r)], w2d.at[tile(r)], w2_s.at[2, r], w2_r.at[2, r], dev_c)

    def o_y(g, n):
        return remote(po.at[rows_of(g), tile(n)], ry.at[rows_of(g), tile(n)], y_s.at[g, n], y_r.at[g, n], dev_y)

    def o_x(g, n):
        return remote(s1.at[rows_of(g), tile(n)], rx.at[rows_of(g), tile(n)], x_s.at[g, n], x_r.at[g, n], dev_x)

    def out_rows(g):
        return pl.ds(pl.multiple_of(c * ROWS + g * M, M), M)

    def o_c(g, n):
        at = out.at[out_rows(g), tile(n)]
        return remote(at, at, o_s.at[g, n], o_r.at[g, n], dev_c)

    sc_y = remote(lns, sc.at[1], m_s.at[0], m_r.at[0], dev_y)
    my_units = pl.ds(pl.multiple_of(y * (UNITS // 2), UNITS // 2), UNITS // 2)
    ub_c = remote(mb.at[:, my_units], ub.at[1], m_s.at[1], m_r.at[1], dev_c)

    def loop(lo, hi, body):
        def run(i, carry):
            body(i)
            return carry
        lax.fori_loop(lo, hi, run, 0)

    sc_y.start()
    ub_c.start()
    t_dir(0).start()
    loop(0, NJ, lambda j: w_c(j).start())
    t_dir(1).start()
    loop(0, NR, lambda r: w2_c(r).start())
    t_dir(2).start()
    t_dir(3).start()
    loop(0, NJ, lambda j: w_b(j).start())
    loop(0, NR, lambda r: w2_b(r).start())
    small = [
        pltpu.make_async_copy(lns, sc.at[0], csem.at[0]),
        pltpu.make_async_copy(mb.at[:, my_units], ub.at[0], csem.at[1]),
        pltpu.make_async_copy(qs, gains.at[0], csem.at[2]),
        pltpu.make_async_copy(ks, gains.at[1], csem.at[3]),
    ]
    for one in small:
        one.start()
    t_dir(0).wait_recv()
    t_rel(0).start()
    for one in small:
        one.wait()
    sc_y.wait_recv()
    ub_c.wait_recv()

    def w_copies(t_slot, top, bottom, depth):
        return (
            pltpu.make_async_copy(top, wbuf.at[t_slot, pl.ds(0, depth)], wsem.at[t_slot, 0]),
            pltpu.make_async_copy(bottom, wbuf.at[t_slot, pl.ds(depth, depth)], wsem.at[t_slot, 1]),
        )

    def fetch(g, t):
        slot = t % 2
        j, side = t // 2, t % 2

        @pl.when((t < T1) & (side == 0))
        def _():
            @pl.when(g == 0)
            def _():
                w_c(j).wait_recv()
                w_d(j).start()
            for one in w_copies(slot, w_in.at[:, pl.ds(in_col(j, y), TN)], wc.at[:, tile(j)], WID):
                one.start()

        @pl.when((t < T1) & (side == 1))
        def _():
            @pl.when(g == 0)
            def _():
                w_b(j).wait_recv()
                w_d(j).wait_recv()
            for one in w_copies(slot, wb.at[:, tile(j)], wd.at[:, tile(j)], WID):
                one.start()

        @pl.when(t >= T1)
        def _():
            ue = (t - T1 + NN * ((7 - g) // 7)) % T2

            @pl.when(ue < NN)
            def _():
                @pl.when((g == 0) & (ue == 0))
                def _():
                    def relay(r):
                        w2_c(r).wait_recv()
                        w2_d(r).start()
                    loop(0, NR, relay)
                    loop(0, NR, lambda r: w2_d(r).wait_recv())
                for one in w_copies(slot, w2c.at[:, tile(ue)], w2d.at[:, tile(ue)], JB):
                    one.start()

            @pl.when(ue >= NN)
            def _():
                @pl.when((g == 0) & (ue == NN))
                def _():
                    loop(0, NR, lambda r: w2_b(r).wait_recv())
                cols = tile(ue - NN)
                top = w_out.at[pl.ds(out_row(0, y), TN), cols]
                rest = w_out.at[pl.ds(out_row(1, y), JB - TN), cols]
                pltpu.make_async_copy(top, wbuf.at[slot, pl.ds(0, TN)], wsem.at[slot, 2]).start()
                pltpu.make_async_copy(rest, wbuf.at[slot, pl.ds(TN, JB - TN)], wsem.at[slot, 0]).start()
                pltpu.make_async_copy(w2b.at[:, cols], wbuf.at[slot, pl.ds(JB, JB)], wsem.at[slot, 1]).start()

    def arrive1(slot):
        for one in w_copies(slot, wb.at[:, tile(0)], wd.at[:, tile(0)], WID):
            one.wait()

    def arrive2(g, t):
        slot = t % 2
        ue = (t - T1 + NN * ((7 - g) // 7)) % T2

        @pl.when(ue < NN)
        def _():
            for one in w_copies(slot, w2c.at[:, tile(0)], w2d.at[:, tile(0)], JB):
                one.wait()

        @pl.when(ue >= NN)
        def _():
            cols = tile(0)
            pltpu.make_async_copy(w2b.at[pl.ds(0, TN), cols], wbuf.at[slot, pl.ds(0, TN)], wsem.at[slot, 2]).wait()
            pltpu.make_async_copy(w2b.at[pl.ds(0, JB - TN), cols], wbuf.at[slot, pl.ds(TN, JB - TN)], wsem.at[slot, 0]).wait()
            pltpu.make_async_copy(w2b.at[:, cols], wbuf.at[slot, pl.ds(JB, JB)], wsem.at[slot, 1]).wait()

    def fetch_next(g, t):
        nt = t + 1
        ng = g + nt // TT

        @pl.when(ng < GROUPS)
        def _():
            fetch(ng, nt % TT)

    def load(k, src):
        return pltpu.make_async_copy(src, sv.at[k], vsem.at[k])

    def add_loads(g, n):
        return [load(0, py.at[rows_of(g), tile(n)]), load(1, ry.at[rows_of(g), tile(n)])]

    def add_store(g, n):
        return pltpu.make_async_copy(sv.at[3], s1.at[rows_of(g), tile(n)], vsem.at[3])

    def add_load(g, n):
        o_y(g, n).wait_recv()
        for one in add_loads(g, n):
            one.start()

    def add_do(g, n):
        for one in add_loads(g, n):
            one.wait()
        sv[3] = (sv[0].astype(F32) + sv[1].astype(F32)).astype(BF16)
        add_store(g, n).start()

    def add_send(g, n):
        add_store(g, n).wait()
        o_x(g, n).start()

    def fin_loads(g, n):
        return [load(0, s1.at[rows_of(g), tile(n)]), load(1, rx.at[rows_of(g), tile(n)]), load(2, tok.at[out_rows(g), tile(n)])]

    def fin_store(g, n):
        return pltpu.make_async_copy(sv.at[3], out.at[out_rows(g), tile(n)], vsem.at[3])

    def fin_load(g, n):
        o_x(g, n).wait_recv()
        for one in fin_loads(g, n):
            one.start()

    def fin_do(g, n):
        for one in fin_loads(g, n):
            one.wait()
        total = sv[0].astype(F32) + sv[1].astype(F32) + ob[:, tile(n)] + sv[2].astype(F32)
        sv[3] = total.astype(BF16)
        fin_store(g, n).start()

    def fin_send(g, n):
        fin_store(g, n).wait()
        o_c(g, n).start()

    def service(g, t):
        def chain(first, gg, load_, do_, send_):
            u = t - first

            @pl.when((u >= 2) & (u <= 2 * NN) & (u % 2 == 0))
            def _():
                send_(gg, u // 2 - 1)

            @pl.when((u >= 0) & (u < 2 * NN) & (u % 2 == 0))
            def _():
                load_(gg, u // 2)

            @pl.when((u >= 0) & (u < 2 * NN) & (u % 2 == 1))
            def _():
                do_(gg, u // 2)

        @pl.when(g >= 2)
        def _():
            chain(0, g - 2, add_load, add_do, add_send)

        @pl.when(g >= 3)
        def _():
            chain(9, g - 3, fin_load, fin_do, fin_send)

    def l_copies(g, i, slot):
        at = pl.multiple_of(g * M + i * SEQ, SEQ)
        return (
            pltpu.make_async_copy(tok.at[pl.ds(pl.multiple_of(c * ROWS + at, SEQ), SEQ)], lbuf.at[slot, 0], lsem.at[slot, 0]),
            pltpu.make_async_copy(toth.at[pl.ds(at, SEQ)], lbuf.at[slot, 1], lsem.at[slot, 1]),
        )

    def layer_norm(g):
        for one in l_copies(g, 0, 0):
            one.start()

        def image(i):
            slot = i % 2

            @pl.when(i + 1 < M // SEQ)
            def _():
                for one in l_copies(g, i + 1, 1 - slot):
                    one.start()
            for one in l_copies(g, i, slot):
                one.wait()
            step = 64

            def part(k):
                at = pl.ds(pl.multiple_of(k * step, step), step)
                a, b = lbuf[slot, 0, at].astype(F32), lbuf[slot, 1, at].astype(F32)
                mean = (jnp.sum(a, -1, keepdims=True) + jnp.sum(b, -1, keepdims=True)) * (0.5 / WID)
                a, b = a - mean, b - mean
                var = (jnp.sum(a * a, -1, keepdims=True) + jnp.sum(b * b, -1, keepdims=True)) * (0.5 / WID)
                inv = lax.rsqrt(var + EPS)
                to = pl.ds(pl.multiple_of(i * SEQ + k * step, step), step)
                z[to, :WID] = (a * inv * sc[0]).astype(BF16)
                z[to, WID:] = (b * inv * sc[1]).astype(BF16)
            loop(0, SEQ // step, part)
        loop(0, M // SEQ, image)

    def project(slot):
        return (jnp.dot(z[:, :WID], wbuf[slot, :WID], preferred_element_type=F32)
                + jnp.dot(z[:, WID:], wbuf[slot, WID:2 * WID], preferred_element_type=F32)).astype(BF16)

    def around(g, t, compute):
        @pl.when(g > 0)
        def _():
            fetch_next(g, t)
        compute()

        @pl.when(g == 0)
        def _():
            fetch_next(g, t)
        service(g, t)

    def group(g):
        @pl.when((g >= 1) & (g + 3 < GROUPS))
        def _():
            t_dir(g + 3).start()

        t_rel(g).wait_recv()
        layer_norm(g)

        def qk_tile(t):
            def compute():
                arrive1(t % 2)
                h = project(t % 2).astype(F32)
                gain = gains[t // 2]
                for k in range(2):
                    part = h[:, k * DH:(k + 1) * DH]
                    part = part - jnp.mean(part, -1, keepdims=True)
                    var = jnp.mean(part * part, -1, keepdims=True)
                    qk[t // 2, t % 2, :, k * DH:(k + 1) * DH] = (part * lax.rsqrt(var + EPS) * gain).astype(BF16)
            around(g, t, compute)
        loop(0, 4, qk_tile)

        def v_tile(t):
            def compute():
                arrive1(t % 2)
                vv[t % 2] = project(t % 2)
            around(g, t, compute)
        loop(4, 6, v_tile)

        def mlp_tile(t):
            def compute():
                arrive1(t % 2)
                u = t // 2 - 3
                h = project(t % 2).astype(F32) + ub[t % 2, :, tile(u)]
                act = 0.5 * h * (1.0 + lax.erf(h * 0.7071067811865476))
                joined[:, pl.ds(pl.multiple_of((t % 2) * JB + TN + u * TN, TN), TN)] = act.astype(BF16)
            around(g, t, compute)
        loop(6, T1, mlp_tile)

        @pl.when(g == 0)
        def _():
            t_dir(1).wait_recv()
            t_rel(1).start()

        def attend(i):
            at = pl.ds(pl.multiple_of(i * SEQ, SEQ), SEQ)
            for side in range(2):
                for k in range(2):
                    cols = slice(k * DH, (k + 1) * DH)
                    q, kk, v = qk[0, side, at, cols], qk[1, side, at, cols], vv[side, at, cols]
                    lg = lax.dot_general(q, kk, (((1,), (1,)), ((), ())), preferred_element_type=F32) * (DH ** -0.5)
                    e = jnp.exp(lg - jnp.max(lg, -1, keepdims=True))
                    p = (e / jnp.sum(e, -1, keepdims=True)).astype(BF16)
                    mixed = jnp.dot(p, v, preferred_element_type=F32).astype(BF16)
                    joined[at, side * JB + k * DH:side * JB + (k + 1) * DH] = mixed
        loop(0, M // SEQ, attend)

        def p_store(u):
            ue = (u + NN * ((7 - g) // 7)) % T2
            slot = u % 2

            def to(ref, n):
                return pltpu.make_async_copy(ptile.at[slot], ref.at[rows_of(g), tile(n)], psem.at[slot])
            return ue, to

        def p_start(u):
            ue, to = p_store(u)

            @pl.when(ue < NN)
            def _():
                to(po, ue).start()

            @pl.when(ue >= NN)
            def _():
                to(py, ue - NN).start()

        def p_finish(u):
            ue, to = p_store(u)

            @pl.when(ue < NN)
            def _():
                to(po, ue).wait()
                o_y(g, ue).start()

            @pl.when(ue >= NN)
            def _():
                to(py, ue - NN).wait()

        def out_tile(u):
            t = T1 + u

            def compute():
                arrive2(g, t)
                slot = t % 2
                part = (jnp.dot(joined[:, :JB], wbuf[slot, :JB], preferred_element_type=F32)
                        + jnp.dot(joined[:, JB:], wbuf[slot, JB:], preferred_element_type=F32))
                ptile[u % 2] = part.astype(BF16)
                p_start(u)

                @pl.when(u >= 1)
                def _():
                    p_finish(u - 1)
            around(g, t, compute)
        loop(0, T2, out_tile)
        p_finish(T2 - 1)

        @pl.when(g + 2 < GROUPS)
        def _():
            t_dir(g + 2).wait_recv()
            t_rel(g + 2).start()

    fetch(0, 0)
    loop(0, GROUPS, group)

    def whole(gg, load_, do_, send_):
        def one(n):
            load_(gg, n)
            do_(gg, n)
            send_(gg, n)
        loop(0, NN, one)

    whole(GROUPS - 2, add_load, add_do, add_send)
    whole(GROUPS - 3, fin_load, fin_do, fin_send)
    whole(GROUPS - 1, add_load, add_do, add_send)
    whole(GROUPS - 2, fin_load, fin_do, fin_send)
    whole(GROUPS - 1, fin_load, fin_do, fin_send)

    sc_y.wait_send()
    ub_c.wait_send()
    for one in (w_c, w_b, w_d):
        loop(0, NJ, lambda j, one=one: one(j).wait_send())
    for one in (w2_c, w2_b, w2_d):
        loop(0, NR, lambda r, one=one: one(r).wait_send())

    def settle(g):
        t_dir(g).wait_send()
        t_rel(g).wait_send()

        def chunk(n):
            o_y(g, n).wait_send()
            o_x(g, n).wait_send()
            o_c(g, n).wait_send()
            o_c(g, n).wait_recv()
        loop(0, NN, chunk)
    loop(0, GROUPS, settle)


def solution(mesh):
    hbm = pl.BlockSpec(memory_space=pltpu.HBM)
    vmem = pl.BlockSpec(memory_space=pltpu.VMEM)
    dma = pltpu.SemaphoreType.DMA

    def local_layer(tokens, ln_scale, w_in, mlp_bias, q_scale, k_scale, w_out, attn_out_bias, mlp_out_bias):
        images = tokens.shape[0]
        tok = tokens.reshape(images * SEQ, WID)
        row = lambda v: v.astype(F32).reshape(1, -1)
        act = jax.ShapeDtypeStruct((ROWS, WID), BF16)
        in_half = jax.ShapeDtypeStruct((WID, NJ * TN), BF16)
        out_half = jax.ShapeDtypeStruct((JB, WID), BF16)
        shapes = [jax.ShapeDtypeStruct(tok.shape, BF16), act] + [in_half] * 3 + [out_half] * 3 + [act] * 5
        flops = 2 * ROWS * (2 * WID * T1 * TN + 2 * JB * 2 * WID)
        res = pl.pallas_call(
            kernel,
            out_shape=shapes,
            in_specs=[hbm, hbm, hbm, hbm, hbm, hbm, hbm, vmem],
            out_specs=[hbm] * len(shapes),
            scratch_shapes=[
                pltpu.VMEM((M, 2 * WID), BF16),
                pltpu.VMEM((M, 2 * JB), BF16),
                pltpu.VMEM((2, 2, M, TN), BF16),
                pltpu.VMEM((2, M, TN), BF16),
                pltpu.VMEM((2, 2 * JB, TN), BF16),
                pltpu.VMEM((2, M, TN), BF16),
                pltpu.VMEM((4, M, TN), BF16),
                pltpu.VMEM((2, 2, SEQ, WID), BF16),
                pltpu.VMEM((2, 1, WID), F32),
                pltpu.VMEM((2, 1, UNITS // 2), F32),
                pltpu.VMEM((2, 1, DH), F32),
                dma((2, 3)), dma((2,)), dma((4,)), dma((2, 2)), dma((4,)),
                dma((2, GROUPS)), dma((2, GROUPS)), dma((3, NJ)), dma((3, NJ)), dma((3, NR)), dma((3, NR)),
                dma((GROUPS, NN)), dma((GROUPS, NN)), dma((GROUPS, NN)), dma((GROUPS, NN)), dma((GROUPS, NN)), dma((GROUPS, NN)),
                dma((2,)), dma((2,)),
            ],
            compiler_params=pltpu.CompilerParams(collective_id=0, has_side_effects=True, vmem_limit_bytes=63 * 2**20),
            cost_estimate=pl.CostEstimate(flops=flops, bytes_accessed=2**30, transcendentals=0),
            name="layer",
        )(tok, row(ln_scale), w_in, row(mlp_bias), row(q_scale), row(k_scale), w_out, row(attn_out_bias) + row(mlp_out_bias))
        return res[0].reshape(tokens.shape)

    specs_in = (P('dp', None, 'my'), P('my'), P('my', 'mx'), P('mx'), P(), P(), P('mx', 'my'), P('my'), P('my'))
    return jax.shard_map(local_layer, mesh=mesh, in_specs=specs_in, out_specs=P('dp', None, 'my'), check_vma=False)
```

```python
import jax
import jax.numpy as jnp
from jax import lax
from jax.experimental import pallas as pl
from jax.experimental.pallas import tpu as pltpu
from jax.sharding import PartitionSpec as P

MESH = pl.DeviceIdType.MESH
F32, BF16 = jnp.float32, jnp.bfloat16

SEQ, DH, WID = 256, 256, 2048
M, GROUPS = 1024, 4
ROWS = M * GROUPS
HALF = M // 2
TN = 512
QKV, UNITS = 1024, 4096
NS = 4
NJ = 7
NT = NS * NJ
NN = WID // TN
JB = 5 * TN
KH = 2 * JB
LN = 128
EPS = 1e-6


def in_col(j, side):
    mlp = (j + 1) // 4
    at = (1 - mlp) * (QKV * j + (QKV // 2) * side) + mlp * (3 * QKV + (UNITS // 2) * side + TN * (j - 3))
    return pl.ds(pl.multiple_of(at, TN), TN)


def out_row(part, side):
    if part == 0:
        return pl.ds(pl.multiple_of((QKV // 2) * side, QKV // 2), TN)
    return pl.ds(pl.multiple_of(QKV + (UNITS // 2) * side, QKV), UNITS // 2)


PART_ROWS = (pl.ds(0, TN), pl.ds(TN, JB - TN))


def tile(n):
    return pl.ds(pl.multiple_of(n * TN, TN), TN)


def rows_of(g):
    return pl.ds(pl.multiple_of(g * M, M), M)


def tile_of(t):
    a, b = (t + 24) // 28, t // 24
    j = (1 - a) * (t // 2) + (a - b) * (t // 4 + 1 - 2 * ((t % 4) // 2)) + b * (t // 2 - 7)
    s = (1 - a) * (t % 2) + (a - b) * (t % 4) + b * (2 + t % 2)
    return j, s


def loop(lo, hi, body):
    def run(i, carry):
        body(i)
        return carry
    lax.fori_loop(lo, hi, run, 0)


def start_all(copies):
    for one in copies:
        one.start()


def wait_all(copies):
    for one in copies:
        one.wait()


def kernel(tok, lns, w_in, mb, qs, ks, w_out, ob,
           out, toth, w1t, w1b, w2y, w2n, qkv, jb, pa, pb, ry,
           zj, wbuf, ptile, acc, abuf, sv, lbuf, sc, ub, gains,
           w1sem, w2sem, jsem, psem, asem, vsem, lsem, csem,
           t_s, t_r, w_s, w_r, e_s, e_r, d_s, d_r, y_s, y_r, x_s, x_r, o_s, o_r, m_s, m_r):
    y = lax.axis_index("my")
    mi = lax.axis_index("mx")
    x, c = mi // 2, mi % 2
    dev_y = {"my": 1 - y, "mx": mi}
    dev_x = {"my": y, "mx": 2 * (1 - x) + c}
    dev_c = {"my": y, "mx": 2 * x + 1 - c}
    dev_d = {"my": y, "mx": 2 * (1 - x) + 1 - c}
    row0 = (2 * x + c) * ROWS
    row0_x = (2 * (1 - x) + c) * ROWS

    barrier = pltpu.get_barrier_semaphore()
    for dev in (dev_y, dev_x, dev_c, dev_d):
        pl.semaphore_signal(barrier, inc=1, device_id=dev, device_id_type=MESH)
    pl.semaphore_wait(barrier, 4)

    def remote(src, dst, ss, rs, dev):
        return pltpu.make_async_remote_copy(src_ref=src, dst_ref=dst, send_sem=ss, recv_sem=rs, device_id=dev, device_id_type=MESH)

    def t_dir(k):
        src = tok.at[pl.ds(pl.multiple_of(row0 + k * HALF, HALF), HALF)]
        return remote(src, toth.at[pl.ds(pl.multiple_of(k * HALF, HALF), HALF)], t_s.at[k], t_r.at[k], dev_y)

    def w_c(j):
        return remote(w_in.at[:, in_col(j, 1 - y)], w1b.at[0, :, tile(j)], w_s.at[0, j], w_r.at[0, j], dev_y)

    def w_b(j):
        return remote(w_in.at[:, in_col(j, y)], w1t.at[0, :, tile(j)], w_s.at[1, j], w_r.at[1, j], dev_c)

    def w_d(j):
        return remote(w1b.at[0, :, tile(j)], w1b.at[1, :, tile(j)], w_s.at[2, j], w_r.at[2, j], dev_c)

    def w_e(j):
        return remote(w_in.at[:, in_col(j, y)], w1t.at[1, :, tile(j)], w_s.at[3, j], w_r.at[3, j], dev_x)

    def w_f(j):
        return remote(w1b.at[0, :, tile(j)], w1b.at[2, :, tile(j)], w_s.at[4, j], w_r.at[4, j], dev_x)

    def w_g(j):
        return remote(w1t.at[1, :, tile(j)], w1t.at[2, :, tile(j)], w_s.at[5, j], w_r.at[5, j], dev_c)

    def w_h(j):
        return remote(w1b.at[2, :, tile(j)], w1b.at[3, :, tile(j)], w_s.at[6, j], w_r.at[6, j], dev_c)

    class Two:
        def __init__(self, copies):
            self.copies = copies

        def start(self):
            start_all(self.copies)

        def wait_send(self):
            for one in self.copies:
                one.wait_send()

        def wait_recv(self):
            for one in self.copies:
                one.wait_recv()

    def v_c(n):
        return Two([remote(w_out.at[out_row(p, 1 - y), tile(n)], w2n.at[0, PART_ROWS[p], tile(n)],
                           e_s.at[0, n, p], e_r.at[0, n, p], dev_y) for p in range(2)])

    def v_b(n):
        return Two([remote(w_out.at[out_row(p, y), tile(n)], w2y.at[0, PART_ROWS[p], tile(n)],
                           e_s.at[1, n, p], e_r.at[1, n, p], dev_c) for p in range(2)])

    def v_e(n):
        return Two([remote(w_out.at[out_row(p, y), tile(n)], w2y.at[1, PART_ROWS[p], tile(n)],
                           e_s.at[2, n, p], e_r.at[2, n, p], dev_x) for p in range(2)])

    def v_d(n):
        return remote(w2n.at[0, :, tile(n)], w2n.at[1, :, tile(n)], d_s.at[0, n], d_r.at[0, n], dev_c)

    def v_f(n):
        return remote(w2n.at[0, :, tile(n)], w2n.at[2, :, tile(n)], d_s.at[1, n], d_r.at[1, n], dev_x)

    def v_g(n):
        return remote(w2y.at[1, :, tile(n)], w2y.at[2, :, tile(n)], d_s.at[2, n], d_r.at[2, n], dev_c)

    def v_h(n):
        return remote(w2n.at[2, :, tile(n)], w2n.at[3, :, tile(n)], d_s.at[3, n], d_r.at[3, n], dev_c)

    def o_y(g, n):
        return remote(pb.at[rows_of(g), tile(n)], ry.at[rows_of(g), tile(n)], y_s.at[g, n], y_r.at[g, n], dev_y)

    def part_rows(k):
        return pl.ds(pl.multiple_of(k * HALF, HALF), HALF)

    def own_out(k):
        return pl.ds(pl.multiple_of(row0 + k * HALF, HALF), HALF)

    def o_x(k, n):
        at = out.at[own_out(k), tile(n)]
        return remote(at, at, x_s.at[k, n], x_r.at[k, n], dev_x)

    def o_c(k, n):
        at = out.at[own_out(k), tile(n)]
        return remote(at, at, o_s.at[0, k, n], o_r.at[0, k, n], dev_c)

    def o_f(k, n):
        at = out.at[pl.ds(pl.multiple_of(row0_x + k * HALF, HALF), HALF), tile(n)]
        return remote(at, at, o_s.at[1, k, n], o_r.at[1, k, n], dev_c)

    my_units = pl.ds(pl.multiple_of(y * (UNITS // 2), UNITS // 2), UNITS // 2)
    small_far = [
        remote(lns, sc.at[1], m_s.at[0], m_r.at[0], dev_y),
        remote(mb.at[:, my_units], ub.at[1], m_s.at[1], m_r.at[1], dev_c),
        remote(mb.at[:, my_units], ub.at[2], m_s.at[2], m_r.at[2], dev_x),
        remote(mb.at[:, my_units], ub.at[3], m_s.at[3], m_r.at[3], dev_d),
    ]
    small = [
        pltpu.make_async_copy(lns, sc.at[0], csem.at[0]),
        pltpu.make_async_copy(mb.at[:, my_units], ub.at[0], csem.at[1]),
        pltpu.make_async_copy(qs, gains.at[0], csem.at[2]),
        pltpu.make_async_copy(ks, gains.at[1], csem.at[3]),
    ]

    start_all(small_far)
    loop(0, 4, lambda k: t_dir(k).start())
    loop(0, NJ, lambda j: w_c(j).start())
    loop(4, 8, lambda k: t_dir(k).start())
    loop(0, NN, lambda n: v_c(n).start())
    loop(0, 5, lambda j: w_e(j).start())
    loop(0, NJ, lambda j: w_b(j).start())
    loop(0, NN, lambda n: v_b(n).start())
    start_all(small)
    wait_all(small)
    for one in small_far:
        one.wait_recv()

    def l_copies(g, i, slot):
        at = pl.multiple_of(g * M + i * LN, LN)
        return (
            pltpu.make_async_copy(tok.at[pl.ds(pl.multiple_of(row0 + at, LN), LN)], lbuf.at[slot, 0], lsem.at[slot, 0]),
            pltpu.make_async_copy(toth.at[pl.ds(at, LN)], lbuf.at[slot, 1], lsem.at[slot, 1]),
        )

    def layer_norm(g):
        steps = M // LN
        t_dir(2 * g).wait_recv()
        start_all(l_copies(g, 0, 0))

        def rows(i):
            slot = i % 2

            @pl.when(i == steps // 2 - 1)
            def _():
                t_dir(2 * g + 1).wait_recv()

            @pl.when(i + 1 < steps)
            def _():
                start_all(l_copies(g, i + 1, 1 - slot))
            wait_all(l_copies(g, i, slot))
            step = 64

            def part(k):
                at = pl.ds(pl.multiple_of(k * step, step), step)
                a, b = lbuf[slot, 0, at].astype(F32), lbuf[slot, 1, at].astype(F32)
                mean = (jnp.sum(a, -1, keepdims=True) + jnp.sum(b, -1, keepdims=True)) * (0.5 / WID)
                a, b = a - mean, b - mean
                var = (jnp.sum(a * a, -1, keepdims=True) + jnp.sum(b * b, -1, keepdims=True)) * (0.5 / WID)
                inv = lax.rsqrt(var + EPS)
                to = pl.ds(pl.multiple_of(i * LN + k * step, step), step)
                zj[g % 2, to, :WID] = (a * inv * sc[0]).astype(BF16)
                zj[g % 2, to, WID:2 * WID] = (b * inv * sc[1]).astype(BF16)
            loop(0, LN // step, part)
        loop(0, steps, rows)

    def w1_copies(slot, top, bottom):
        return (
            pltpu.make_async_copy(top, wbuf.at[slot, :WID], w1sem.at[slot, 0]),
            pltpu.make_async_copy(bottom, wbuf.at[slot, WID:2 * WID], w1sem.at[slot, 1]),
        )

    def fetch1(p, t):
        j, s = tile_of(t)
        slot = t % 2

        @pl.when(p == 0)
        def _():
            @pl.when(s == 0)
            def _():
                w_c(j).wait_recv()
                w_d(j).start()
                w_f(j).start()

                @pl.when((j == 1) | (j == 3))
                def _():
                    w_e((j + 9) // 2).start()

                @pl.when(j == NJ - 1)
                def _():
                    v_e(0).start()
                    v_e(1).start()

            @pl.when(s == 1)
            def _():
                w_b(j).wait_recv()
                w_d(j).wait_recv()

            @pl.when(s == 2)
            def _():
                w_e(j).wait_recv()
                w_g(j).start()
                w_f(j).wait_recv()
                w_h(j).start()

            @pl.when(s == 3)
            def _():
                w_g(j).wait_recv()
                w_h(j).wait_recv()

        @pl.when(s == 0)
        def _():
            start_all(w1_copies(slot, w_in.at[:, in_col(j, y)], w1b.at[0, :, tile(j)]))

        @pl.when(s > 0)
        def _():
            start_all(w1_copies(slot, w1t.at[s - 1, :, tile(j)], w1b.at[s, :, tile(j)]))

    def h_store(slot, dst):
        return pltpu.make_async_copy(ptile.at[slot], dst, psem.at[slot])

    def h_done(slot):
        h_store(slot, pb.at[rows_of(0), tile(0)]).wait()

    def w1_tile(p, t):
        j, s = tile_of(t)
        wait_all(w1_copies(t % 2, w1t.at[0, :, tile(0)], w1b.at[0, :, tile(0)]))

        def one(gl):
            g = 2 * p + gl

            def project():
                h = (jnp.dot(zj[gl, :, :WID], wbuf[t % 2, :WID], preferred_element_type=F32)
                     + jnp.dot(zj[gl, :, WID:2 * WID], wbuf[t % 2, WID:2 * WID], preferred_element_type=F32))
                return h.astype(BF16)

            @pl.when((t > 0) & (t != 24))
            def _():
                h_done(gl)

            @pl.when(j < 2)
            def _():
                h = project().astype(F32)
                gain = gains[j]
                for k in range(2):
                    part = h[:, k * DH:(k + 1) * DH]
                    part = part - jnp.mean(part, -1, keepdims=True)
                    var = jnp.mean(part * part, -1, keepdims=True)
                    ptile[gl, :, k * DH:(k + 1) * DH] = (part * lax.rsqrt(var + EPS) * gain).astype(BF16)

            @pl.when(j == 2)
            def _():
                ptile[gl] = project()

            @pl.when(j > 2)
            def _():
                h = project().astype(F32) + ub[s, :, tile(j - 3)]
                ptile[gl] = (0.5 * h * (1.0 + lax.erf(h * 0.7071067811865476))).astype(BF16)

            @pl.when(j <= 2)
            def _():
                h_store(gl, qkv.at[j, s, rows_of(g)]).start()

            @pl.when(j > 2)
            def _():
                h_store(gl, jb.at[rows_of(g), pl.ds(pl.multiple_of(s * JB + (j - 2) * TN, TN), TN)]).start()
        loop(0, 2, one)

    def a_loads(p, w, slot):
        g, s = 2 * p + w // NS, w % NS
        return [pltpu.make_async_copy(qkv.at[i, s, rows_of(g)], abuf.at[slot, i], asem.at[slot, i]) for i in range(3)]

    def a_store(p, w, slot):
        g, s = 2 * p + w // NS, w % NS
        return h_store(slot, jb.at[rows_of(g), pl.ds(pl.multiple_of(s * JB, TN), TN)])

    def attention(p):
        units = 2 * NS
        start_all(a_loads(p, 0, 0))

        def unit(w):
            slot = w % 2

            @pl.when(w + 1 < units)
            def _():
                start_all(a_loads(p, w + 1, 1 - slot))
            wait_all(a_loads(p, w, slot))

            @pl.when(w >= 2)
            def _():
                a_store(p, w - 2, slot).wait()

            def images(i):
                for ii in range(2):
                    at = pl.ds(pl.multiple_of((2 * i + ii) * SEQ, SEQ), SEQ)
                    for k in range(2):
                        cols = slice(k * DH, (k + 1) * DH)
                        q, kk, v = abuf[slot, 0, at, cols], abuf[slot, 1, at, cols], abuf[slot, 2, at, cols]
                        lg = lax.dot_general(q, kk, (((1,), (1,)), ((), ())), preferred_element_type=F32) * (DH ** -0.5)
                        e = jnp.exp(lg - jnp.max(lg, -1, keepdims=True))
                        prob = (e / jnp.sum(e, -1, keepdims=True)).astype(BF16)
                        ptile[slot, at, cols] = jnp.dot(prob, v, preferred_element_type=F32).astype(BF16)
            loop(0, M // SEQ // 2, images)
            a_store(p, w, slot).start()
        loop(0, units, unit)
        a_store(p, units - 2, 0).wait()
        a_store(p, units - 1, 1).wait()

    def w2_slot(m, half):
        return 2 * ((m + 1) % 2) + half

    def w2_dst(m, s):
        return wbuf.at[w2_slot(m, s // 2), pl.ds((s % 2) * JB, JB)]

    def fetch2(m):
        n = m // 2
        e = m % 2

        @pl.when(e == 0)
        def _():
            v_d(n).wait_recv()
            v_h(n).wait_recv()
            for s in range(NS):
                pltpu.make_async_copy(w2n.at[s, :, tile(n)], w2_dst(m, s), w2sem.at[e, s]).start()

        @pl.when(e == 1)
        def _():
            v_b(n).wait_recv()
            v_g(n).wait_recv()
            for p in range(2):
                to = wbuf.at[w2_slot(m, 0), PART_ROWS[p]]
                pltpu.make_async_copy(w_out.at[out_row(p, y), tile(n)], to, w2sem.at[e, 4 * p]).start()
            for s in range(1, NS):
                pltpu.make_async_copy(w2y.at[s - 1, :, tile(n)], w2_dst(m, s), w2sem.at[e, s]).start()

    def arrive2(m):
        e = m % 2

        @pl.when(e == 0)
        def _():
            for s in range(NS):
                pltpu.make_async_copy(w2n.at[s, :, tile(0)], w2_dst(m, s), w2sem.at[e, s]).wait()

        @pl.when(e == 1)
        def _():
            for p in range(2):
                to = wbuf.at[w2_slot(m, 0), PART_ROWS[p]]
                pltpu.make_async_copy(w2n.at[0, PART_ROWS[p], tile(0)], to, w2sem.at[e, 4 * p]).wait()
            for s in range(1, NS):
                pltpu.make_async_copy(w2n.at[s, :, tile(0)], w2_dst(m, s), w2sem.at[e, s]).wait()

    def hand_c(n):
        v_c(n).wait_recv()
        v_d(n).start()
        v_f(n).start()

    def hand_e(n):
        v_e(n).wait_recv()
        v_g(n).start()

    def hand_f(n):
        v_f(n).wait_recv()
        v_h(n).start()

    hands = {7: [lambda: hand_c(0)], 10: [lambda: hand_e(0)], 13: [lambda: hand_c(1), lambda: v_e(2).start()],
             16: [lambda: hand_e(1), lambda: hand_f(0)], 19: [lambda: hand_c(2), lambda: v_e(3).start()],
             22: [lambda: hand_f(1)], 25: [lambda: hand_c(3)]}

    def w1_pass(p):
        layer_norm(2 * p)
        layer_norm(2 * p + 1)

        @pl.when(p == 0)
        def _():
            fetch1(p, 0)

        def step(t):
            @pl.when(t == 24)
            def _():
                h_done(0)
                h_done(1)
                attention(p)

            def fetch_next():
                @pl.when(t + 1 < NT)
                def _():
                    fetch1(p, t + 1)

                @pl.when((t + 1 == NT) & (p == 0))
                def _():
                    fetch1(1, 0)

                @pl.when((t + 1 == NT) & (p == 1))
                def _():
                    fetch2(0)

            @pl.when(p == 1)
            def _():
                fetch_next()
            w1_tile(p, t)

            @pl.when(p == 0)
            def _():
                fetch_next()

            for at, todo in hands.items():
                @pl.when((p == 1) & (t == at))
                def _(todo=todo):
                    for one in todo:
                        one()
        loop(0, NT, step)
        h_done(0)
        h_done(1)
    loop(0, 2, w1_pass)

    def load(e, i, src):
        return pltpu.make_async_copy(src, sv.at[e, i], vsem.at[e, i])

    def fin_loads(k, n, e):
        at = (part_rows(k), tile(n))
        return [load(e, 0, pa.at[at]), load(e, 1, ry.at[at]), load(e, 2, tok.at[own_out(k), tile(n)])]

    def fin_store(k, n, e):
        return pltpu.make_async_copy(sv.at[e, 3], out.at[own_out(k), tile(n)], vsem.at[e, 3])

    def fin_load(k, n, e):
        @pl.when(k % 2 == 0)
        def _():
            o_y(k // 2, n).wait_recv()
        start_all(fin_loads(k, n, e))

    def fin_do(k, n, e):
        wait_all(fin_loads(k, n, e))
        total = sv[e, 0].astype(F32) + sv[e, 1].astype(F32) + ob[:, tile(n)] + sv[e, 2].astype(F32)
        sv[e, 3] = total.astype(BF16)
        fin_store(k, n, e).start()

    def fin_send(k, n, e):
        fin_store(k, n, e).wait()
        o_x(k, n).start()
        o_c(k, n).start()

    def hand_out(k, n):
        o_x(k, n).wait_recv()
        o_f(k, n).start()

    fin_at = (16, 32, 52)
    NK = 2 * GROUPS

    def service(v):
        for n, at in enumerate(fin_at):
            i = v - at

            @pl.when((i >= 2) & (i < NK + 2))
            def _(n=n, i=i):
                fin_send(i - 2, n, v % 2)

            @pl.when((i >= 0) & (i < NK))
            def _(n=n, i=i):
                fin_load(i, n, v % 2)

            @pl.when((i >= 1) & (i < NK + 1))
            def _(n=n, i=i):
                fin_do(i - 1, n, (v + 1) % 2)

        @pl.when((v >= 42) & (v < 42 + NK))
        def _():
            hand_out(v - 42, 0)

    def j_copy(v):
        g, half = (v % 8) // 2, v % 2
        src = jb.at[rows_of(g), pl.ds(pl.multiple_of(half * KH, KH), KH)]
        return pltpu.make_async_copy(src, zj.at[half], jsem.at[half])

    def p_copy(m, g):
        n, slot = m // 2, g % 2
        return n, lambda ref: pltpu.make_async_copy(ptile.at[slot], ref.at[rows_of(g), tile(n)], psem.at[slot])

    def p_start(m, g):
        n, to = p_copy(m, g)

        @pl.when(m % 2 == 0)
        def _():
            to(pb).start()

        @pl.when(m % 2 == 1)
        def _():
            to(pa).start()

    def p_finish(m, g):
        n, to = p_copy(m, g)

        @pl.when(m % 2 == 0)
        def _():
            to(pb).wait()
            o_y(g, n).start()

        @pl.when(m % 2 == 1)
        def _():
            to(pa).wait()

    j_copy(0).start()

    def w2_tile(m):
        for at, todo in enumerate((lambda: hand_e(2), lambda: hand_f(2), lambda: hand_e(3), lambda: hand_f(3))):
            @pl.when(m == at)
            def _(todo=todo):
                todo()

        @pl.when(m + 1 < 2 * NN)
        def _():
            fetch2(m + 1)
        arrive2(m)

        def one(g):
            v = m * 2 * GROUPS + 2 * g
            j_copy(v + 1).start()
            j_copy(v).wait()
            acc[...] = jnp.dot(zj[0], wbuf[w2_slot(m, 0)], preferred_element_type=F32)
            service(v)

            @pl.when(v + 2 < 2 * NN * 2 * GROUPS)
            def _():
                j_copy(v + 2).start()
            j_copy(v + 1).wait()
            ptile[g % 2] = (acc[...] + jnp.dot(zj[1], wbuf[w2_slot(m, 1)], preferred_element_type=F32)).astype(BF16)
            p_start(m, g)

            @pl.when(g > 0)
            def _():
                p_finish(m, g - 1)
            service(v + 1)
        loop(0, GROUPS, one)
        p_finish(m, GROUPS - 1)
    loop(0, 2 * NN, w2_tile)

    def last(k):
        hand_out(k, 1)
        fin_load(k, NN - 1, 0)
        fin_do(k, NN - 1, 0)
        fin_send(k, NN - 1, 0)
    loop(0, NK, last)
    loop(0, NK, lambda k: hand_out(k, 2))
    loop(0, NK, lambda k: hand_out(k, 3))

    for one in small_far:
        one.wait_send()
    loop(0, 8, lambda k: t_dir(k).wait_send())
    for one in (w_c, w_b, w_d, w_e, w_f, w_g, w_h):
        loop(0, NJ, lambda j, one=one: one(j).wait_send())
    for one in (v_c, v_b, v_e, v_d, v_f, v_g, v_h):
        loop(0, NN, lambda n, one=one: one(n).wait_send())

    def settle(n):
        loop(0, GROUPS, lambda g: o_y(g, n).wait_send())

        def chunk(k):
            o_x(k, n).wait_send()
            for one in (o_c, o_f):
                one(k, n).wait_send()
                one(k, n).wait_recv()
        loop(0, NK, chunk)
    loop(0, NN, settle)


def solution(mesh):
    hbm = pl.BlockSpec(memory_space=pltpu.HBM)
    vmem = pl.BlockSpec(memory_space=pltpu.VMEM)

    def dma(*shape):
        return pltpu.SemaphoreType.DMA(shape)

    def local_layer(tokens, ln_scale, w_in, mlp_bias, q_scale, k_scale, w_out, attn_out_bias, mlp_out_bias):
        tok = tokens.reshape(-1, WID)
        row = lambda v: v.astype(F32).reshape(1, -1)
        of = lambda *shape: jax.ShapeDtypeStruct(shape, BF16)
        shapes = [of(*tok.shape), of(ROWS, WID), of(3, WID, NJ * TN), of(4, WID, NJ * TN), of(3, JB, WID), of(4, JB, WID),
                  of(3, NS, ROWS, TN), of(ROWS, NS * JB), of(ROWS, WID), of(ROWS, WID), of(ROWS, WID)]
        flops = 2 * ROWS * (2 * WID * NT * TN + NS * JB * 2 * WID)
        pairs = [(8,), (7, NJ), (3, NN, 2), (4, NN), (GROUPS, NN), (2 * GROUPS, NN), (2, 2 * GROUPS, NN), (4,)]
        res = pl.pallas_call(
            kernel,
            out_shape=shapes,
            in_specs=[hbm, hbm, hbm, hbm, hbm, hbm, hbm, vmem],
            out_specs=[hbm] * len(shapes),
            scratch_shapes=[
                pltpu.VMEM((2, M, KH), BF16),
                pltpu.VMEM((4, KH, TN), BF16),
                pltpu.VMEM((2, M, TN), BF16),
                pltpu.VMEM((M, TN), F32),
                pltpu.VMEM((2, 3, M, TN), BF16),
                pltpu.VMEM((2, 4, HALF, TN), BF16),
                pltpu.VMEM((2, 2, LN, WID), BF16),
                pltpu.VMEM((2, 1, WID), F32),
                pltpu.VMEM((NS, 1, UNITS // 2), F32),
                pltpu.VMEM((2, 1, DH), F32),
                dma(2, 2), dma(2, 5), dma(2), dma(2), dma(2, 3), dma(2, 4), dma(2, 2), dma(4),
            ] + [dma(*shape) for shape in pairs for _ in range(2)],
            compiler_params=pltpu.CompilerParams(collective_id=0, has_side_effects=True, vmem_limit_bytes=63 * 2**20),
            cost_estimate=pl.CostEstimate(flops=flops, bytes_accessed=2**30, transcendentals=0),
            name="layer",
        )(tok, row(ln_scale), w_in, row(mlp_bias), row(q_scale), row(k_scale), w_out, row(attn_out_bias) + row(mlp_out_bias))
        return res[0].reshape(tokens.shape)

    specs_in = (P('dp', None, 'my'), P('my'), P('my', 'mx'), P('mx'), P(), P(), P('mx', 'my'), P('my'), P('my'))
    return jax.shard_map(local_layer, mesh=mesh, in_specs=specs_in, out_specs=P('dp', None, 'my'), check_vma=False)
```

```python
import jax
import jax.numpy as jnp
from jax import lax
from jax.experimental import pallas as pl
from jax.experimental.pallas import tpu as pltpu
from jax.sharding import PartitionSpec as P

MESH = pl.DeviceIdType.MESH
F32, BF16 = jnp.float32, jnp.bfloat16

SEQ, DH, WID = 256, 256, 2048
M, GROUPS = 1024, 4
ROWS = M * GROUPS
HALF = M // 2
TN = 512
QKV, UNITS = 1024, 4096
NS = 4
NJ = 7
NT = NS * NJ
NN = WID // TN
JB = 5 * TN
KH = 2 * JB
LN = 128
EPS = 1e-6
NK = 2 * GROUPS
NL = NK // 2


def in_col(j, side):
    mlp = (j + 1) // 4
    at = (1 - mlp) * (QKV * j + (QKV // 2) * side) + mlp * (3 * QKV + (UNITS // 2) * side + TN * (j - 3))
    return pl.ds(pl.multiple_of(at, TN), TN)


def out_row(part, side):
    if part == 0:
        return pl.ds(pl.multiple_of((QKV // 2) * side, QKV // 2), TN)
    return pl.ds(pl.multiple_of(QKV + (UNITS // 2) * side, QKV), UNITS // 2)


PART_ROWS = (pl.ds(0, TN), pl.ds(TN, JB - TN))


def tile(n):
    return pl.ds(pl.multiple_of(n * TN, TN), TN)


def rows_of(g):
    return pl.ds(pl.multiple_of(g * M, M), M)


def tile_of(t):
    a, b = (t + 24) // 28, t // 24
    j = (1 - a) * (t // 2) + (a - b) * (t // 4 + 1 - 2 * ((t % 4) // 2)) + b * (t // 2 - 7)
    s = (1 - a) * (t % 2) + (a - b) * (t % 4) + b * (2 + t % 2)
    return j, s


def loop(lo, hi, body):
    def run(i, carry):
        body(i)
        return carry
    lax.fori_loop(lo, hi, run, 0)


def start_all(copies):
    for one in copies:
        one.start()


def wait_all(copies):
    for one in copies:
        one.wait()


def kernel(tok, w_in, w_out, vec,
           out, tail, toth, w1t, w1b, w2y, w2n, qkv, jb, pa, pb, ry,
           zj, wbuf, ptile, acc, abuf, sv, lbuf, sc, ub, gains, ob,
           w1sem, w2sem, jsem, psem, asem, vsem, lsem, csem,
           t_s, t_r, w_s, w_r, e_s, e_r, d_s, d_r, y_s, y_r, x_s, x_r, o_s, o_r, m_s, m_r):
    y = lax.axis_index("my")
    mi = lax.axis_index("mx")
    x, c = mi // 2, mi % 2
    dev_y = {"my": 1 - y, "mx": mi}
    dev_x = {"my": y, "mx": 2 * (1 - x) + c}
    dev_c = {"my": y, "mx": 2 * x + 1 - c}
    dev_d = {"my": y, "mx": 2 * (1 - x) + 1 - c}
    row0 = (2 * x + c) * ROWS
    row0_x = (2 * (1 - x) + c) * ROWS

    barrier = pltpu.get_barrier_semaphore()
    for dev in (dev_y, dev_x, dev_c, dev_d):
        pl.semaphore_signal(barrier, inc=1, device_id=dev, device_id_type=MESH)
    pl.semaphore_wait(barrier, 4)

    def remote(src, dst, ss, rs, dev):
        return pltpu.make_async_remote_copy(src_ref=src, dst_ref=dst, send_sem=ss, recv_sem=rs, device_id=dev, device_id_type=MESH)

    def t_dir(k):
        src = tok.at[pl.ds(pl.multiple_of(row0 + k * HALF, HALF), HALF)]
        return remote(src, toth.at[pl.ds(pl.multiple_of(k * HALF, HALF), HALF)], t_s.at[k], t_r.at[k], dev_y)

    C, B, D, E, F, G, H = range(7)

    def w_own(kind, j, side, dst, dev):
        return remote(w_in.at[:, in_col(j, side)], dst.at[:, tile(j)], w_s.at[kind, j], w_r.at[kind, j], dev)

    def w_pass(kind, j, src, dst, dev):
        return remote(src.at[:, tile(j)], dst.at[:, tile(j)], w_s.at[kind, j], w_r.at[kind, j], dev)

    tops = [None] + [w1t.at[i] for i in range(NS - 1)]
    bots = [w1b.at[i] for i in range(NS)]
    OWN, CORE, FAR, FAR_CORE = range(NS)
    w_c = lambda j: w_own(C, j, 1 - y, bots[OWN], dev_y)
    w_b = lambda j: w_own(B, j, y, tops[CORE], dev_c)
    w_d = lambda j: w_pass(D, j, bots[OWN], bots[CORE], dev_c)
    w_e = lambda j: w_own(E, j, y, tops[FAR], dev_x)
    w_f = lambda j: w_pass(F, j, bots[OWN], bots[FAR], dev_x)
    w_g = lambda j: w_pass(G, j, tops[FAR], tops[FAR_CORE], dev_c)
    w_h = lambda j: w_pass(H, j, bots[FAR], bots[FAR_CORE], dev_c)

    class Two:
        def __init__(self, kind, n, side, dst, dev):
            self.copies = [remote(w_out.at[out_row(p, side), tile(n)], dst.at[rows, tile(n)], e_s.at[kind, n, p], e_r.at[kind, n, p], dev)
                           for p, rows in enumerate(PART_ROWS)]

        def start(self):
            start_all(self.copies)

        def wait_send(self):
            for one in self.copies:
                one.wait_send()

        def wait_recv(self):
            for one in self.copies:
                one.wait_recv()

    def v_pass(kind, n, src, dst, dev):
        return remote(src.at[:, tile(n)], dst.at[:, tile(n)], d_s.at[kind, n], d_r.at[kind, n], dev)

    mine = [None] + [w2y.at[i] for i in range(NS - 1)]
    theirs = [w2n.at[i] for i in range(NS)]
    v_c = lambda n: Two(C, n, 1 - y, theirs[OWN], dev_y)
    v_b = lambda n: Two(B, n, y, mine[CORE], dev_c)
    v_e = lambda n: Two(D, n, y, mine[FAR], dev_x)
    v_d = lambda n: v_pass(C, n, theirs[OWN], theirs[CORE], dev_c)
    v_f = lambda n: v_pass(B, n, theirs[OWN], theirs[FAR], dev_x)
    v_g = lambda n: v_pass(D, n, mine[FAR], mine[FAR_CORE], dev_c)
    v_h = lambda n: v_pass(E, n, theirs[FAR], theirs[FAR_CORE], dev_c)

    def o_y(g, n):
        return remote(pb.at[rows_of(g), tile(n)], ry.at[rows_of(g), tile(n)], y_s.at[g, n], y_r.at[g, n], dev_y)

    def part_rows(k):
        return pl.ds(pl.multiple_of(k * HALF, HALF), HALF)

    def own_out(k):
        return pl.ds(pl.multiple_of(row0 + k * HALF, HALF), HALF)

    def o_x(k, n):
        at = out.at[own_out(k), tile(n)]
        return remote(at, at, x_s.at[k, n], x_r.at[k, n], dev_x)

    def o_c(k, n):
        at = out.at[own_out(k), tile(n)]
        return remote(at, at, o_s.at[0, k, n], o_r.at[0, k, n], dev_c)

    def o_f(k, n):
        at = out.at[pl.ds(pl.multiple_of(row0_x + k * HALF, HALF), HALF), tile(n)]
        return remote(at, at, o_s.at[1, k, n], o_r.at[1, k, n], dev_c)

    lns = vec.at[:, pl.ds(0, WID)]
    my_units = vec.at[:, pl.ds(pl.multiple_of(WID + y * (UNITS // 2), UNITS // 2), UNITS // 2)]
    at = WID + UNITS
    small_far = [remote(src, dst, m_s.at[i], m_r.at[i], dev) for i, (src, dst, dev) in enumerate((
        (lns, sc.at[1], dev_y), (my_units, ub.at[CORE], dev_c), (my_units, ub.at[FAR], dev_x), (my_units, ub.at[FAR_CORE], dev_d)))]
    small = [pltpu.make_async_copy(src, dst, csem.at[i]) for i, (src, dst) in enumerate((
        (lns, sc.at[0]), (my_units, ub.at[OWN]), (vec.at[:, pl.ds(at, DH)], gains.at[0]),
        (vec.at[:, pl.ds(at + DH, DH)], gains.at[1]), (vec.at[:, pl.ds(at + 2 * DH, WID)], ob)))]

    start_all(small_far)
    loop(0, 4, lambda k: t_dir(k).start())
    loop(0, NJ, lambda j: w_c(j).start())
    loop(4, 8, lambda k: t_dir(k).start())
    loop(0, NN, lambda n: v_c(n).start())
    loop(0, 5, lambda j: w_e(j).start())
    loop(0, NJ, lambda j: w_b(j).start())
    loop(0, NN, lambda n: v_b(n).start())
    start_all(small)
    wait_all(small)
    for one in small_far:
        one.wait_recv()

    def l_copies(g, i, slot):
        at = pl.multiple_of(g * M + i * LN, LN)
        return (
            pltpu.make_async_copy(tok.at[pl.ds(pl.multiple_of(row0 + at, LN), LN)], lbuf.at[slot, 0], lsem.at[slot, 0]),
            pltpu.make_async_copy(toth.at[pl.ds(at, LN)], lbuf.at[slot, 1], lsem.at[slot, 1]),
        )

    def layer_norm(g):
        steps = M // LN
        t_dir(2 * g).wait_recv()
        start_all(l_copies(g, 0, 0))

        def rows(i):
            slot = i % 2

            @pl.when(i == steps // 2 - 1)
            def _():
                t_dir(2 * g + 1).wait_recv()

            @pl.when(i + 1 < steps)
            def _():
                start_all(l_copies(g, i + 1, 1 - slot))
            wait_all(l_copies(g, i, slot))
            step = 64

            def part(k):
                at = pl.ds(pl.multiple_of(k * step, step), step)
                a, b = lbuf[slot, 0, at].astype(F32), lbuf[slot, 1, at].astype(F32)
                mean = (jnp.sum(a, -1, keepdims=True) + jnp.sum(b, -1, keepdims=True)) * (0.5 / WID)
                a, b = a - mean, b - mean
                var = (jnp.sum(a * a, -1, keepdims=True) + jnp.sum(b * b, -1, keepdims=True)) * (0.5 / WID)
                inv = lax.rsqrt(var + EPS)
                to = pl.ds(pl.multiple_of(i * LN + k * step, step), step)
                zj[g % 2, to, :WID] = (a * inv * sc[0]).astype(BF16)
                zj[g % 2, to, WID:2 * WID] = (b * inv * sc[1]).astype(BF16)
            loop(0, LN // step, part)
        loop(0, steps, rows)

    def w1_copies(slot, top, bottom):
        return (
            pltpu.make_async_copy(top, wbuf.at[slot, :WID], w1sem.at[slot, 0]),
            pltpu.make_async_copy(bottom, wbuf.at[slot, WID:2 * WID], w1sem.at[slot, 1]),
        )

    def fetch1(p, t):
        j, s = tile_of(t)
        slot = t % 2

        @pl.when(p == 0)
        def _():
            @pl.when(s == 0)
            def _():
                w_c(j).wait_recv()
                w_d(j).start()
                w_f(j).start()

                @pl.when((j == 1) | (j == 3))
                def _():
                    w_e((j + 9) // 2).start()

                @pl.when(j == NJ - 1)
                def _():
                    v_e(0).start()
                    v_e(1).start()

            @pl.when(s == 1)
            def _():
                w_b(j).wait_recv()
                w_d(j).wait_recv()

            @pl.when(s == 2)
            def _():
                w_e(j).wait_recv()
                w_g(j).start()
                w_f(j).wait_recv()
                w_h(j).start()

            @pl.when(s == 3)
            def _():
                w_g(j).wait_recv()
                w_h(j).wait_recv()

        @pl.when(s == 0)
        def _():
            start_all(w1_copies(slot, w_in.at[:, in_col(j, y)], w1b.at[0, :, tile(j)]))

        @pl.when(s > 0)
        def _():
            start_all(w1_copies(slot, w1t.at[s - 1, :, tile(j)], w1b.at[s, :, tile(j)]))

    def h_store(slot, dst):
        return pltpu.make_async_copy(ptile.at[slot], dst, psem.at[slot])

    def h_done(slot):
        h_store(slot, pb.at[rows_of(0), tile(0)]).wait()

    def w1_tile(p, t):
        j, s = tile_of(t)
        wait_all(w1_copies(t % 2, w1t.at[0, :, tile(0)], w1b.at[0, :, tile(0)]))

        def one(gl):
            g = 2 * p + gl

            def project():
                h = (jnp.dot(zj[gl, :, :WID], wbuf[t % 2, :WID], preferred_element_type=F32)
                     + jnp.dot(zj[gl, :, WID:2 * WID], wbuf[t % 2, WID:2 * WID], preferred_element_type=F32))
                return h.astype(BF16)

            @pl.when((t > 0) & (t != 24))
            def _():
                h_done(gl)

            @pl.when(j < 2)
            def _():
                h = project().astype(F32)
                gain = gains[j]
                for k in range(2):
                    part = h[:, k * DH:(k + 1) * DH]
                    part = part - jnp.mean(part, -1, keepdims=True)
                    var = jnp.mean(part * part, -1, keepdims=True)
                    ptile[gl, :, k * DH:(k + 1) * DH] = (part * lax.rsqrt(var + EPS) * gain).astype(BF16)

            @pl.when(j == 2)
            def _():
                ptile[gl] = project()

            @pl.when(j > 2)
            def _():
                h = project().astype(F32) + ub[s, :, tile(j - 3)]
                ptile[gl] = (0.5 * h * (1.0 + lax.erf(h * 0.7071067811865476))).astype(BF16)

            @pl.when(j <= 2)
            def _():
                h_store(gl, qkv.at[j, s, rows_of(g)]).start()

            @pl.when(j > 2)
            def _():
                h_store(gl, jb.at[rows_of(g), pl.ds(pl.multiple_of(s * JB + (j - 2) * TN, TN), TN)]).start()
        loop(0, 2, one)

    def a_loads(p, w, slot):
        g, s = 2 * p + w // NS, w % NS
        return [pltpu.make_async_copy(qkv.at[i, s, rows_of(g)], abuf.at[slot, i], asem.at[slot, i]) for i in range(3)]

    def a_store(p, w, slot):
        g, s = 2 * p + w // NS, w % NS
        return h_store(slot, jb.at[rows_of(g), pl.ds(pl.multiple_of(s * JB, TN), TN)])

    def attention(p):
        units = 2 * NS
        start_all(a_loads(p, 0, 0))

        def unit(w):
            slot = w % 2

            @pl.when(w + 1 < units)
            def _():
                start_all(a_loads(p, w + 1, 1 - slot))
            wait_all(a_loads(p, w, slot))

            @pl.when(w >= 2)
            def _():
                a_store(p, w - 2, slot).wait()

            def images(i):
                for ii in range(2):
                    at = pl.ds(pl.multiple_of((2 * i + ii) * SEQ, SEQ), SEQ)
                    for k in range(2):
                        cols = slice(k * DH, (k + 1) * DH)
                        q, kk, v = abuf[slot, 0, at, cols], abuf[slot, 1, at, cols], abuf[slot, 2, at, cols]
                        lg = lax.dot_general(q, kk, (((1,), (1,)), ((), ())), preferred_element_type=F32) * (DH ** -0.5)
                        e = jnp.exp(lg - jnp.max(lg, -1, keepdims=True))
                        prob = (e / jnp.sum(e, -1, keepdims=True)).astype(BF16)
                        ptile[slot, at, cols] = jnp.dot(prob, v, preferred_element_type=F32).astype(BF16)
            loop(0, M // SEQ // 2, images)
            a_store(p, w, slot).start()
        loop(0, units, unit)
        a_store(p, units - 2, 0).wait()
        a_store(p, units - 1, 1).wait()

    def w2_slot(m, half):
        return 2 * ((m + 1) % 2) + half

    def w2_dst(m, s):
        return wbuf.at[w2_slot(m, s // 2), pl.ds((s % 2) * JB, JB)]

    def fetch2(m):
        n = m // 2
        e = m % 2

        @pl.when(e == 0)
        def _():
            v_d(n).wait_recv()
            v_h(n).wait_recv()
            for s in range(NS):
                pltpu.make_async_copy(w2n.at[s, :, tile(n)], w2_dst(m, s), w2sem.at[e, s]).start()

        @pl.when(e == 1)
        def _():
            v_b(n).wait_recv()
            v_g(n).wait_recv()
            for p in range(2):
                to = wbuf.at[w2_slot(m, 0), PART_ROWS[p]]
                pltpu.make_async_copy(w_out.at[out_row(p, y), tile(n)], to, w2sem.at[e, 4 * p]).start()
            for s in range(1, NS):
                pltpu.make_async_copy(w2y.at[s - 1, :, tile(n)], w2_dst(m, s), w2sem.at[e, s]).start()

    def arrive2(m):
        e = m % 2

        @pl.when(e == 0)
        def _():
            for s in range(NS):
                pltpu.make_async_copy(w2n.at[s, :, tile(0)], w2_dst(m, s), w2sem.at[e, s]).wait()

        @pl.when(e == 1)
        def _():
            for p in range(2):
                to = wbuf.at[w2_slot(m, 0), PART_ROWS[p]]
                pltpu.make_async_copy(w2n.at[0, PART_ROWS[p], tile(0)], to, w2sem.at[e, 4 * p]).wait()
            for s in range(1, NS):
                pltpu.make_async_copy(w2n.at[s, :, tile(0)], w2_dst(m, s), w2sem.at[e, s]).wait()

    def hand_c(n):
        v_c(n).wait_recv()
        v_d(n).start()
        v_f(n).start()

    def hand_e(n):
        v_e(n).wait_recv()
        v_g(n).start()

    def hand_f(n):
        v_f(n).wait_recv()
        v_h(n).start()

    hands = {5: [lambda: hand_c(0)], 8: [lambda: hand_e(0)], 11: [lambda: hand_c(1), lambda: v_e(2).start()],
             14: [lambda: hand_e(1), lambda: hand_f(0)], 17: [lambda: hand_c(2), lambda: v_e(3).start()],
             20: [lambda: hand_f(1)], 23: [lambda: hand_c(3)]}

    def w1_pass(p):
        layer_norm(2 * p)
        layer_norm(2 * p + 1)

        @pl.when(p == 0)
        def _():
            fetch1(p, 0)

        def step(t):
            @pl.when(t == 24)
            def _():
                h_done(0)
                h_done(1)
                attention(p)

            def fetch_next():
                @pl.when(t + 1 < NT)
                def _():
                    fetch1(p, t + 1)

                @pl.when((t + 1 == NT) & (p == 0))
                def _():
                    fetch1(1, 0)

                @pl.when((t + 1 == NT) & (p == 1))
                def _():
                    fetch2(0)

            @pl.when(p == 1)
            def _():
                fetch_next()
            w1_tile(p, t)

            @pl.when(p == 0)
            def _():
                fetch_next()

            for at, todo in hands.items():
                @pl.when((p == 1) & (t == at))
                def _(todo=todo):
                    for one in todo:
                        one()
        loop(0, NT, step)
        h_done(0)
        h_done(1)
    loop(0, 2, w1_pass)

    def load(e, i, src):
        return pltpu.make_async_copy(src, sv.at[e, i], vsem.at[e, i])

    def fin_loads(k, n, e):
        at = (part_rows(k), tile(n))
        return [load(e, 0, pa.at[at]), load(e, 1, ry.at[at]), load(e, 2, tok.at[own_out(k), tile(n)])]

    def fin_store(k, n, e):
        return pltpu.make_async_copy(sv.at[e, 3], out.at[own_out(k), tile(n)], vsem.at[e, 3])

    def tail_store(k, e):
        return pltpu.make_async_copy(sv.at[e, 3], tail.at[part_rows(k - NL)], vsem.at[e, 4])

    def is_tail(k, n):
        return (n == NN - 1) & (k >= NL)

    def fin_load(k, n, e):
        @pl.when(k % 2 == 0)
        def _():
            o_y(k // 2, n).wait_recv()
        start_all(fin_loads(k, n, e))

    def fin_do(k, n, e):
        wait_all(fin_loads(k, n, e))
        total = sv[e, 0].astype(F32) + sv[e, 1].astype(F32) + ob[:, tile(n)] + sv[e, 2].astype(F32)
        sv[e, 3] = total.astype(BF16)
        fin_store(k, n, e).start()

        @pl.when(is_tail(k, n))
        def _():
            tail_store(k, e).start()

    def fin_send(k, n, e):
        fin_store(k, n, e).wait()

        @pl.when(is_tail(k, n))
        def _():
            tail_store(k, e).wait()

        @pl.when(jnp.logical_not(is_tail(k, n)))
        def _():
            o_x(k, n).start()
        o_c(k, n).start()

    def hand_out(k, n):
        o_x(k, n).wait_recv()
        o_f(k, n).start()

    STEPS = 2 * NN * NK

    def service(v):
        f = v - 12
        n, i = f // 16, f % 16

        @pl.when((f >= 0) & (i >= 2) & (i < NK + 2))
        def _():
            fin_send(i - 2, n, v % 2)

        @pl.when((f >= 0) & (i < NK))
        def _():
            fin_load(i, n, v % 2)

        @pl.when((f >= 0) & (i >= 1) & (i < NK + 1))
        def _():
            fin_do(i - 1, n, (v + 1) % 2)

        for n, at in enumerate((33, 49)):
            @pl.when((v >= at) & (v < at + NK))
            def _(n=n, at=at):
                hand_out(v - at, n)

    def j_copy(v):
        g, half = (v % 8) // 2, v % 2
        src = jb.at[rows_of(g), pl.ds(pl.multiple_of(half * KH, KH), KH)]
        return pltpu.make_async_copy(src, zj.at[half], jsem.at[half])

    def p_copy(m, g):
        n, slot = m // 2, g % 2
        return n, lambda ref: pltpu.make_async_copy(ptile.at[slot], ref.at[rows_of(g), tile(n)], psem.at[slot])

    def p_start(m, g):
        n, to = p_copy(m, g)

        @pl.when(m % 2 == 0)
        def _():
            to(pb).start()

        @pl.when(m % 2 == 1)
        def _():
            to(pa).start()

    def p_finish(m, g):
        n, to = p_copy(m, g)

        @pl.when(m % 2 == 0)
        def _():
            to(pb).wait()
            o_y(g, n).start()

        @pl.when(m % 2 == 1)
        def _():
            to(pa).wait()

    j_copy(0).start()

    def w2_tile(m):
        for at, todo in enumerate((lambda: hand_e(2), lambda: hand_f(2), lambda: hand_e(3), lambda: hand_f(3))):
            @pl.when(m == at)
            def _(todo=todo):
                todo()

        @pl.when(m + 1 < 2 * NN)
        def _():
            fetch2(m + 1)
        arrive2(m)

        def one(g):
            v = m * 2 * GROUPS + 2 * g
            j_copy(v + 1).start()
            j_copy(v).wait()
            acc[...] = jnp.dot(zj[0], wbuf[w2_slot(m, 0)], preferred_element_type=F32)
            service(v)

            @pl.when(v + 2 < STEPS)
            def _():
                j_copy(v + 2).start()
            j_copy(v + 1).wait()
            ptile[g % 2] = (acc[...] + jnp.dot(zj[1], wbuf[w2_slot(m, 1)], preferred_element_type=F32)).astype(BF16)
            p_start(m, g)

            @pl.when(g > 0)
            def _():
                p_finish(m, g - 1)
            service(v + 1)
        loop(0, GROUPS, one)
        p_finish(m, GROUPS - 1)
    loop(0, 2 * NN, w2_tile)

    loop(STEPS, STEPS + 6, service)
    loop(0, NK, lambda k: hand_out(k, 2))
    loop(0, NK - NL, lambda k: hand_out(k, 3))

    for one in small_far:
        one.wait_send()
    loop(0, 8, lambda k: t_dir(k).wait_send())
    for one in (w_c, w_b, w_d, w_e, w_f, w_g, w_h):
        loop(0, NJ, lambda j, one=one: one(j).wait_send())
    for one in (v_c, v_b, v_e, v_d, v_f, v_g, v_h):
        loop(0, NN, lambda n, one=one: one(n).wait_send())

    def settle(n):
        loop(0, GROUPS, lambda g: o_y(g, n).wait_send())

        def chunk(k):
            o_c(k, n).wait_send()
            o_c(k, n).wait_recv()
        loop(0, NK, chunk)

        def far_chunk(k):
            o_x(k, n).wait_send()
            o_f(k, n).wait_send()
            o_f(k, n).wait_recv()
        loop(0, NK - NL * (n // (NN - 1)), far_chunk)
    loop(0, NN, settle)


def copy_kernel(src, dst, buf, sem):
    slots = buf.shape[0]
    x = lax.axis_index("mx") // 2

    def moves(i):
        first = (x + i // (2 * NK)) % 2
        rows = pl.ds(pl.multiple_of(first * 2 * ROWS + (i % (2 * NK)) * HALF, HALF), HALF)
        late = i >= 2 * NK and i % NK >= NL
        cols = pl.ds(0, WID - TN if late else WID)
        k = i % slots
        return (pltpu.make_async_copy(src.at[rows, cols], buf.at[k, :, cols], sem.at[0, k]),
                pltpu.make_async_copy(buf.at[k, :, cols], dst.at[rows, cols], sem.at[1, k]))
    every = [moves(i) for i in range(4 * NK)]
    ahead = slots // 2
    for i in range(4 * NK + ahead):
        if i < 4 * NK:
            if i >= slots:
                every[i - slots][1].wait()
            every[i][0].start()
        if i >= ahead:
            every[i - ahead][0].wait()
            every[i - ahead][1].start()
    for i in range(4 * NK - slots, 4 * NK):
        every[i][1].wait()


def tail_kernel(base, far, farther, out, buf, sem):
    mi = lax.axis_index("mx")
    x, c = mi // 2, mi % 2
    pieces = ((far, c), (farther, 1 - c))
    loads = [pltpu.make_async_copy(ref, buf.at[i], sem.at[0, i]) for i, (ref, _) in enumerate(pieces)]
    start_all(loads)
    stores = []
    for i, (_, cc) in enumerate(pieces):
        at = pl.multiple_of((2 * (1 - x) + cc) * ROWS + NL * HALF, HALF)
        store = pltpu.make_async_copy(buf.at[i], out.at[pl.ds(at, (NK - NL) * HALF), pl.ds((NN - 1) * TN, TN)], sem.at[1, i])
        loads[i].wait()
        store.start()
        stores.append(store)
    wait_all(stores)


def solution(mesh):
    hbm = pl.BlockSpec(memory_space=pltpu.HBM)

    def dma(*shape):
        return pltpu.SemaphoreType.DMA(shape)

    def local_layer(tokens, ln_scale, w_in, mlp_bias, q_scale, k_scale, w_out, attn_out_bias, mlp_out_bias):
        tok = tokens.reshape(-1, WID)
        ob = attn_out_bias.astype(F32) + mlp_out_bias.astype(F32)
        vec = jnp.concatenate([v.astype(F32) for v in (ln_scale, mlp_bias, q_scale, k_scale)] + [ob]).reshape(1, -1)
        of = lambda *shape: jax.ShapeDtypeStruct(shape, BF16)
        shapes = [of(*tok.shape), of((NK - NL) * HALF, TN), of(ROWS, WID), of(3, WID, NJ * TN), of(4, WID, NJ * TN), of(3, JB, WID), of(4, JB, WID),
                  of(3, NS, ROWS, TN), of(ROWS, NS * JB), of(ROWS, WID), of(ROWS, WID), of(ROWS, WID)]
        flops = 2 * ROWS * (2 * WID * NT * TN + NS * JB * 2 * WID)
        pairs = [(8,), (7, NJ), (3, NN, 2), (4, NN), (GROUPS, NN), (2 * GROUPS, NN), (2, 2 * GROUPS, NN), (4,)]
        res = pl.pallas_call(
            kernel,
            out_shape=shapes,
            in_specs=[hbm] * 4,
            out_specs=[hbm] * len(shapes),
            scratch_shapes=[
                pltpu.VMEM((2, M, KH), BF16),
                pltpu.VMEM((4, KH, TN), BF16),
                pltpu.VMEM((2, M, TN), BF16),
                pltpu.VMEM((M, TN), F32),
                pltpu.VMEM((2, 3, M, TN), BF16),
                pltpu.VMEM((2, 4, HALF, TN), BF16),
                pltpu.VMEM((2, 2, LN, WID), BF16),
                pltpu.VMEM((2, 1, WID), F32),
                pltpu.VMEM((NS, 1, UNITS // 2), F32),
                pltpu.VMEM((2, 1, DH), F32),
                pltpu.VMEM((1, WID), F32),
                dma(2, 2), dma(2, 5), dma(2), dma(2), dma(2, 3), dma(2, 5), dma(2, 2), dma(5),
            ] + [dma(*shape) for shape in pairs for _ in range(2)],
            compiler_params=pltpu.CompilerParams(collective_id=0, has_side_effects=True, vmem_limit_bytes=63 * 2**20),
            cost_estimate=pl.CostEstimate(flops=flops, bytes_accessed=2**30, transcendentals=0),
            name="layer",
        )(tok, w_in, w_out, vec)
        base, own = res[0], res[1]
        far = lax.ppermute(own, 'mx', [(0, 2), (1, 3), (2, 0), (3, 1)])
        base = pl.pallas_call(
            copy_kernel,
            out_shape=of(*tok.shape),
            in_specs=[hbm],
            out_specs=hbm,
            scratch_shapes=[pltpu.VMEM((16, HALF, WID), BF16), dma(2, 16)],
            compiler_params=pltpu.CompilerParams(vmem_limit_bytes=40 * 2**20),
            cost_estimate=pl.CostEstimate(flops=2 * 10**10, bytes_accessed=4 * tok.size, transcendentals=0),
            name="place",
        )(base)
        far, base = lax.optimization_barrier((far, base))
        farther = lax.ppermute(far, 'mx', [(0, 1), (1, 0), (2, 3), (3, 2)])
        out = pl.pallas_call(
            tail_kernel,
            out_shape=of(*tok.shape),
            in_specs=[hbm] * 3,
            out_specs=hbm,
            input_output_aliases={0: 0},
            scratch_shapes=[pltpu.VMEM((2, (NK - NL) * HALF, TN), BF16), dma(2, 2)],
            name="place_last",
        )(base, far, farther)
        return out.reshape(tokens.shape)

    specs_in = (P('dp', None, 'my'), P('my'), P('my', 'mx'), P('mx'), P(), P(), P('mx', 'my'), P('my'), P('my'))
    return jax.shard_map(local_layer, mesh=mesh, in_specs=specs_in, out_specs=P('dp', None, 'my'), check_vma=False)
```

```python
import jax
import jax.numpy as jnp
from jax import lax
from jax.experimental import pallas as pl
from jax.experimental.pallas import tpu as pltpu
from jax.sharding import PartitionSpec as P

MESH = pl.DeviceIdType.MESH
F32, BF16 = jnp.float32, jnp.bfloat16

SEQ, DH, WID = 256, 256, 2048
M, GROUPS = 1024, 4
ROWS = M * GROUPS
HALF = M // 2
TN = 512
QKV, UNITS = 1024, 4096
NS = 4
NJ = 7
NT = NS * NJ
NN = WID // TN
JB = 5 * TN
KH = 2 * JB
VEC = 3 * WID + UNITS + 2 * DH
LN = 128
EPS = 1e-6
NK = 2 * GROUPS
NL = NK // 2


def in_col(j, side):
    mlp = (j + 1) // 4
    at = (1 - mlp) * (QKV * j + (QKV // 2) * side) + mlp * (3 * QKV + (UNITS // 2) * side + TN * (j - 3))
    return pl.ds(pl.multiple_of(at, TN), TN)


def out_row(part, side):
    if part == 0:
        return pl.ds(pl.multiple_of((QKV // 2) * side, QKV // 2), TN)
    return pl.ds(pl.multiple_of(QKV + (UNITS // 2) * side, QKV), UNITS // 2)


PART_ROWS = (pl.ds(0, TN), pl.ds(TN, JB - TN))


def tile(n):
    return pl.ds(pl.multiple_of(n * TN, TN), TN)


def rows_of(g):
    return pl.ds(pl.multiple_of(g * M, M), M)


def tile_of(t):
    a, b = (t + 24) // 28, t // 24
    j = (1 - a) * (t // 2) + (a - b) * (t // 4 + 1 - 2 * ((t % 4) // 2)) + b * (t // 2 - 7)
    s = (1 - a) * (t % 2) + (a - b) * (t % 4) + b * (2 + t % 2)
    return j, s


def loop(lo, hi, body):
    def run(i, carry):
        body(i)
        return carry
    lax.fori_loop(lo, hi, run, 0)


def start_all(copies):
    for one in copies:
        one.start()


def wait_all(copies):
    for one in copies:
        one.wait()


def kernel(tok, w_in, w_out, vec,
           out, tail, toth, w1t, w1b, w2y, w2n, qkv, jb, pa, pb, ry,
           zj, wbuf, ptile, acc, abuf, sv, lbuf, sc, ub, gains, ob,
           w1sem, w2sem, jsem, psem, asem, vsem, lsem, csem,
           t_s, t_r, w_s, w_r, e_s, e_r, d_s, d_r, y_s, y_r, x_s, x_r, o_s, o_r, m_s, m_r):
    y = lax.axis_index("my")
    mi = lax.axis_index("mx")
    x, c = mi // 2, mi % 2
    dev_y = {"my": 1 - y, "mx": mi}
    dev_x = {"my": y, "mx": 2 * (1 - x) + c}
    dev_c = {"my": y, "mx": 2 * x + 1 - c}
    dev_d = {"my": y, "mx": 2 * (1 - x) + 1 - c}
    row0 = (2 * x + c) * ROWS
    row0_x = (2 * (1 - x) + c) * ROWS

    barrier = pltpu.get_barrier_semaphore()
    for dev in (dev_y, dev_x, dev_c, dev_d):
        pl.semaphore_signal(barrier, inc=1, device_id=dev, device_id_type=MESH)
    pl.semaphore_wait(barrier, 4)

    def remote(src, dst, ss, rs, dev):
        return pltpu.make_async_remote_copy(src_ref=src, dst_ref=dst, send_sem=ss, recv_sem=rs, device_id=dev, device_id_type=MESH)

    def t_dir(k):
        src = tok.at[pl.ds(pl.multiple_of(row0 + k * HALF, HALF), HALF)]
        return remote(src, toth.at[pl.ds(pl.multiple_of(k * HALF, HALF), HALF)], t_s, t_r.at[k], dev_y)

    C, B, D, E, F, G, H = range(7)

    def w_own(kind, j, side, dst, dev):
        return remote(w_in.at[:, in_col(j, side)], dst.at[:, tile(j)], w_s.at[kind], w_r.at[kind, j], dev)

    def w_pass(kind, j, src, dst, dev):
        return remote(src.at[:, tile(j)], dst.at[:, tile(j)], w_s.at[kind], w_r.at[kind, j], dev)

    tops = [None] + [w1t.at[i] for i in range(NS - 1)]
    bots = [w1b.at[i] for i in range(NS)]
    OWN, CORE, FAR, FAR_CORE = range(NS)
    w_c = lambda j: w_own(C, j, 1 - y, bots[OWN], dev_y)
    w_b = lambda j: w_own(B, j, y, tops[CORE], dev_c)
    w_d = lambda j: w_pass(D, j, bots[OWN], bots[CORE], dev_c)
    w_e = lambda j: w_own(E, j, y, tops[FAR], dev_x)
    w_f = lambda j: w_pass(F, j, bots[OWN], bots[FAR], dev_x)
    w_g = lambda j: w_pass(G, j, tops[FAR], tops[FAR_CORE], dev_c)
    w_h = lambda j: w_pass(H, j, bots[FAR], bots[FAR_CORE], dev_c)

    class Two:
        def __init__(self, kind, n, side, dst, dev):
            self.copies = [remote(w_out.at[out_row(p, side), tile(n)], dst.at[rows, tile(n)], e_s.at[kind], e_r.at[kind, n], dev)
                           for p, rows in enumerate(PART_ROWS)]
            self.both = remote(dst.at[:, tile(n)], dst.at[:, tile(n)], e_s.at[kind], e_r.at[kind, n], dev)

        def start(self):
            start_all(self.copies)

        def wait_recv(self):
            self.both.wait_recv()

    def v_pass(kind, n, src, dst, dev):
        return remote(src.at[:, tile(n)], dst.at[:, tile(n)], d_s.at[kind], d_r.at[kind, n], dev)

    mine = [None] + [w2y.at[i] for i in range(NS - 1)]
    theirs = [w2n.at[i] for i in range(NS)]
    v_c = lambda n: Two(C, n, 1 - y, theirs[OWN], dev_y)
    v_b = lambda n: Two(B, n, y, mine[CORE], dev_c)
    v_e = lambda n: Two(D, n, y, mine[FAR], dev_x)
    v_d = lambda n: v_pass(C, n, theirs[OWN], theirs[CORE], dev_c)
    v_f = lambda n: v_pass(B, n, theirs[OWN], theirs[FAR], dev_x)
    v_g = lambda n: v_pass(D, n, mine[FAR], mine[FAR_CORE], dev_c)
    v_h = lambda n: v_pass(E, n, theirs[FAR], theirs[FAR_CORE], dev_c)

    def o_y(g, n):
        return remote(pb.at[rows_of(g), tile(n)], ry.at[rows_of(g), tile(n)], y_s, y_r.at[g, n], dev_y)

    def part_rows(k):
        return pl.ds(pl.multiple_of(k * HALF, HALF), HALF)

    def own_out(k):
        return pl.ds(pl.multiple_of(row0 + k * HALF, HALF), HALF)

    def o_x(k, n):
        at = out.at[own_out(k), tile(n)]
        return remote(at, at, x_s, x_r.at[k, n], dev_x)

    def o_c(k, n):
        at = out.at[own_out(k), tile(n)]
        return remote(at, at, o_s.at[0], o_r.at[0], dev_c)

    def o_f(k, n):
        at = out.at[pl.ds(pl.multiple_of(row0_x + k * HALF, HALF), HALF), tile(n)]
        return remote(at, at, o_s.at[1], o_r.at[1], dev_c)

    lns = vec.at[:, pl.ds(0, WID)]
    my_units = vec.at[:, pl.ds(pl.multiple_of(WID + y * (UNITS // 2), UNITS // 2), UNITS // 2)]
    at = WID + UNITS
    small_far = [remote(src, dst, m_s.at[i], m_r.at[i], dev) for i, (src, dst, dev) in enumerate((
        (lns, sc.at[1], dev_y), (my_units, ub.at[CORE], dev_c), (my_units, ub.at[FAR], dev_x), (my_units, ub.at[FAR_CORE], dev_d)))]
    small = [pltpu.make_async_copy(src, dst, csem.at[i]) for i, (src, dst) in enumerate((
        (lns, sc.at[0]), (my_units, ub.at[OWN]), (vec.at[:, pl.ds(at, DH)], gains.at[0]),
        (vec.at[:, pl.ds(at + DH, DH)], gains.at[1]), (vec.at[:, pl.ds(at + 2 * DH, WID)], ob.at[0]),
        (vec.at[:, pl.ds(at + 2 * DH + WID, WID)], ob.at[1])))]

    loop(0, NS, lambda j: w_e(j).start())
    start_all(small_far)
    loop(0, NS, lambda k: t_dir(k).start())
    loop(0, NJ, lambda j: w_c(j).start())
    loop(NS, NK, lambda k: t_dir(k).start())
    loop(0, NN, lambda n: v_c(n).start())
    w_e(NS).start()
    loop(0, NJ, lambda j: w_b(j).start())
    loop(0, NN, lambda n: v_b(n).start())
    start_all(small)
    wait_all(small)
    for one in small_far:
        one.wait_recv()

    def l_copies(g, i, slot):
        at = pl.multiple_of(g * M + i * LN, LN)
        return (
            pltpu.make_async_copy(tok.at[pl.ds(pl.multiple_of(row0 + at, LN), LN)], lbuf.at[slot, 0], lsem.at[slot, 0]),
            pltpu.make_async_copy(toth.at[pl.ds(at, LN)], lbuf.at[slot, 1], lsem.at[slot, 1]),
        )

    def layer_norm(g):
        steps = M // LN
        t_dir(2 * g).wait_recv()
        start_all(l_copies(g, 0, 0))

        def rows(i):
            slot = i % 2

            @pl.when(i == steps // 2 - 1)
            def _():
                t_dir(2 * g + 1).wait_recv()

            @pl.when(i + 1 < steps)
            def _():
                start_all(l_copies(g, i + 1, 1 - slot))
            wait_all(l_copies(g, i, slot))
            step = 64

            def part(k):
                at = pl.ds(pl.multiple_of(k * step, step), step)
                a, b = lbuf[slot, 0, at].astype(F32), lbuf[slot, 1, at].astype(F32)
                mean = (jnp.sum(a, -1, keepdims=True) + jnp.sum(b, -1, keepdims=True)) * (0.5 / WID)
                a, b = a - mean, b - mean
                var = (jnp.sum(a * a, -1, keepdims=True) + jnp.sum(b * b, -1, keepdims=True)) * (0.5 / WID)
                inv = lax.rsqrt(var + EPS)
                to = pl.ds(pl.multiple_of(i * LN + k * step, step), step)
                zj[g % 2, to, :WID] = (a * inv * sc[0]).astype(BF16)
                zj[g % 2, to, WID:2 * WID] = (b * inv * sc[1]).astype(BF16)
            loop(0, LN // step, part)
        loop(0, steps, rows)

    def w1_copies(slot, top, bottom):
        return (
            pltpu.make_async_copy(top, wbuf.at[slot, :WID], w1sem.at[slot, 0]),
            pltpu.make_async_copy(bottom, wbuf.at[slot, WID:2 * WID], w1sem.at[slot, 1]),
        )

    def fetch1(p, t):
        j, s = tile_of(t)
        slot = t % 2

        @pl.when(p == 0)
        def _():
            @pl.when(s == 0)
            def _():
                w_c(j).wait_recv()
                w_d(j).start()
                w_f(j).start()

                @pl.when((j == 1) | (j == 3))
                def _():
                    w_e((j + 9) // 2).start()

                @pl.when(j == NJ - 1)
                def _():
                    v_e(0).start()
                    v_e(1).start()

            @pl.when(s == 1)
            def _():
                w_b(j).wait_recv()
                w_d(j).wait_recv()

            @pl.when(s == 2)
            def _():
                w_e(j).wait_recv()
                w_g(j).start()
                w_f(j).wait_recv()
                w_h(j).start()

            @pl.when(s == 3)
            def _():
                w_g(j).wait_recv()
                w_h(j).wait_recv()

        @pl.when(s == 0)
        def _():
            start_all(w1_copies(slot, w_in.at[:, in_col(j, y)], w1b.at[0, :, tile(j)]))

        @pl.when(s > 0)
        def _():
            start_all(w1_copies(slot, w1t.at[s - 1, :, tile(j)], w1b.at[s, :, tile(j)]))

    def h_store(slot, dst):
        return pltpu.make_async_copy(ptile.at[slot], dst, psem.at[slot])

    def h_done(slot):
        h_store(slot, pb.at[rows_of(0), tile(0)]).wait()

    def w1_tile(p, t):
        j, s = tile_of(t)
        wait_all(w1_copies(t % 2, w1t.at[0, :, tile(0)], w1b.at[0, :, tile(0)]))

        def one(gl):
            g = 2 * p + gl

            def project():
                h = (jnp.dot(zj[gl, :, :WID], wbuf[t % 2, :WID], preferred_element_type=F32)
                     + jnp.dot(zj[gl, :, WID:2 * WID], wbuf[t % 2, WID:2 * WID], preferred_element_type=F32))
                return h.astype(BF16)

            @pl.when((t > 0) & (t != 24))
            def _():
                h_done(gl)

            @pl.when(j < 2)
            def _():
                h = project().astype(F32)
                gain = gains[j]
                for k in range(2):
                    part = h[:, k * DH:(k + 1) * DH]
                    part = part - jnp.mean(part, -1, keepdims=True)
                    var = jnp.mean(part * part, -1, keepdims=True)
                    ptile[gl, :, k * DH:(k + 1) * DH] = (part * lax.rsqrt(var + EPS) * gain).astype(BF16)

            @pl.when(j == 2)
            def _():
                ptile[gl] = project()

            @pl.when(j > 2)
            def _():
                h = project().astype(F32) + ub[s, :, tile(j - 3)]
                ptile[gl] = (0.5 * h * (1.0 + lax.erf(h * 0.7071067811865476))).astype(BF16)

            @pl.when(j <= 2)
            def _():
                h_store(gl, qkv.at[j, s, rows_of(g)]).start()

            @pl.when(j > 2)
            def _():
                h_store(gl, jb.at[rows_of(g), pl.ds(pl.multiple_of(s * JB + (j - 2) * TN, TN), TN)]).start()
        loop(0, 2, one)

    def a_loads(p, w, slot):
        g, s = 2 * p + w // NS, w % NS
        return [pltpu.make_async_copy(qkv.at[i, s, rows_of(g)], abuf.at[slot, i], asem.at[slot, i]) for i in range(3)]

    def a_store(p, w, slot):
        g, s = 2 * p + w // NS, w % NS
        return h_store(slot, jb.at[rows_of(g), pl.ds(pl.multiple_of(s * JB, TN), TN)])

    def attention(p):
        units = 2 * NS
        start_all(a_loads(p, 0, 0))

        def unit(w):
            slot = w % 2

            @pl.when(w + 1 < units)
            def _():
                start_all(a_loads(p, w + 1, 1 - slot))
            wait_all(a_loads(p, w, slot))

            @pl.when(w >= 2)
            def _():
                a_store(p, w - 2, slot).wait()

            def images(i):
                for ii in range(2):
                    at = pl.ds(pl.multiple_of((2 * i + ii) * SEQ, SEQ), SEQ)
                    for k in range(2):
                        cols = slice(k * DH, (k + 1) * DH)
                        q, kk, v = abuf[slot, 0, at, cols], abuf[slot, 1, at, cols], abuf[slot, 2, at, cols]
                        lg = lax.dot_general(q, kk, (((1,), (1,)), ((), ())), preferred_element_type=F32) * (DH ** -0.5)
                        e = jnp.exp(lg - jnp.max(lg, -1, keepdims=True))
                        prob = (e / jnp.sum(e, -1, keepdims=True)).astype(BF16)
                        ptile[slot, at, cols] = jnp.dot(prob, v, preferred_element_type=F32).astype(BF16)
            loop(0, M // SEQ // 2, images)
            a_store(p, w, slot).start()
        loop(0, units, unit)
        a_store(p, units - 2, 0).wait()
        a_store(p, units - 1, 1).wait()

    def w2_slot(m, half):
        return 2 * ((m + 1) % 2) + half

    def w2_dst(m, s):
        return wbuf.at[w2_slot(m, s // 2), pl.ds((s % 2) * JB, JB)]

    def fetch2(m):
        n = m // 2
        e = m % 2

        @pl.when(e == 0)
        def _():
            v_d(n).wait_recv()
            v_h(n).wait_recv()
            for s in range(NS):
                pltpu.make_async_copy(w2n.at[s, :, tile(n)], w2_dst(m, s), w2sem.at[e, s]).start()

        @pl.when(e == 1)
        def _():
            v_b(n).wait_recv()
            v_g(n).wait_recv()
            for p in range(2):
                to = wbuf.at[w2_slot(m, 0), PART_ROWS[p]]
                pltpu.make_async_copy(w_out.at[out_row(p, y), tile(n)], to, w2sem.at[e, 4 * p]).start()
            for s in range(1, NS):
                pltpu.make_async_copy(w2y.at[s - 1, :, tile(n)], w2_dst(m, s), w2sem.at[e, s]).start()

    def arrive2(m):
        e = m % 2

        @pl.when(e == 0)
        def _():
            for s in range(NS):
                pltpu.make_async_copy(w2n.at[s, :, tile(0)], w2_dst(m, s), w2sem.at[e, s]).wait()

        @pl.when(e == 1)
        def _():
            for p in range(2):
                to = wbuf.at[w2_slot(m, 0), PART_ROWS[p]]
                pltpu.make_async_copy(w2n.at[0, PART_ROWS[p], tile(0)], to, w2sem.at[e, 4 * p]).wait()
            for s in range(1, NS):
                pltpu.make_async_copy(w2n.at[s, :, tile(0)], w2_dst(m, s), w2sem.at[e, s]).wait()

    def hand_c(n):
        v_c(n).wait_recv()
        v_d(n).start()
        v_f(n).start()

    def hand_e(n):
        v_e(n).wait_recv()
        v_g(n).start()

    def hand_f(n):
        v_f(n).wait_recv()
        v_h(n).start()

    hands = {5: [lambda: hand_c(0)], 8: [lambda: hand_e(0)], 11: [lambda: hand_c(1), lambda: v_e(2).start()],
             14: [lambda: hand_e(1), lambda: hand_f(0)], 17: [lambda: hand_c(2), lambda: v_e(3).start()],
             20: [lambda: hand_f(1)], 23: [lambda: hand_c(3)]}

    def w1_pass(p):
        layer_norm(2 * p)
        layer_norm(2 * p + 1)

        @pl.when(p == 0)
        def _():
            fetch1(p, 0)

        def step(t):
            @pl.when(t == 24)
            def _():
                h_done(0)
                h_done(1)
                attention(p)

            def fetch_next():
                @pl.when(t + 1 < NT)
                def _():
                    fetch1(p, t + 1)

                @pl.when((t + 1 == NT) & (p == 0))
                def _():
                    fetch1(1, 0)

                @pl.when((t + 1 == NT) & (p == 1))
                def _():
                    fetch2(0)

            @pl.when(p == 1)
            def _():
                fetch_next()
            w1_tile(p, t)

            @pl.when(p == 0)
            def _():
                fetch_next()

            for at, todo in hands.items():
                @pl.when((p == 1) & (t == at))
                def _(todo=todo):
                    for one in todo:
                        one()
        loop(0, NT, step)
        h_done(0)
        h_done(1)
    loop(0, 2, w1_pass)

    def load(e, i, src):
        return pltpu.make_async_copy(src, sv.at[e, i], vsem.at[e, i])

    def fin_loads(k, n, e):
        at = (part_rows(k), tile(n))
        return [load(e, 0, pa.at[at]), load(e, 1, ry.at[at]), load(e, 2, tok.at[own_out(k), tile(n)])]

    def fin_store(k, n, e):
        return pltpu.make_async_copy(sv.at[e, 3], out.at[own_out(k), tile(n)], vsem.at[e, 3])

    def tail_store(k, e):
        return pltpu.make_async_copy(sv.at[e, 3], tail.at[part_rows(k - NL)], vsem.at[e, 4])

    def is_tail(k, n):
        return (n == NN - 1) & (k >= NL)

    def fin_load(k, n, e):
        @pl.when(k % 2 == 0)
        def _():
            o_y(k // 2, n).wait_recv()
        start_all(fin_loads(k, n, e))

    def fin_do(k, n, e):
        wait_all(fin_loads(k, n, e))
        total = sv[e, 0].astype(F32) + sv[e, 1].astype(F32) + (ob[0, :, tile(n)] + ob[1, :, tile(n)]) + sv[e, 2].astype(F32)
        sv[e, 3] = total.astype(BF16)
        fin_store(k, n, e).start()

        @pl.when(is_tail(k, n))
        def _():
            tail_store(k, e).start()

    def fin_send(k, n, e):
        fin_store(k, n, e).wait()

        @pl.when(is_tail(k, n))
        def _():
            tail_store(k, e).wait()

        @pl.when(jnp.logical_not(is_tail(k, n)))
        def _():
            o_x(k, n).start()
        o_c(k, n).start()

    def hand_out(k, n):
        o_x(k, n).wait_recv()
        o_f(k, n).start()

    STEPS = 2 * NN * NK

    def service(v):
        f = v - 12
        n, i = f // 16, f % 16

        @pl.when((f >= 0) & (i >= 2) & (i < NK + 2))
        def _():
            fin_send(i - 2, n, v % 2)

        @pl.when((f >= 0) & (i < NK))
        def _():
            fin_load(i, n, v % 2)

        @pl.when((f >= 0) & (i >= 1) & (i < NK + 1))
        def _():
            fin_do(i - 1, n, (v + 1) % 2)

        for n, at in enumerate((33, 49)):
            @pl.when((v >= at) & (v < at + NK))
            def _(n=n, at=at):
                hand_out(v - at, n)

    def j_copy(v):
        g, half = (v % 8) // 2, v % 2
        src = jb.at[rows_of(g), pl.ds(pl.multiple_of(half * KH, KH), KH)]
        return pltpu.make_async_copy(src, zj.at[half], jsem.at[half])

    def p_copy(m, g):
        n, slot = m // 2, g % 2
        return n, lambda ref: pltpu.make_async_copy(ptile.at[slot], ref.at[rows_of(g), tile(n)], psem.at[slot])

    def p_start(m, g):
        n, to = p_copy(m, g)

        @pl.when(m % 2 == 0)
        def _():
            to(pb).start()

        @pl.when(m % 2 == 1)
        def _():
            to(pa).start()

    def p_finish(m, g):
        n, to = p_copy(m, g)

        @pl.when(m % 2 == 0)
        def _():
            to(pb).wait()
            o_y(g, n).start()

        @pl.when(m % 2 == 1)
        def _():
            to(pa).wait()

    j_copy(0).start()

    def w2_tile(m):
        for at, todo in enumerate((lambda: hand_e(2), lambda: hand_f(2), lambda: hand_e(3), lambda: hand_f(3))):
            @pl.when(m == at)
            def _(todo=todo):
                todo()

        @pl.when(m + 1 < 2 * NN)
        def _():
            fetch2(m + 1)
        arrive2(m)

        def one(g):
            v = m * 2 * GROUPS + 2 * g
            j_copy(v + 1).start()
            j_copy(v).wait()
            acc[...] = jnp.dot(zj[0], wbuf[w2_slot(m, 0)], preferred_element_type=F32)
            service(v)

            @pl.when(v + 2 < STEPS)
            def _():
                j_copy(v + 2).start()
            j_copy(v + 1).wait()
            ptile[g % 2] = (acc[...] + jnp.dot(zj[1], wbuf[w2_slot(m, 1)], preferred_element_type=F32)).astype(BF16)
            p_start(m, g)

            @pl.when(g > 0)
            def _():
                p_finish(m, g - 1)
            service(v + 1)
        loop(0, GROUPS, one)
        p_finish(m, GROUPS - 1)
    loop(0, 2 * NN, w2_tile)

    loop(STEPS, STEPS + 6, service)
    loop(0, NK, lambda k: hand_out(k, 2))

    for one in small_far:
        one.wait_send()
    remote(toth, toth, t_s, t_s, dev_y).wait_send()
    for kind in range(C + NJ):
        remote(bots[OWN], bots[OWN], w_s.at[kind], w_s.at[kind], dev_y).wait_send()
    for kind in range(NS):
        remote(theirs[OWN], theirs[OWN], d_s.at[kind], d_s.at[kind], dev_y).wait_send()
    for kind in range(NS - 1):
        remote(theirs[OWN], theirs[OWN], e_s.at[kind], e_s.at[kind], dev_y).wait_send()
    remote(pb, pb, y_s, y_s, dev_y).wait_send()
    mine_out = out.at[pl.ds(pl.multiple_of(row0, ROWS), ROWS)]
    near_out = remote(mine_out, mine_out, o_s.at[0], o_r.at[0], dev_c)
    near_out.wait_send()
    near_out.wait_recv()

    loop(0, NK - NL, lambda k: hand_out(k, NN - 1))
    sent = out.at[pl.ds(pl.multiple_of(row0, ROWS), ROWS - (NK - NL) * HALF // NN)]
    remote(sent, sent, x_s, x_s, dev_x).wait_send()
    far_out = remote(sent, sent, o_s.at[1], o_r.at[1], dev_c)
    far_out.wait_send()
    far_out.wait_recv()


def copy_kernel(src, dst, buf, sem):
    slots = buf.shape[0]
    x = lax.axis_index("mx") // 2

    def moves(i):
        first = (x + i // (2 * NK)) % 2
        rows = pl.ds(pl.multiple_of(first * 2 * ROWS + (i % (2 * NK)) * HALF, HALF), HALF)
        late = i >= 2 * NK and i % NK >= NL
        cols = pl.ds(0, WID - TN if late else WID)
        k = i % slots
        return (pltpu.make_async_copy(src.at[rows, cols], buf.at[k, :, cols], sem.at[0, k]),
                pltpu.make_async_copy(buf.at[k, :, cols], dst.at[rows, cols], sem.at[1, k]))
    every = [moves(i) for i in range(4 * NK)]
    ahead = slots // 2
    for i in range(4 * NK + ahead):
        if i < 4 * NK:
            if i >= slots:
                every[i - slots][1].wait()
            every[i][0].start()
        if i >= ahead:
            every[i - ahead][0].wait()
            every[i - ahead][1].start()
    for i in range(4 * NK - slots, 4 * NK):
        every[i][1].wait()


def tail_kernel(base, far, farther, out, buf, sem):
    mi = lax.axis_index("mx")
    x, c = mi // 2, mi % 2
    moves = []
    for i, (ref, cc) in enumerate(((far, c), (farther, 1 - c))):
        at = pl.multiple_of((2 * (1 - x) + cc) * ROWS + NL * HALF, HALF)
        to = out.at[pl.ds(at, (NK - NL) * HALF), pl.ds((NN - 1) * TN, TN)]
        moves.append((pltpu.make_async_copy(ref, buf.at[i], sem.at[0, i]), pltpu.make_async_copy(buf.at[i], to, sem.at[1, i])))
    start_all(load for load, _ in moves)
    for load, store in moves:
        load.wait()
        store.start()
    wait_all(store for _, store in moves)


def solution(mesh):
    hbm = pl.BlockSpec(memory_space=pltpu.HBM)

    def dma(*shape):
        return pltpu.SemaphoreType.DMA(shape)

    def local_layer(tokens, ln_scale, w_in, mlp_bias, q_scale, k_scale, w_out, attn_out_bias, mlp_out_bias):
        tok = tokens.reshape(-1, WID)
        vec, at = None, 0
        for v in (ln_scale, mlp_bias, q_scale, k_scale, attn_out_bias, mlp_out_bias):
            wide = jnp.pad(v.astype(F32), (at, VEC - at - v.size), constant_values=-jnp.inf)
            vec = wide if vec is None else jnp.maximum(vec, wide)
            at += v.size
        of = lambda *shape: jax.ShapeDtypeStruct(shape, BF16)
        shapes = [of(*tok.shape), of((NK - NL) * HALF, TN), of(ROWS, WID), of(3, WID, NJ * TN), of(4, WID, NJ * TN), of(3, JB, WID), of(4, JB, WID),
                  of(3, NS, ROWS, TN), of(ROWS, NS * JB), of(ROWS, WID), of(ROWS, WID), of(ROWS, WID)]
        flops = 2 * ROWS * (2 * WID * NT * TN + NS * JB * 2 * WID)
        pairs = [(), (NK,), (7,), (7, NJ), (3,), (3, NN), (NS,), (NS, NN), (), (GROUPS, NN), (), (NK, NN), (2,), (2,), (NS,), (NS,)]
        res = pl.pallas_call(
            kernel,
            out_shape=shapes,
            in_specs=[hbm] * 4,
            out_specs=[hbm] * len(shapes),
            scratch_shapes=[
                pltpu.VMEM((2, M, KH), BF16),
                pltpu.VMEM((4, KH, TN), BF16),
                pltpu.VMEM((2, M, TN), BF16),
                pltpu.VMEM((M, TN), F32),
                pltpu.VMEM((2, 3, M, TN), BF16),
                pltpu.VMEM((2, 4, HALF, TN), BF16),
                pltpu.VMEM((2, 2, LN, WID), BF16),
                pltpu.VMEM((2, 1, WID), F32),
                pltpu.VMEM((NS, 1, UNITS // 2), F32),
                pltpu.VMEM((2, 1, DH), F32),
                pltpu.VMEM((2, 1, WID), F32),
                dma(2, 2), dma(2, 5), dma(2), dma(2), dma(2, 3), dma(2, 5), dma(2, 2), dma(6),
            ] + [dma(*shape) for shape in pairs],
            compiler_params=pltpu.CompilerParams(collective_id=0, has_side_effects=True, vmem_limit_bytes=63 * 2**20),
            cost_estimate=pl.CostEstimate(flops=flops, bytes_accessed=2**30, transcendentals=0),
            name="layer",
        )(tok, w_in, w_out, vec.reshape(1, VEC))
        base, own = res[0], res[1]
        far = lax.ppermute(own, 'mx', [(0, 2), (1, 3), (2, 0), (3, 1)])
        base = pl.pallas_call(
            copy_kernel,
            out_shape=of(*tok.shape),
            in_specs=[hbm],
            out_specs=hbm,
            scratch_shapes=[pltpu.VMEM((16, HALF, WID), BF16), dma(2, 16)],
            compiler_params=pltpu.CompilerParams(vmem_limit_bytes=40 * 2**20),
            cost_estimate=pl.CostEstimate(flops=2 * 10**10, bytes_accessed=4 * tok.size, transcendentals=0),
            name="place",
        )(base)
        far, base = lax.optimization_barrier((far, base))
        farther = lax.ppermute(far, 'mx', [(0, 1), (1, 0), (2, 3), (3, 2)])
        out = pl.pallas_call(
            tail_kernel,
            out_shape=of(*tok.shape),
            in_specs=[hbm] * 3,
            out_specs=hbm,
            input_output_aliases={0: 0},
            scratch_shapes=[pltpu.VMEM((2, (NK - NL) * HALF, TN), BF16), dma(2, 2)],
            name="place_last",
        )(base, far, farther)
        return out.reshape(tokens.shape)

    specs_in = (P('dp', None, 'my'), P('my'), P('my', 'mx'), P('mx'), P(), P(), P('mx', 'my'), P('my'), P('my'))
    return jax.shard_map(local_layer, mesh=mesh, in_specs=specs_in, out_specs=P('dp', None, 'my'), check_vma=False)
```

```python
import functools

import jax
import jax.numpy as jnp
from jax import lax
from jax.experimental import pallas as pl
from jax.experimental.pallas import tpu as pltpu
from jax.sharding import PartitionSpec as P

MESH = pl.DeviceIdType.MESH
F32, BF16 = jnp.float32, jnp.bfloat16

SEQ, DH, WID = 256, 256, 2048
M, GROUPS = 1024, 4
ROWS = M * GROUPS
HALF = M // 2
TN = 512
QKV, UNITS = 1024, 4096
NS = 4
NJ = 7
NT = NS * NJ
NN = WID // TN
JB = 5 * TN
KH = 2 * JB
VEC = 3 * WID + UNITS + 2 * DH
LN = 128
EPS = 1e-6
NK = 2 * GROUPS
NL = NK // 2


def in_col(j, side):
    mlp = (j + 1) // 4
    at = (1 - mlp) * (QKV * j + (QKV // 2) * side) + mlp * (3 * QKV + (UNITS // 2) * side + TN * (j - 3))
    return pl.ds(pl.multiple_of(at, TN), TN)


def out_row(part, side):
    if part == 0:
        return pl.ds(pl.multiple_of((QKV // 2) * side, QKV // 2), TN)
    return pl.ds(pl.multiple_of(QKV + (UNITS // 2) * side, QKV), UNITS // 2)


PART_ROWS = (pl.ds(0, TN), pl.ds(TN, JB - TN))


def tile(n):
    return pl.ds(pl.multiple_of(n * TN, TN), TN)


def rows_of(g):
    return pl.ds(pl.multiple_of(g * M, M), M)


def tile_of(t):
    a, b = (t + 24) // 28, t // 24
    j = (1 - a) * (t // 2) + (a - b) * (t // 4 + 1 - 2 * ((t % 4) // 2)) + b * (t // 2 - 7)
    s = (1 - a) * (t % 2) + (a - b) * (t % 4) + b * (2 + t % 2)
    return j, s


def loop(lo, hi, body):
    def run(i, carry):
        body(i)
        return carry
    lax.fori_loop(lo, hi, run, 0)


def start_all(copies):
    for one in copies:
        one.start()


def wait_all(copies):
    for one in copies:
        one.wait()


def kernel(tok, w_in, w_out, vec,
           out, tail, toth, w1t, w1b, w2y, w2n, qkv, jb, pa, pb, ry,
           zj, wbuf, ptile, acc, abuf, sv, lbuf, sc, ub, gains, ob,
           w1sem, w2sem, jsem, psem, asem, vsem, lsem, csem,
           t_s, t_r, w_s, w_r, e_s, e_r, d_s, d_r, y_s, y_r, x_s, x_r, o_s, o_r, m_s, m_r):
    y = lax.axis_index("my")
    mi = lax.axis_index("mx")
    x, c = mi // 2, mi % 2
    dev_y = {"my": 1 - y, "mx": mi}
    dev_x = {"my": y, "mx": 2 * (1 - x) + c}
    dev_c = {"my": y, "mx": 2 * x + 1 - c}
    dev_d = {"my": y, "mx": 2 * (1 - x) + 1 - c}
    row0 = (2 * x + c) * ROWS
    row0_x = (2 * (1 - x) + c) * ROWS

    barrier = pltpu.get_barrier_semaphore()
    for dev in (dev_y, dev_x, dev_c, dev_d):
        pl.semaphore_signal(barrier, inc=1, device_id=dev, device_id_type=MESH)
    pl.semaphore_wait(barrier, 4)

    def remote(src, dst, ss, rs, dev):
        return pltpu.make_async_remote_copy(src_ref=src, dst_ref=dst, send_sem=ss, recv_sem=rs, device_id=dev, device_id_type=MESH)

    def t_dir(k):
        src = tok.at[pl.ds(pl.multiple_of(row0 + k * HALF, HALF), HALF)]
        return remote(src, toth.at[pl.ds(pl.multiple_of(k * HALF, HALF), HALF)], t_s, t_r.at[k], dev_y)

    C, B, D, E, F, G, H = range(7)

    def w_own(kind, j, side, dst, dev):
        return remote(w_in.at[:, in_col(j, side)], dst.at[:, tile(j)], w_s.at[kind], w_r.at[kind, j], dev)

    def w_pass(kind, j, src, dst, dev):
        return remote(src.at[:, tile(j)], dst.at[:, tile(j)], w_s.at[kind], w_r.at[kind, j], dev)

    tops = [None] + [w1t.at[i] for i in range(NS - 1)]
    bots = [w1b.at[i] for i in range(NS)]
    OWN, CORE, FAR, FAR_CORE = range(NS)
    w_c = lambda j: w_own(C, j, 1 - y, bots[OWN], dev_y)
    w_b = lambda j: w_own(B, j, y, tops[CORE], dev_c)
    w_d = lambda j: w_pass(D, j, bots[OWN], bots[CORE], dev_c)
    w_e = lambda j: w_own(E, j, y, tops[FAR], dev_x)
    w_f = lambda j: w_pass(F, j, bots[OWN], bots[FAR], dev_x)
    w_g = lambda j: w_pass(G, j, tops[FAR], tops[FAR_CORE], dev_c)
    w_h = lambda j: w_pass(H, j, bots[FAR], bots[FAR_CORE], dev_c)

    class Two:
        def __init__(self, kind, n, side, dst, dev):
            self.copies = [remote(w_out.at[out_row(p, side), tile(n)], dst.at[rows, tile(n)], e_s.at[kind], e_r.at[kind, n], dev)
                           for p, rows in enumerate(PART_ROWS)]
            self.both = remote(dst.at[:, tile(n)], dst.at[:, tile(n)], e_s.at[kind], e_r.at[kind, n], dev)

        def start(self):
            start_all(self.copies)

        def wait_recv(self):
            self.both.wait_recv()

    def v_pass(kind, n, src, dst, dev):
        return remote(src.at[:, tile(n)], dst.at[:, tile(n)], d_s.at[kind], d_r.at[kind, n], dev)

    mine = [None] + [w2y.at[i] for i in range(NS - 1)]
    theirs = [w2n.at[i] for i in range(NS)]
    v_c = lambda n: Two(C, n, 1 - y, theirs[OWN], dev_y)
    v_b = lambda n: Two(B, n, y, mine[CORE], dev_c)
    v_e = lambda n: Two(D, n, y, mine[FAR], dev_x)
    v_d = lambda n: v_pass(C, n, theirs[OWN], theirs[CORE], dev_c)
    v_f = lambda n: v_pass(B, n, theirs[OWN], theirs[FAR], dev_x)
    v_g = lambda n: v_pass(D, n, mine[FAR], mine[FAR_CORE], dev_c)
    v_h = lambda n: v_pass(E, n, theirs[FAR], theirs[FAR_CORE], dev_c)

    def o_y(g, n):
        return remote(pb.at[rows_of(g), tile(n)], ry.at[rows_of(g), tile(n)], y_s, y_r.at[g, n], dev_y)

    def part_rows(k):
        return pl.ds(pl.multiple_of(k * HALF, HALF), HALF)

    def own_out(k):
        return pl.ds(pl.multiple_of(row0 + k * HALF, HALF), HALF)

    def o_x(k, n):
        at = out.at[own_out(k), tile(n)]
        return remote(at, at, x_s, x_r.at[k, n], dev_x)

    def o_c(k, n):
        at = out.at[own_out(k), tile(n)]
        return remote(at, at, o_s.at[0], o_r.at[0], dev_c)

    def o_f(k, n):
        at = out.at[pl.ds(pl.multiple_of(row0_x + k * HALF, HALF), HALF), tile(n)]
        return remote(at, at, o_s.at[1], o_r.at[1], dev_c)

    lns = vec.at[:, pl.ds(0, WID)]
    my_units = vec.at[:, pl.ds(pl.multiple_of(WID + y * (UNITS // 2), UNITS // 2), UNITS // 2)]
    at = WID + UNITS
    small_far = [remote(src, dst, m_s.at[i], m_r.at[i], dev) for i, (src, dst, dev) in enumerate((
        (lns, sc.at[1], dev_y), (my_units, ub.at[CORE], dev_c), (my_units, ub.at[FAR], dev_x), (my_units, ub.at[FAR_CORE], dev_d)))]
    small = [pltpu.make_async_copy(src, dst, csem.at[i]) for i, (src, dst) in enumerate((
        (lns, sc.at[0]), (my_units, ub.at[OWN]), (vec.at[:, pl.ds(at, DH)], gains.at[0]),
        (vec.at[:, pl.ds(at + DH, DH)], gains.at[1]), (vec.at[:, pl.ds(at + 2 * DH, WID)], ob.at[0]),
        (vec.at[:, pl.ds(at + 2 * DH + WID, WID)], ob.at[1])))]

    loop(0, NS, lambda j: w_e(j).start())
    start_all(small_far)
    loop(0, NS, lambda k: t_dir(k).start())
    loop(0, NJ, lambda j: w_c(j).start())
    loop(NS, NK, lambda k: t_dir(k).start())
    loop(0, NN, lambda n: v_c(n).start())
    w_e(NS).start()
    w_e(NS + 1).start()
    loop(0, NJ, lambda j: w_b(j).start())
    loop(0, NN, lambda n: v_b(n).start())
    start_all(small)
    wait_all(small)
    for one in small_far:
        one.wait_recv()

    def l_copies(g, i, slot):
        at = pl.multiple_of(g * M + i * LN, LN)
        return (
            pltpu.make_async_copy(tok.at[pl.ds(pl.multiple_of(row0 + at, LN), LN)], lbuf.at[slot, 0], lsem.at[slot, 0]),
            pltpu.make_async_copy(toth.at[pl.ds(at, LN)], lbuf.at[slot, 1], lsem.at[slot, 1]),
        )

    def layer_norm(g):
        steps = M // LN
        t_dir(2 * g).wait_recv()
        start_all(l_copies(g, 0, 0))

        def rows(i):
            slot = i % 2

            @pl.when(i == steps // 2 - 1)
            def _():
                t_dir(2 * g + 1).wait_recv()

            @pl.when(i + 1 < steps)
            def _():
                start_all(l_copies(g, i + 1, 1 - slot))
            wait_all(l_copies(g, i, slot))
            step = 64

            def part(k):
                at = pl.ds(pl.multiple_of(k * step, step), step)
                a, b = lbuf[slot, 0, at].astype(F32), lbuf[slot, 1, at].astype(F32)
                mean = (jnp.sum(a, -1, keepdims=True) + jnp.sum(b, -1, keepdims=True)) * (0.5 / WID)
                a, b = a - mean, b - mean
                var = (jnp.sum(a * a, -1, keepdims=True) + jnp.sum(b * b, -1, keepdims=True)) * (0.5 / WID)
                inv = lax.rsqrt(var + EPS)
                to = pl.ds(pl.multiple_of(i * LN + k * step, step), step)
                zj[g % 2, to, :WID] = (a * inv * sc[0]).astype(BF16)
                zj[g % 2, to, WID:2 * WID] = (b * inv * sc[1]).astype(BF16)
            loop(0, LN // step, part)
        loop(0, steps, rows)

    def w1_copies(slot, top, bottom):
        return (
            pltpu.make_async_copy(top, wbuf.at[slot, :WID], w1sem.at[slot, 0]),
            pltpu.make_async_copy(bottom, wbuf.at[slot, WID:2 * WID], w1sem.at[slot, 1]),
        )

    def fetch1(p, t):
        j, s = tile_of(t)
        slot = t % 2

        @pl.when(p == 0)
        def _():
            @pl.when(s == 0)
            def _():
                w_c(j).wait_recv()
                w_d(j).start()
                w_f(j).start()

                @pl.when(j == 2)
                def _():
                    w_e(NJ - 1).start()

                @pl.when(j == NJ - 1)
                def _():
                    v_e(0).start()
                    v_e(1).start()

            @pl.when(s == 1)
            def _():
                w_b(j).wait_recv()
                w_d(j).wait_recv()

            @pl.when(s == 2)
            def _():
                w_e(j).wait_recv()
                w_g(j).start()
                w_f(j).wait_recv()
                w_h(j).start()

            @pl.when(s == 3)
            def _():
                w_g(j).wait_recv()
                w_h(j).wait_recv()

        @pl.when(s == 0)
        def _():
            start_all(w1_copies(slot, w_in.at[:, in_col(j, y)], w1b.at[0, :, tile(j)]))

        @pl.when(s > 0)
        def _():
            start_all(w1_copies(slot, w1t.at[s - 1, :, tile(j)], w1b.at[s, :, tile(j)]))

    def h_store(slot, dst):
        return pltpu.make_async_copy(ptile.at[slot], dst, psem.at[slot])

    def h_done(slot):
        h_store(slot, pb.at[rows_of(0), tile(0)]).wait()

    def w1_tile(p, t):
        j, s = tile_of(t)
        wait_all(w1_copies(t % 2, w1t.at[0, :, tile(0)], w1b.at[0, :, tile(0)]))

        def one(gl):
            g = 2 * p + gl

            def project():
                h = (jnp.dot(zj[gl, :, :WID], wbuf[t % 2, :WID], preferred_element_type=F32)
                     + jnp.dot(zj[gl, :, WID:2 * WID], wbuf[t % 2, WID:2 * WID], preferred_element_type=F32))
                return h.astype(BF16)

            @pl.when((t > 0) & (t != 24))
            def _():
                h_done(gl)

            @pl.when(j < 2)
            def _():
                h = project().astype(F32)
                gain = gains[j]
                for k in range(2):
                    part = h[:, k * DH:(k + 1) * DH]
                    part = part - jnp.mean(part, -1, keepdims=True)
                    var = jnp.mean(part * part, -1, keepdims=True)
                    ptile[gl, :, k * DH:(k + 1) * DH] = (part * lax.rsqrt(var + EPS) * gain).astype(BF16)

            @pl.when(j == 2)
            def _():
                ptile[gl] = project()

            @pl.when(j > 2)
            def _():
                h = project().astype(F32) + ub[s, :, tile(j - 3)]
                ptile[gl] = (0.5 * h * (1.0 + lax.erf(h * 0.7071067811865476))).astype(BF16)

            @pl.when(j <= 2)
            def _():
                h_store(gl, qkv.at[j, s, rows_of(g)]).start()

            @pl.when(j > 2)
            def _():
                h_store(gl, jb.at[rows_of(g), pl.ds(pl.multiple_of(s * JB + (j - 2) * TN, TN), TN)]).start()
        loop(0, 2, one)

    def a_loads(p, w, slot):
        g, s = 2 * p + w // NS, w % NS
        return [pltpu.make_async_copy(qkv.at[i, s, rows_of(g)], abuf.at[slot, i], asem.at[slot, i]) for i in range(3)]

    def a_store(p, w, slot):
        g, s = 2 * p + w // NS, w % NS
        return h_store(slot, jb.at[rows_of(g), pl.ds(pl.multiple_of(s * JB, TN), TN)])

    def attention(p):
        units = 2 * NS
        start_all(a_loads(p, 0, 0))

        def unit(w):
            slot = w % 2

            @pl.when(w + 1 < units)
            def _():
                start_all(a_loads(p, w + 1, 1 - slot))
            wait_all(a_loads(p, w, slot))

            @pl.when(w >= 2)
            def _():
                a_store(p, w - 2, slot).wait()

            def images(i):
                for ii in range(2):
                    at = pl.ds(pl.multiple_of((2 * i + ii) * SEQ, SEQ), SEQ)
                    for k in range(2):
                        cols = slice(k * DH, (k + 1) * DH)
                        q, kk, v = abuf[slot, 0, at, cols], abuf[slot, 1, at, cols], abuf[slot, 2, at, cols]
                        lg = lax.dot_general(q, kk, (((1,), (1,)), ((), ())), preferred_element_type=F32) * (DH ** -0.5)
                        e = jnp.exp(lg - jnp.max(lg, -1, keepdims=True))
                        prob = (e / jnp.sum(e, -1, keepdims=True)).astype(BF16)
                        ptile[slot, at, cols] = jnp.dot(prob, v, preferred_element_type=F32).astype(BF16)
            loop(0, M // SEQ // 2, images)
            a_store(p, w, slot).start()
        loop(0, units, unit)
        a_store(p, units - 2, 0).wait()
        a_store(p, units - 1, 1).wait()

    def w2_slot(m, half):
        return 2 * ((m + 1) % 2) + half

    def w2_dst(m, s):
        return wbuf.at[w2_slot(m, s // 2), pl.ds((s % 2) * JB, JB)]

    def fetch2(m):
        n = m // 2
        e = m % 2

        @pl.when(e == 0)
        def _():
            v_d(n).wait_recv()
            v_h(n).wait_recv()
            for s in range(NS):
                pltpu.make_async_copy(w2n.at[s, :, tile(n)], w2_dst(m, s), w2sem.at[e, s]).start()

        @pl.when(e == 1)
        def _():
            v_b(n).wait_recv()
            v_g(n).wait_recv()
            for p in range(2):
                to = wbuf.at[w2_slot(m, 0), PART_ROWS[p]]
                pltpu.make_async_copy(w_out.at[out_row(p, y), tile(n)], to, w2sem.at[e, 4 * p]).start()
            for s in range(1, NS):
                pltpu.make_async_copy(w2y.at[s - 1, :, tile(n)], w2_dst(m, s), w2sem.at[e, s]).start()

    def arrive2(m):
        e = m % 2

        @pl.when(e == 0)
        def _():
            for s in range(NS):
                pltpu.make_async_copy(w2n.at[s, :, tile(0)], w2_dst(m, s), w2sem.at[e, s]).wait()

        @pl.when(e == 1)
        def _():
            for p in range(2):
                to = wbuf.at[w2_slot(m, 0), PART_ROWS[p]]
                pltpu.make_async_copy(w2n.at[0, PART_ROWS[p], tile(0)], to, w2sem.at[e, 4 * p]).wait()
            for s in range(1, NS):
                pltpu.make_async_copy(w2n.at[s, :, tile(0)], w2_dst(m, s), w2sem.at[e, s]).wait()

    def hand_c(n):
        v_c(n).wait_recv()
        v_d(n).start()
        v_f(n).start()

    def hand_e(n):
        v_e(n).wait_recv()
        v_g(n).start()

    def hand_f(n):
        v_f(n).wait_recv()
        v_h(n).start()

    hands = {5: [lambda: hand_c(0)], 8: [lambda: hand_e(0)], 11: [lambda: hand_c(1), lambda: v_e(2).start()],
             14: [lambda: hand_e(1), lambda: hand_f(0)], 17: [lambda: hand_c(2), lambda: v_e(3).start()],
             20: [lambda: hand_f(1)], 23: [lambda: hand_c(3)]}

    def w1_pass(p):
        layer_norm(2 * p)
        layer_norm(2 * p + 1)

        @pl.when(p == 0)
        def _():
            fetch1(p, 0)

        def step(t):
            @pl.when(t == 24)
            def _():
                h_done(0)
                h_done(1)
                attention(p)

            def fetch_next():
                @pl.when(t + 1 < NT)
                def _():
                    fetch1(p, t + 1)

                @pl.when((t + 1 == NT) & (p == 0))
                def _():
                    fetch1(1, 0)

                @pl.when((t + 1 == NT) & (p == 1))
                def _():
                    fetch2(0)

            @pl.when(p == 1)
            def _():
                fetch_next()
            w1_tile(p, t)

            @pl.when(p == 0)
            def _():
                fetch_next()

            for at, todo in hands.items():
                @pl.when((p == 1) & (t == at))
                def _(todo=todo):
                    for one in todo:
                        one()
        loop(0, NT, step)
        h_done(0)
        h_done(1)
    loop(0, 2, w1_pass)

    def load(e, i, src):
        return pltpu.make_async_copy(src, sv.at[e, i], vsem.at[e, i])

    def fin_loads(k, n, e):
        at = (part_rows(k), tile(n))
        return [load(e, 0, pa.at[at]), load(e, 1, ry.at[at]), load(e, 2, tok.at[own_out(k), tile(n)])]

    def fin_store(k, n, e):
        return pltpu.make_async_copy(sv.at[e, 3], out.at[own_out(k), tile(n)], vsem.at[e, 3])

    def tail_store(k, e):
        return pltpu.make_async_copy(sv.at[e, 3], tail.at[part_rows(k - NL)], vsem.at[e, 4])

    def is_tail(k, n):
        return (n == NN - 1) & (k >= NL)

    def fin_load(k, n, e):
        @pl.when(k % 2 == 0)
        def _():
            o_y(k // 2, n).wait_recv()
        start_all(fin_loads(k, n, e))

    def fin_do(k, n, e):
        wait_all(fin_loads(k, n, e))
        total = sv[e, 0].astype(F32) + sv[e, 1].astype(F32) + (ob[0, :, tile(n)] + ob[1, :, tile(n)]) + sv[e, 2].astype(F32)
        sv[e, 3] = total.astype(BF16)
        fin_store(k, n, e).start()

        @pl.when(is_tail(k, n))
        def _():
            tail_store(k, e).start()

    def fin_send(k, n, e):
        fin_store(k, n, e).wait()

        @pl.when(is_tail(k, n))
        def _():
            tail_store(k, e).wait()

        @pl.when(jnp.logical_not(is_tail(k, n)))
        def _():
            o_x(k, n).start()
        o_c(k, n).start()

    def hand_out(k, n):
        o_x(k, n).wait_recv()
        o_f(k, n).start()

    STEPS = 2 * NN * NK

    def service(v):
        f = v - 11
        n, i = f // 16, f % 16

        @pl.when((f >= 0) & (i >= 2) & (i < NK + 2))
        def _():
            fin_send(i - 2, n, v % 2)

        @pl.when((f >= 0) & (i < NK))
        def _():
            fin_load(i, n, v % 2)

        @pl.when((f >= 0) & (i >= 1) & (i < NK + 1))
        def _():
            fin_do(i - 1, n, (v + 1) % 2)

        for n, at in enumerate((33, 49)):
            @pl.when((v >= at) & (v < at + NK))
            def _(n=n, at=at):
                hand_out(v - at, n)

    def j_copy(v):
        g, half = (v % 8) // 2, v % 2
        src = jb.at[rows_of(g), pl.ds(pl.multiple_of(half * KH, KH), KH)]
        return pltpu.make_async_copy(src, zj.at[half], jsem.at[half])

    def p_copy(m, g):
        n, slot = m // 2, g % 2
        return n, lambda ref: pltpu.make_async_copy(ptile.at[slot], ref.at[rows_of(g), tile(n)], psem.at[slot])

    def p_start(m, g):
        n, to = p_copy(m, g)

        @pl.when(m % 2 == 0)
        def _():
            to(pb).start()

        @pl.when(m % 2 == 1)
        def _():
            to(pa).start()

    def p_finish(m, g):
        n, to = p_copy(m, g)

        @pl.when(m % 2 == 0)
        def _():
            to(pb).wait()
            o_y(g, n).start()

        @pl.when(m % 2 == 1)
        def _():
            to(pa).wait()

    j_copy(0).start()

    def w2_tile(m):
        for at, todo in enumerate((lambda: hand_e(2), lambda: hand_f(2), lambda: hand_e(3), lambda: hand_f(3))):
            @pl.when(m == at)
            def _(todo=todo):
                todo()

        @pl.when(m + 1 < 2 * NN)
        def _():
            fetch2(m + 1)
        arrive2(m)

        def one(g):
            v = m * 2 * GROUPS + 2 * g
            j_copy(v + 1).start()
            j_copy(v).wait()
            acc[...] = jnp.dot(zj[0], wbuf[w2_slot(m, 0)], preferred_element_type=F32)

            @pl.when(g > 0)
            def _():
                p_finish(m, g - 1)
            service(v)

            @pl.when(v + 2 < STEPS)
            def _():
                j_copy(v + 2).start()
            j_copy(v + 1).wait()
            ptile[g % 2] = (acc[...] + jnp.dot(zj[1], wbuf[w2_slot(m, 1)], preferred_element_type=F32)).astype(BF16)
            p_start(m, g)
            service(v + 1)
        loop(0, GROUPS, one)
        p_finish(m, GROUPS - 1)
    loop(0, 2 * NN, w2_tile)

    loop(STEPS, STEPS + 5, service)
    loop(0, NK, lambda k: hand_out(k, 2))

    for one in small_far:
        one.wait_send()
    remote(toth, toth, t_s, t_s, dev_y).wait_send()
    for kind in range(C + NJ):
        remote(bots[OWN], bots[OWN], w_s.at[kind], w_s.at[kind], dev_y).wait_send()
    for kind in range(NS):
        remote(theirs[OWN], theirs[OWN], d_s.at[kind], d_s.at[kind], dev_y).wait_send()
    for kind in range(NS - 1):
        remote(theirs[OWN], theirs[OWN], e_s.at[kind], e_s.at[kind], dev_y).wait_send()
    remote(pb, pb, y_s, y_s, dev_y).wait_send()
    mine_out = out.at[pl.ds(pl.multiple_of(row0, ROWS), ROWS)]
    near_out = remote(mine_out, mine_out, o_s.at[0], o_r.at[0], dev_c)
    near_out.wait_send()
    near_out.wait_recv()

    loop(0, NK - NL, lambda k: hand_out(k, NN - 1))
    sent = out.at[pl.ds(pl.multiple_of(row0, ROWS), ROWS - (NK - NL) * HALF // NN)]
    remote(sent, sent, x_s, x_s, dev_x).wait_send()
    far_out = remote(sent, sent, o_s.at[1], o_r.at[1], dev_c)
    far_out.wait_send()
    far_out.wait_recv()


def copy_kernel(src, dst, buf, sem):
    slots = buf.shape[0]
    x = lax.axis_index("mx") // 2

    def moves(i):
        first = (x + i // (2 * NK)) % 2
        rows = pl.ds(pl.multiple_of(first * 2 * ROWS + (i % (2 * NK)) * HALF, HALF), HALF)
        late = i >= 2 * NK and i % NK >= NL
        cols = pl.ds(0, WID - TN if late else WID)
        k = i % slots
        return (pltpu.make_async_copy(src.at[rows, cols], buf.at[k, :, cols], sem.at[0, k]),
                pltpu.make_async_copy(buf.at[k, :, cols], dst.at[rows, cols], sem.at[1, k]))
    every = [moves(i) for i in range(4 * NK)]
    ahead = slots // 2
    for i in range(4 * NK + ahead):
        if i < 4 * NK:
            if i >= slots:
                every[i - slots][1].wait()
            every[i][0].start()
        if i >= ahead:
            every[i - ahead][0].wait()
            every[i - ahead][1].start()
    for i in range(4 * NK - slots, 4 * NK):
        every[i][1].wait()


def tail_kernel(other, base, src, out, buf, sem):
    mi = lax.axis_index("mx")
    x, c = mi // 2, (mi + other) % 2
    at = pl.multiple_of((2 * (1 - x) + c) * ROWS + NL * HALF, HALF)
    rows = (NK - NL) * HALF // NN
    moves = []
    for i in range(NN):
        to = out.at[pl.ds(at + i * rows, rows), pl.ds((NN - 1) * TN, TN)]
        part = buf.at[pl.ds(i * rows, rows)]
        moves.append((pltpu.make_async_copy(src.at[pl.ds(i * rows, rows)], part, sem.at[0, i]), pltpu.make_async_copy(part, to, sem.at[1, i])))
    start_all(load for load, _ in moves)
    for load, store in moves:
        load.wait()
        store.start()
    wait_all(store for _, store in moves)


def solution(mesh):
    hbm = pl.BlockSpec(memory_space=pltpu.HBM)

    def dma(*shape):
        return pltpu.SemaphoreType.DMA(shape)

    def local_layer(tokens, ln_scale, w_in, mlp_bias, q_scale, k_scale, w_out, attn_out_bias, mlp_out_bias):
        tok = tokens.reshape(-1, WID)
        vec, at = None, 0
        for v in (ln_scale, mlp_bias, q_scale, k_scale, attn_out_bias, mlp_out_bias):
            wide = jnp.pad(v.astype(F32), (at, VEC - at - v.size), constant_values=-jnp.inf)
            vec = wide if vec is None else jnp.maximum(vec, wide)
            at += v.size
        of = lambda *shape: jax.ShapeDtypeStruct(shape, BF16)
        shapes = [of(*tok.shape), of((NK - NL) * HALF, TN), of(ROWS, WID), of(3, WID, NJ * TN), of(4, WID, NJ * TN), of(3, JB, WID), of(4, JB, WID),
                  of(3, NS, ROWS, TN), of(ROWS, NS * JB), of(ROWS, WID), of(ROWS, WID), of(ROWS, WID)]
        flops = 2 * ROWS * (2 * WID * NT * TN + NS * JB * 2 * WID)
        pairs = [(), (NK,), (7,), (7, NJ), (3,), (3, NN), (NS,), (NS, NN), (), (GROUPS, NN), (), (NK, NN), (2,), (2,), (NS,), (NS,)]
        res = pl.pallas_call(
            kernel,
            out_shape=shapes,
            in_specs=[hbm] * 4,
            out_specs=[hbm] * len(shapes),
            scratch_shapes=[
                pltpu.VMEM((2, M, KH), BF16),
                pltpu.VMEM((4, KH, TN), BF16),
                pltpu.VMEM((2, M, TN), BF16),
                pltpu.VMEM((M, TN), F32),
                pltpu.VMEM((2, 3, M, TN), BF16),
                pltpu.VMEM((2, 4, HALF, TN), BF16),
                pltpu.VMEM((2, 2, LN, WID), BF16),
                pltpu.VMEM((2, 1, WID), F32),
                pltpu.VMEM((NS, 1, UNITS // 2), F32),
                pltpu.VMEM((2, 1, DH), F32),
                pltpu.VMEM((2, 1, WID), F32),
                dma(2, 2), dma(2, 5), dma(2), dma(2), dma(2, 3), dma(2, 5), dma(2, 2), dma(6),
            ] + [dma(*shape) for shape in pairs],
            compiler_params=pltpu.CompilerParams(collective_id=0, has_side_effects=True, vmem_limit_bytes=63 * 2**20),
            cost_estimate=pl.CostEstimate(flops=flops, bytes_accessed=2**30, transcendentals=0),
            name="layer",
        )(tok, w_in, w_out, vec.reshape(1, VEC))
        base, own = res[0], res[1]
        far = lax.ppermute(own, 'mx', [(0, 2), (1, 3), (2, 0), (3, 1)])
        base = pl.pallas_call(
            copy_kernel,
            out_shape=of(*tok.shape),
            in_specs=[hbm],
            out_specs=hbm,
            scratch_shapes=[pltpu.VMEM((16, HALF, WID), BF16), dma(2, 16)],
            compiler_params=pltpu.CompilerParams(vmem_limit_bytes=40 * 2**20),
            cost_estimate=pl.CostEstimate(flops=2 * 10**10, bytes_accessed=4 * tok.size, transcendentals=0),
            name="place",
        )(base)
        far, base = lax.optimization_barrier((far, base))
        farther = lax.ppermute(far, 'mx', [(0, 1), (1, 0), (2, 3), (3, 2)])
        for other, piece in enumerate((far, farther)):
            base = pl.pallas_call(
                functools.partial(tail_kernel, other),
                out_shape=of(*tok.shape),
                in_specs=[hbm] * 2,
                out_specs=hbm,
                input_output_aliases={0: 0},
                scratch_shapes=[pltpu.VMEM(((NK - NL) * HALF, TN), BF16), dma(2, NN)],
                cost_estimate=pl.CostEstimate(flops=10**9, bytes_accessed=4 * piece.size, transcendentals=0),
                name="place_last",
            )(base, piece)
        return base.reshape(tokens.shape)

    specs_in = (P('dp', None, 'my'), P('my'), P('my', 'mx'), P('mx'), P(), P(), P('mx', 'my'), P('my'), P('my'))
    return jax.shard_map(local_layer, mesh=mesh, in_specs=specs_in, out_specs=P('dp', None, 'my'), check_vma=False)
```

```python
import functools

import jax
import jax.numpy as jnp
from jax import lax
from jax.experimental import pallas as pl
from jax.experimental.pallas import tpu as pltpu
from jax.sharding import PartitionSpec as P

MESH = pl.DeviceIdType.MESH
F32, BF16 = jnp.float32, jnp.bfloat16

SEQ, DH, WID = 256, 256, 2048
M, GROUPS = 1024, 4
ROWS = M * GROUPS
HALF = M // 2
TN = 512
QKV, UNITS = 1024, 4096
NS = 4
NJ = 7
NT = NS * NJ
NN = WID // TN
JB = 5 * TN
KH = 2 * JB
LANES = 128
LN = 128
EPS = 1e-6
NK = 2 * GROUPS
NL = NK // 2


def in_col(j, side):
    mlp = (j + 1) // 4
    at = (1 - mlp) * (QKV * j + (QKV // 2) * side) + mlp * (3 * QKV + (UNITS // 2) * side + TN * (j - 3))
    return pl.ds(pl.multiple_of(at, TN), TN)


def out_row(part, side):
    if part == 0:
        return pl.ds(pl.multiple_of((QKV // 2) * side, QKV // 2), TN)
    return pl.ds(pl.multiple_of(QKV + (UNITS // 2) * side, QKV), UNITS // 2)


PART_ROWS = (pl.ds(0, TN), pl.ds(TN, JB - TN))


def tile(n):
    return pl.ds(pl.multiple_of(n * TN, TN), TN)


def rows_of(g):
    return pl.ds(pl.multiple_of(g * M, M), M)


def tile_of(t):
    a, b = (t + 24) // 28, t // 24
    j = (1 - a) * (t // 2) + (a - b) * (t // 4 + 1 - 2 * ((t % 4) // 2)) + b * (t // 2 - 7)
    s = (1 - a) * (t % 2) + (a - b) * (t % 4) + b * (2 + t % 2)
    return j, s


def loop(lo, hi, body):
    def run(i, carry):
        body(i)
        return carry
    lax.fori_loop(lo, hi, run, 0)


def start_all(copies):
    for one in copies:
        one.start()


def wait_all(copies):
    for one in copies:
        one.wait()


def kernel(tok, w_in, w_out, lns, mb, qs, ks, ab, bb,
           out, tail, toth, w1t, w1b, w2y, w2n, qkv, jb, pa, pb, ry,
           zj, wbuf, ptile, acc, abuf, sv, lbuf, sc, ub, gains, ob, raw, raw2,
           w1sem, w2sem, jsem, psem, asem, vsem, lsem, csem,
           t_s, t_r, w_s, w_r, e_s, e_r, d_s, d_r, y_s, y_r, x_s, x_r, o_s, o_r, m_s, m_r):
    y = lax.axis_index("my")
    mi = lax.axis_index("mx")
    x, c = mi // 2, mi % 2
    dev_y = {"my": 1 - y, "mx": mi}
    dev_x = {"my": y, "mx": 2 * (1 - x) + c}
    dev_c = {"my": y, "mx": 2 * x + 1 - c}
    dev_d = {"my": y, "mx": 2 * (1 - x) + 1 - c}
    row0 = (2 * x + c) * ROWS
    row0_x = (2 * (1 - x) + c) * ROWS

    barrier = pltpu.get_barrier_semaphore()
    for dev in (dev_y, dev_x, dev_c, dev_d):
        pl.semaphore_signal(barrier, inc=1, device_id=dev, device_id_type=MESH)
    pl.semaphore_wait(barrier, 4)

    def remote(src, dst, ss, rs, dev):
        return pltpu.make_async_remote_copy(src_ref=src, dst_ref=dst, send_sem=ss, recv_sem=rs, device_id=dev, device_id_type=MESH)

    def t_dir(k):
        src = tok.at[pl.ds(pl.multiple_of(row0 + k * HALF, HALF), HALF)]
        return remote(src, toth.at[pl.ds(pl.multiple_of(k * HALF, HALF), HALF)], t_s, t_r.at[k], dev_y)

    C, B, D, E, F, G, H = range(7)

    def w_own(kind, j, side, dst, dev):
        return remote(w_in.at[:, in_col(j, side)], dst.at[:, tile(j)], w_s.at[kind], w_r.at[kind, j], dev)

    def w_pass(kind, j, src, dst, dev):
        return remote(src.at[:, tile(j)], dst.at[:, tile(j)], w_s.at[kind], w_r.at[kind, j], dev)

    tops = [None] + [w1t.at[i] for i in range(NS - 1)]
    bots = [w1b.at[i] for i in range(NS)]
    OWN, CORE, FAR, FAR_CORE = range(NS)
    w_c = lambda j: w_own(C, j, 1 - y, bots[OWN], dev_y)
    w_b = lambda j: w_own(B, j, y, tops[CORE], dev_c)
    w_d = lambda j: w_pass(D, j, bots[OWN], bots[CORE], dev_c)
    w_e = lambda j: w_own(E, j, y, tops[FAR], dev_x)
    w_f = lambda j: w_pass(F, j, bots[OWN], bots[FAR], dev_x)
    w_g = lambda j: w_pass(G, j, tops[FAR], tops[FAR_CORE], dev_c)
    w_h = lambda j: w_pass(H, j, bots[FAR], bots[FAR_CORE], dev_c)

    class Two:
        def __init__(self, kind, n, side, dst, dev):
            self.copies = [remote(w_out.at[out_row(p, side), tile(n)], dst.at[rows, tile(n)], e_s.at[kind], e_r.at[kind, n], dev)
                           for p, rows in enumerate(PART_ROWS)]
            self.both = remote(dst.at[:, tile(n)], dst.at[:, tile(n)], e_s.at[kind], e_r.at[kind, n], dev)

        def start(self):
            start_all(self.copies)

        def wait_recv(self):
            self.both.wait_recv()

    def v_pass(kind, n, src, dst, dev):
        return remote(src.at[:, tile(n)], dst.at[:, tile(n)], d_s.at[kind], d_r.at[kind, n], dev)

    mine = [None] + [w2y.at[i] for i in range(NS - 1)]
    theirs = [w2n.at[i] for i in range(NS)]
    v_c = lambda n: Two(C, n, 1 - y, theirs[OWN], dev_y)
    v_b = lambda n: Two(B, n, y, mine[CORE], dev_c)
    v_e = lambda n: Two(D, n, y, mine[FAR], dev_x)
    v_d = lambda n: v_pass(C, n, theirs[OWN], theirs[CORE], dev_c)
    v_f = lambda n: v_pass(B, n, theirs[OWN], theirs[FAR], dev_x)
    v_g = lambda n: v_pass(D, n, mine[FAR], mine[FAR_CORE], dev_c)
    v_h = lambda n: v_pass(E, n, theirs[FAR], theirs[FAR_CORE], dev_c)

    def o_y(g, n):
        return remote(pb.at[rows_of(g), tile(n)], ry.at[rows_of(g), tile(n)], y_s, y_r.at[g, n], dev_y)

    def part_rows(k):
        return pl.ds(pl.multiple_of(k * HALF, HALF), HALF)

    def own_out(k):
        return pl.ds(pl.multiple_of(row0 + k * HALF, HALF), HALF)

    def o_x(k, n):
        at = out.at[own_out(k), tile(n)]
        return remote(at, at, x_s, x_r.at[k, n], dev_x)

    def o_c(k, n):
        at = out.at[own_out(k), tile(n)]
        return remote(at, at, o_s.at[0], o_r.at[0], dev_c)

    def o_f(k, n):
        at = out.at[pl.ds(pl.multiple_of(row0_x + k * HALF, HALF), HALF), tile(n)]
        return remote(at, at, o_s.at[1], o_r.at[1], dev_c)

    rows = WID // LANES
    few = DH // LANES
    my_units = mb.at[pl.ds(pl.multiple_of(y * rows, rows), rows)]
    small_far = [remote(src, raw.at[i], m_s.at[i], m_r.at[i], dev) for i, (src, dev) in enumerate((
        (lns, dev_y), (my_units, dev_c), (my_units, dev_x), (my_units, dev_d)))]
    small = [pltpu.make_async_copy(src, dst, csem.at[i]) for i, (src, dst) in enumerate((
        (lns, raw.at[NS]), (my_units, raw.at[NS + 1]), (ab, raw.at[NS + 2]), (bb, raw.at[NS + 3]), (qs, raw2.at[0]), (ks, raw2.at[1])))]

    def spread(src, dst, count):
        for i in range(count):
            dst[:, i * LANES:(i + 1) * LANES] = src[i:i + 1].astype(F32)

    loop(0, NS, lambda j: w_e(j).start())
    start_all(small_far)
    loop(0, NS, lambda k: t_dir(k).start())
    loop(0, NJ, lambda j: w_c(j).start())
    loop(NS, NK, lambda k: t_dir(k).start())
    loop(0, NN, lambda n: v_c(n).start())
    w_e(NS).start()
    w_e(NS + 1).start()
    loop(0, NJ, lambda j: w_b(j).start())
    loop(0, NN, lambda n: v_b(n).start())
    start_all(small)
    wait_all(small)
    for one in small_far:
        one.wait_recv()
    for i, dst in enumerate((sc.at[1], ub.at[CORE], ub.at[FAR], ub.at[FAR_CORE], sc.at[0], ub.at[OWN], ob.at[0], ob.at[1])):
        spread(raw.at[i], dst, rows)
    for i in range(2):
        spread(raw2.at[i], gains.at[i], few)

    def l_copies(g, i, slot):
        at = pl.multiple_of(g * M + i * LN, LN)
        return (
            pltpu.make_async_copy(tok.at[pl.ds(pl.multiple_of(row0 + at, LN), LN)], lbuf.at[slot, 0], lsem.at[slot, 0]),
            pltpu.make_async_copy(toth.at[pl.ds(at, LN)], lbuf.at[slot, 1], lsem.at[slot, 1]),
        )

    def layer_norm(g):
        steps = M // LN
        t_dir(2 * g).wait_recv()
        start_all(l_copies(g, 0, 0))

        def rows(i):
            slot = i % 2

            @pl.when(i == steps // 2 - 1)
            def _():
                t_dir(2 * g + 1).wait_recv()

            @pl.when(i + 1 < steps)
            def _():
                start_all(l_copies(g, i + 1, 1 - slot))
            wait_all(l_copies(g, i, slot))
            step = 64

            def part(k):
                at = pl.ds(pl.multiple_of(k * step, step), step)
                a, b = lbuf[slot, 0, at].astype(F32), lbuf[slot, 1, at].astype(F32)
                mean = (jnp.sum(a, -1, keepdims=True) + jnp.sum(b, -1, keepdims=True)) * (0.5 / WID)
                a, b = a - mean, b - mean
                var = (jnp.sum(a * a, -1, keepdims=True) + jnp.sum(b * b, -1, keepdims=True)) * (0.5 / WID)
                inv = lax.rsqrt(var + EPS)
                to = pl.ds(pl.multiple_of(i * LN + k * step, step), step)
                zj[g % 2, to, :WID] = (a * inv * sc[0]).astype(BF16)
                zj[g % 2, to, WID:2 * WID] = (b * inv * sc[1]).astype(BF16)
            loop(0, LN // step, part)
        loop(0, steps, rows)

    def w1_copies(slot, top, bottom):
        return (
            pltpu.make_async_copy(top, wbuf.at[slot, :WID], w1sem.at[slot, 0]),
            pltpu.make_async_copy(bottom, wbuf.at[slot, WID:2 * WID], w1sem.at[slot, 1]),
        )

    def fetch1(p, t):
        j, s = tile_of(t)
        slot = t % 2

        @pl.when(p == 0)
        def _():
            @pl.when(s == 0)
            def _():
                w_c(j).wait_recv()
                w_d(j).start()
                w_f(j).start()

                @pl.when(j == 2)
                def _():
                    w_e(NJ - 1).start()

                @pl.when(j == NJ - 1)
                def _():
                    v_e(0).start()
                    v_e(1).start()

            @pl.when(s == 1)
            def _():
                w_b(j).wait_recv()
                w_d(j).wait_recv()

            @pl.when(s == 2)
            def _():
                w_e(j).wait_recv()
                w_g(j).start()
                w_f(j).wait_recv()
                w_h(j).start()

            @pl.when(s == 3)
            def _():
                w_g(j).wait_recv()
                w_h(j).wait_recv()

        @pl.when(s == 0)
        def _():
            start_all(w1_copies(slot, w_in.at[:, in_col(j, y)], w1b.at[0, :, tile(j)]))

        @pl.when(s > 0)
        def _():
            start_all(w1_copies(slot, w1t.at[s - 1, :, tile(j)], w1b.at[s, :, tile(j)]))

    def h_store(slot, dst):
        return pltpu.make_async_copy(ptile.at[slot], dst, psem.at[slot])

    def h_done(slot):
        h_store(slot, pb.at[rows_of(0), tile(0)]).wait()

    def w1_tile(p, t):
        j, s = tile_of(t)
        wait_all(w1_copies(t % 2, w1t.at[0, :, tile(0)], w1b.at[0, :, tile(0)]))

        def one(gl):
            g = 2 * p + gl

            def project():
                h = (jnp.dot(zj[gl, :, :WID], wbuf[t % 2, :WID], preferred_element_type=F32)
                     + jnp.dot(zj[gl, :, WID:2 * WID], wbuf[t % 2, WID:2 * WID], preferred_element_type=F32))
                return h.astype(BF16)

            @pl.when((t > 0) & (t != 24))
            def _():
                h_done(gl)

            @pl.when(j < 2)
            def _():
                h = project().astype(F32)
                gain = gains[j]
                for k in range(2):
                    part = h[:, k * DH:(k + 1) * DH]
                    part = part - jnp.mean(part, -1, keepdims=True)
                    var = jnp.mean(part * part, -1, keepdims=True)
                    ptile[gl, :, k * DH:(k + 1) * DH] = (part * lax.rsqrt(var + EPS) * gain).astype(BF16)

            @pl.when(j == 2)
            def _():
                ptile[gl] = project()

            @pl.when(j > 2)
            def _():
                h = project().astype(F32) + ub[s, :, tile(j - 3)]
                ptile[gl] = (0.5 * h * (1.0 + lax.erf(h * 0.7071067811865476))).astype(BF16)

            @pl.when(j <= 2)
            def _():
                h_store(gl, qkv.at[j, s, rows_of(g)]).start()

            @pl.when(j > 2)
            def _():
                h_store(gl, jb.at[rows_of(g), pl.ds(pl.multiple_of(s * JB + (j - 2) * TN, TN), TN)]).start()
        loop(0, 2, one)

    def a_loads(p, w, slot):
        g, s = 2 * p + w // NS, w % NS
        return [pltpu.make_async_copy(qkv.at[i, s, rows_of(g)], abuf.at[slot, i], asem.at[slot, i]) for i in range(3)]

    def a_store(p, w, slot):
        g, s = 2 * p + w // NS, w % NS
        return h_store(slot, jb.at[rows_of(g), pl.ds(pl.multiple_of(s * JB, TN), TN)])

    def attention(p):
        units = 2 * NS
        start_all(a_loads(p, 0, 0))

        def unit(w):
            slot = w % 2

            @pl.when(w + 1 < units)
            def _():
                start_all(a_loads(p, w + 1, 1 - slot))
            wait_all(a_loads(p, w, slot))

            @pl.when(w >= 2)
            def _():
                a_store(p, w - 2, slot).wait()

            def images(i):
                for ii in range(2):
                    at = pl.ds(pl.multiple_of((2 * i + ii) * SEQ, SEQ), SEQ)
                    for k in range(2):
                        cols = slice(k * DH, (k + 1) * DH)
                        q, kk, v = abuf[slot, 0, at, cols], abuf[slot, 1, at, cols], abuf[slot, 2, at, cols]
                        lg = lax.dot_general(q, kk, (((1,), (1,)), ((), ())), preferred_element_type=F32) * (DH ** -0.5)
                        e = jnp.exp(lg - jnp.max(lg, -1, keepdims=True))
                        prob = (e / jnp.sum(e, -1, keepdims=True)).astype(BF16)
                        ptile[slot, at, cols] = jnp.dot(prob, v, preferred_element_type=F32).astype(BF16)
            loop(0, M // SEQ // 2, images)
            a_store(p, w, slot).start()
        loop(0, units, unit)
        a_store(p, units - 2, 0).wait()
        a_store(p, units - 1, 1).wait()

    def w2_slot(m, half):
        return 2 * ((m + 1) % 2) + half

    def w2_dst(m, s):
        return wbuf.at[w2_slot(m, s // 2), pl.ds((s % 2) * JB, JB)]

    def fetch2(m):
        n = m // 2
        e = m % 2

        @pl.when(e == 0)
        def _():
            v_d(n).wait_recv()
            v_h(n).wait_recv()
            for s in range(NS):
                pltpu.make_async_copy(w2n.at[s, :, tile(n)], w2_dst(m, s), w2sem.at[e, s]).start()

        @pl.when(e == 1)
        def _():
            v_b(n).wait_recv()
            v_g(n).wait_recv()
            for p in range(2):
                to = wbuf.at[w2_slot(m, 0), PART_ROWS[p]]
                pltpu.make_async_copy(w_out.at[out_row(p, y), tile(n)], to, w2sem.at[e, 4 * p]).start()
            for s in range(1, NS):
                pltpu.make_async_copy(w2y.at[s - 1, :, tile(n)], w2_dst(m, s), w2sem.at[e, s]).start()

    def arrive2(m):
        e = m % 2

        @pl.when(e == 0)
        def _():
            for s in range(NS):
                pltpu.make_async_copy(w2n.at[s, :, tile(0)], w2_dst(m, s), w2sem.at[e, s]).wait()

        @pl.when(e == 1)
        def _():
            for p in range(2):
                to = wbuf.at[w2_slot(m, 0), PART_ROWS[p]]
                pltpu.make_async_copy(w2n.at[0, PART_ROWS[p], tile(0)], to, w2sem.at[e, 4 * p]).wait()
            for s in range(1, NS):
                pltpu.make_async_copy(w2n.at[s, :, tile(0)], w2_dst(m, s), w2sem.at[e, s]).wait()

    def hand_c(n):
        v_c(n).wait_recv()
        v_d(n).start()
        v_f(n).start()

    def hand_e(n):
        v_e(n).wait_recv()
        v_g(n).start()

    def hand_f(n):
        v_f(n).wait_recv()
        v_h(n).start()

    hands = {5: [lambda: hand_c(0)], 8: [lambda: hand_e(0)], 11: [lambda: hand_c(1), lambda: v_e(2).start()],
             14: [lambda: hand_e(1), lambda: hand_f(0)], 17: [lambda: hand_c(2), lambda: v_e(3).start()],
             20: [lambda: hand_f(1)], 23: [lambda: hand_c(3)]}

    def w1_pass(p):
        layer_norm(2 * p)
        layer_norm(2 * p + 1)

        @pl.when(p == 0)
        def _():
            fetch1(p, 0)

        def step(t):
            @pl.when(t == 24)
            def _():
                h_done(0)
                h_done(1)
                attention(p)

            def fetch_next():
                @pl.when(t + 1 < NT)
                def _():
                    fetch1(p, t + 1)

                @pl.when((t + 1 == NT) & (p == 0))
                def _():
                    fetch1(1, 0)

                @pl.when((t + 1 == NT) & (p == 1))
                def _():
                    fetch2(0)

            @pl.when(p == 1)
            def _():
                fetch_next()
            w1_tile(p, t)

            @pl.when(p == 0)
            def _():
                fetch_next()

            for at, todo in hands.items():
                @pl.when((p == 1) & (t == at))
                def _(todo=todo):
                    for one in todo:
                        one()
        loop(0, NT, step)
        h_done(0)
        h_done(1)
    loop(0, 2, w1_pass)

    def load(e, i, src):
        return pltpu.make_async_copy(src, sv.at[e, i], vsem.at[e, i])

    def fin_loads(k, n, e):
        at = (part_rows(k), tile(n))
        return [load(e, 0, pa.at[at]), load(e, 1, ry.at[at]), load(e, 2, tok.at[own_out(k), tile(n)])]

    def fin_store(k, n, e):
        return pltpu.make_async_copy(sv.at[e, 3], out.at[own_out(k), tile(n)], vsem.at[e, 3])

    def tail_store(k, e):
        return pltpu.make_async_copy(sv.at[e, 3], tail.at[part_rows(k - NL)], vsem.at[e, 4])

    def is_tail(k, n):
        return (n == NN - 1) & (k >= NL)

    def fin_load(k, n, e):
        @pl.when(k % 2 == 0)
        def _():
            o_y(k // 2, n).wait_recv()
        start_all(fin_loads(k, n, e))

    def fin_do(k, n, e):
        wait_all(fin_loads(k, n, e))
        total = sv[e, 0].astype(F32) + sv[e, 1].astype(F32) + (ob[0, :, tile(n)] + ob[1, :, tile(n)]) + sv[e, 2].astype(F32)
        sv[e, 3] = total.astype(BF16)
        fin_store(k, n, e).start()

        @pl.when(is_tail(k, n))
        def _():
            tail_store(k, e).start()

    def fin_send(k, n, e):
        fin_store(k, n, e).wait()

        @pl.when(is_tail(k, n))
        def _():
            tail_store(k, e).wait()

        @pl.when(jnp.logical_not(is_tail(k, n)))
        def _():
            o_x(k, n).start()
        o_c(k, n).start()

    def hand_out(k, n):
        o_x(k, n).wait_recv()
        o_f(k, n).start()

    STEPS = 2 * NN * NK

    def service(v):
        f = v - 11
        n, i = f // 16, f % 16

        @pl.when((f >= 0) & (i >= 2) & (i < NK + 2))
        def _():
            fin_send(i - 2, n, v % 2)

        @pl.when((f >= 0) & (i < NK))
        def _():
            fin_load(i, n, v % 2)

        @pl.when((f >= 0) & (i >= 1) & (i < NK + 1))
        def _():
            fin_do(i - 1, n, (v + 1) % 2)

        for n, at in enumerate((33, 49)):
            @pl.when((v >= at) & (v < at + NK))
            def _(n=n, at=at):
                hand_out(v - at, n)

    def j_copy(v):
        g, half = (v % 8) // 2, v % 2
        src = jb.at[rows_of(g), pl.ds(pl.multiple_of(half * KH, KH), KH)]
        return pltpu.make_async_copy(src, zj.at[half], jsem.at[half])

    def p_copy(m, g):
        n, slot = m // 2, g % 2
        return n, lambda ref: pltpu.make_async_copy(ptile.at[slot], ref.at[rows_of(g), tile(n)], psem.at[slot])

    def p_start(m, g):
        n, to = p_copy(m, g)

        @pl.when(m % 2 == 0)
        def _():
            to(pb).start()

        @pl.when(m % 2 == 1)
        def _():
            to(pa).start()

    def p_finish(m, g):
        n, to = p_copy(m, g)

        @pl.when(m % 2 == 0)
        def _():
            to(pb).wait()
            o_y(g, n).start()

        @pl.when(m % 2 == 1)
        def _():
            to(pa).wait()

    j_copy(0).start()

    def w2_tile(m):
        for at, todo in enumerate((lambda: hand_e(2), lambda: hand_f(2), lambda: hand_e(3), lambda: hand_f(3))):
            @pl.when(m == at)
            def _(todo=todo):
                todo()

        @pl.when(m + 1 < 2 * NN)
        def _():
            fetch2(m + 1)
        arrive2(m)

        def one(g):
            v = m * 2 * GROUPS + 2 * g
            j_copy(v + 1).start()
            j_copy(v).wait()
            acc[...] = jnp.dot(zj[0], wbuf[w2_slot(m, 0)], preferred_element_type=F32)

            @pl.when(g > 0)
            def _():
                p_finish(m, g - 1)
            service(v)

            @pl.when(v + 2 < STEPS)
            def _():
                j_copy(v + 2).start()
            j_copy(v + 1).wait()
            ptile[g % 2] = (acc[...] + jnp.dot(zj[1], wbuf[w2_slot(m, 1)], preferred_element_type=F32)).astype(BF16)
            p_start(m, g)
            service(v + 1)
        loop(0, GROUPS, one)
        p_finish(m, GROUPS - 1)
    loop(0, 2 * NN, w2_tile)

    loop(STEPS, STEPS + 5, service)
    loop(0, NK, lambda k: hand_out(k, 2))

    for one in small_far:
        one.wait_send()
    remote(toth, toth, t_s, t_s, dev_y).wait_send()
    for kind in range(C + NJ):
        remote(bots[OWN], bots[OWN], w_s.at[kind], w_s.at[kind], dev_y).wait_send()
    for kind in range(NS):
        remote(theirs[OWN], theirs[OWN], d_s.at[kind], d_s.at[kind], dev_y).wait_send()
    for kind in range(NS - 1):
        remote(theirs[OWN], theirs[OWN], e_s.at[kind], e_s.at[kind], dev_y).wait_send()
    remote(pb, pb, y_s, y_s, dev_y).wait_send()
    mine_out = out.at[pl.ds(pl.multiple_of(row0, ROWS), ROWS)]
    near_out = remote(mine_out, mine_out, o_s.at[0], o_r.at[0], dev_c)
    near_out.wait_send()
    near_out.wait_recv()

    loop(0, NK - NL, lambda k: hand_out(k, NN - 1))
    sent = out.at[pl.ds(pl.multiple_of(row0, ROWS), ROWS - (NK - NL) * HALF // NN)]
    remote(sent, sent, x_s, x_s, dev_x).wait_send()
    far_out = remote(sent, sent, o_s.at[1], o_r.at[1], dev_c)
    far_out.wait_send()
    far_out.wait_recv()


def copy_kernel(src, dst, buf, sem):
    slots = buf.shape[0]
    x = lax.axis_index("mx") // 2

    def moves(i):
        first = (x + i // (2 * NK)) % 2
        rows = pl.ds(pl.multiple_of(first * 2 * ROWS + (i % (2 * NK)) * HALF, HALF), HALF)
        late = i >= 2 * NK and i % NK >= NL
        cols = pl.ds(0, WID - TN if late else WID)
        k = i % slots
        return (pltpu.make_async_copy(src.at[rows, cols], buf.at[k, :, cols], sem.at[0, k]),
                pltpu.make_async_copy(buf.at[k, :, cols], dst.at[rows, cols], sem.at[1, k]))
    every = [moves(i) for i in range(4 * NK)]
    ahead = slots // 2
    for i in range(4 * NK + ahead):
        if i < 4 * NK:
            if i >= slots:
                every[i - slots][1].wait()
            every[i][0].start()
        if i >= ahead:
            every[i - ahead][0].wait()
            every[i - ahead][1].start()
    for i in range(4 * NK - slots, 4 * NK):
        every[i][1].wait()


def tail_kernel(other, base, src, out, buf, sem):
    mi = lax.axis_index("mx")
    x, c = mi // 2, (mi + other) % 2
    at = pl.multiple_of((2 * (1 - x) + c) * ROWS + NL * HALF, HALF)
    rows = (NK - NL) * HALF // NN
    moves = []
    for i in range(NN):
        to = out.at[pl.ds(at + i * rows, rows), pl.ds((NN - 1) * TN, TN)]
        part = buf.at[pl.ds(i * rows, rows)]
        moves.append((pltpu.make_async_copy(src.at[pl.ds(i * rows, rows)], part, sem.at[0, i]), pltpu.make_async_copy(part, to, sem.at[1, i])))
    start_all(load for load, _ in moves)
    for load, store in moves:
        load.wait()
        store.start()
    wait_all(store for _, store in moves)


def solution(mesh):
    hbm = pl.BlockSpec(memory_space=pltpu.HBM)

    def dma(*shape):
        return pltpu.SemaphoreType.DMA(shape)

    def local_layer(tokens, ln_scale, w_in, mlp_bias, q_scale, k_scale, w_out, attn_out_bias, mlp_out_bias):
        tok = tokens.reshape(-1, WID)
        vecs = [v.reshape(-1, LANES) for v in (ln_scale, mlp_bias, q_scale, k_scale, attn_out_bias, mlp_out_bias)]
        of = lambda *shape: jax.ShapeDtypeStruct(shape, BF16)
        shapes = [of(*tok.shape), of((NK - NL) * HALF, TN), of(ROWS, WID), of(3, WID, NJ * TN), of(4, WID, NJ * TN), of(3, JB, WID), of(4, JB, WID),
                  of(3, NS, ROWS, TN), of(ROWS, NS * JB), of(ROWS, WID), of(ROWS, WID), of(ROWS, WID)]
        flops = 2 * ROWS * (2 * WID * NT * TN + NS * JB * 2 * WID)
        pairs = [(), (NK,), (7,), (7, NJ), (3,), (3, NN), (NS,), (NS, NN), (), (GROUPS, NN), (), (NK, NN), (2,), (2,), (NS,), (NS,)]
        res = pl.pallas_call(
            kernel,
            out_shape=shapes,
            in_specs=[hbm] * 9,
            out_specs=[hbm] * len(shapes),
            scratch_shapes=[
                pltpu.VMEM((2, M, KH), BF16),
                pltpu.VMEM((4, KH, TN), BF16),
                pltpu.VMEM((2, M, TN), BF16),
                pltpu.VMEM((M, TN), F32),
                pltpu.VMEM((2, 3, M, TN), BF16),
                pltpu.VMEM((2, 4, HALF, TN), BF16),
                pltpu.VMEM((2, 2, LN, WID), BF16),
                pltpu.VMEM((2, 1, WID), F32),
                pltpu.VMEM((NS, 1, UNITS // 2), F32),
                pltpu.VMEM((2, 1, DH), F32),
                pltpu.VMEM((2, 1, WID), F32),
                pltpu.VMEM((2 * NS, WID // LANES, LANES), BF16),
                pltpu.VMEM((2, DH // LANES, LANES), BF16),
                dma(2, 2), dma(2, 5), dma(2), dma(2), dma(2, 3), dma(2, 5), dma(2, 2), dma(6),
            ] + [dma(*shape) for shape in pairs],
            compiler_params=pltpu.CompilerParams(collective_id=0, has_side_effects=True, vmem_limit_bytes=63 * 2**20),
            cost_estimate=pl.CostEstimate(flops=flops, bytes_accessed=2**30, transcendentals=0),
            name="layer",
        )(tok, w_in, w_out, *vecs)
        base, own = res[0], res[1]
        far = lax.ppermute(own, 'mx', [(0, 2), (1, 3), (2, 0), (3, 1)])
        base = pl.pallas_call(
            copy_kernel,
            out_shape=of(*tok.shape),
            in_specs=[hbm],
            out_specs=hbm,
            scratch_shapes=[pltpu.VMEM((16, HALF, WID), BF16), dma(2, 16)],
            compiler_params=pltpu.CompilerParams(vmem_limit_bytes=40 * 2**20),
            cost_estimate=pl.CostEstimate(flops=2 * 10**10, bytes_accessed=4 * tok.size, transcendentals=0),
            name="place",
        )(base)
        far, base = lax.optimization_barrier((far, base))
        farther = lax.ppermute(far, 'mx', [(0, 1), (1, 0), (2, 3), (3, 2)])
        for other, piece in enumerate((far, farther)):
            base = pl.pallas_call(
                functools.partial(tail_kernel, other),
                out_shape=of(*tok.shape),
                in_specs=[hbm] * 2,
                out_specs=hbm,
                input_output_aliases={0: 0},
                scratch_shapes=[pltpu.VMEM(((NK - NL) * HALF, TN), BF16), dma(2, NN)],
                cost_estimate=pl.CostEstimate(flops=10**9, bytes_accessed=4 * piece.size, transcendentals=0),
                name="place_last",
            )(base, piece)
        return base.reshape(tokens.shape)

    specs_in = (P('dp', None, 'my'), P('my'), P('my', 'mx'), P('mx'), P(), P(), P('mx', 'my'), P('my'), P('my'))
    return jax.shard_map(local_layer, mesh=mesh, in_specs=specs_in, out_specs=P('dp', None, 'my'), check_vma=False)
```

```python
import functools

import jax
import jax.numpy as jnp
from jax import lax
from jax.experimental import pallas as pl
from jax.experimental.pallas import tpu as pltpu
from jax.sharding import PartitionSpec as P


MESH = pl.DeviceIdType.MESH
F32, BF16 = jnp.float32, jnp.bfloat16

SEQ, DH, WID = 256, 256, 2048
M, GROUPS = 1024, 4
ROWS = M * GROUPS
HALF = M // 2
TN = 512
QKV, UNITS = 1024, 4096
NS = 4
NJ = 7
NT = NS * NJ
NN = WID // TN
JB = 5 * TN
KH = 2 * JB
LANES = 128
LN = 128
EPS = 1e-6
NK = 2 * GROUPS
NL = NK // 2
TAILS = ((NL, NK - 1), (NK - 1, NK))
SPLIT = 3 * NK + NL


def in_col(j, side):
    mlp = (j + 1) // 4
    at = (1 - mlp) * (QKV * j + (QKV // 2) * side) + mlp * (3 * QKV + (UNITS // 2) * side + TN * (j - 3))
    return pl.ds(pl.multiple_of(at, TN), TN)


def out_row(part, side):
    if part == 0:
        return pl.ds(pl.multiple_of((QKV // 2) * side, QKV // 2), TN)
    return pl.ds(pl.multiple_of(QKV + (UNITS // 2) * side, QKV), UNITS // 2)


PART_ROWS = (pl.ds(0, TN), pl.ds(TN, JB - TN))


def tile(n):
    return pl.ds(pl.multiple_of(n * TN, TN), TN)


def rows_of(g):
    return pl.ds(pl.multiple_of(g * M, M), M)


def tile_of(t):
    a, b = (t + 24) // 28, t // 24
    j = (1 - a) * (t // 2) + (a - b) * (t // 4 + 1 - 2 * ((t % 4) // 2)) + b * (t // 2 - 7)
    s = (1 - a) * (t % 2) + (a - b) * (t % 4) + b * (2 + t % 2)
    return j, s


def loop(lo, hi, body):
    def run(i, carry):
        body(i)
        return carry

    lax.fori_loop(lo, hi, run, 0)


def start_all(copies):
    for one in copies:
        one.start()


def wait_all(copies):
    for one in copies:
        one.wait()


def kernel(tok, w_in, w_out, lns, mb, qs, ks, ab, bb,
           out, tail, tail2, toth, w1t, w1b, w2y, w2n, qkv, jb, pa, pb, ry,
           zj, wbuf, ptile, acc, abuf, sv, lbuf, sc, ub, gains, ob, raw, raw2,
           w1sem, w2sem, jsem, psem, asem, vsem, lsem, csem,
           t_s, t_r, w_s, w_r, e_s, e_r, d_s, d_r, y_s, y_r, x_s, x_r, o_s, o_r, m_s, m_r):
    y = lax.axis_index("my")
    mi = lax.axis_index("mx")
    x, c = mi // 2, mi % 2
    dev_y = {"my": 1 - y, "mx": mi}
    dev_x = {"my": y, "mx": 2 * (1 - x) + c}
    dev_c = {"my": y, "mx": 2 * x + 1 - c}
    dev_d = {"my": y, "mx": 2 * (1 - x) + 1 - c}
    row0 = (2 * x + c) * ROWS
    row0_x = (2 * (1 - x) + c) * ROWS

    barrier = pltpu.get_barrier_semaphore()
    for dev in (dev_y, dev_x, dev_c, dev_d):
        pl.semaphore_signal(barrier, inc=1, device_id=dev, device_id_type=MESH)
    pl.semaphore_wait(barrier, 4)

    def remote(src, dst, ss, rs, dev):
        return pltpu.make_async_remote_copy(src_ref=src, dst_ref=dst, send_sem=ss, recv_sem=rs, device_id=dev, device_id_type=MESH)

    def t_dir(k):
        src = tok.at[pl.ds(pl.multiple_of(row0 + k * HALF, HALF), HALF)]
        return remote(src, toth.at[pl.ds(pl.multiple_of(k * HALF, HALF), HALF)], t_s, t_r.at[k], dev_y)

    C, B, D, E, F, G, H = range(7)

    def w_own(kind, j, side, dst, dev):
        return remote(w_in.at[:, in_col(j, side)], dst.at[:, tile(j)], w_s.at[kind], w_r.at[kind, j], dev)

    def w_pass(kind, j, src, dst, dev):
        return remote(src.at[:, tile(j)], dst.at[:, tile(j)], w_s.at[kind], w_r.at[kind, j], dev)

    tops = [None] + [w1t.at[i] for i in range(NS - 1)]
    bots = [w1b.at[i] for i in range(NS)]
    OWN, CORE, FAR, FAR_CORE = range(NS)
    w_c = lambda j: w_own(C, j, 1 - y, bots[OWN], dev_y)
    w_b = lambda j: w_own(B, j, y, tops[CORE], dev_c)
    w_d = lambda j: w_pass(D, j, bots[OWN], bots[CORE], dev_c)
    w_e = lambda j: w_own(E, j, y, tops[FAR], dev_x)
    w_f = lambda j: w_pass(F, j, bots[OWN], bots[FAR], dev_x)
    w_g = lambda j: w_pass(G, j, tops[FAR], tops[FAR_CORE], dev_c)
    w_h = lambda j: w_pass(H, j, bots[FAR], bots[FAR_CORE], dev_c)

    class Two:
        def __init__(self, kind, n, side, dst, dev):
            self.copies = [remote(w_out.at[out_row(p, side), tile(n)], dst.at[rows, tile(n)], e_s.at[kind], e_r.at[kind, n], dev)
                           for p, rows in enumerate(PART_ROWS)]
            self.both = remote(dst.at[:, tile(n)], dst.at[:, tile(n)], e_s.at[kind], e_r.at[kind, n], dev)

        def start(self):
            start_all(self.copies)

        def wait_recv(self):
            self.both.wait_recv()

    def v_pass(kind, n, src, dst, dev):
        return remote(src.at[:, tile(n)], dst.at[:, tile(n)], d_s.at[kind], d_r.at[kind, n], dev)

    mine = [None] + [w2y.at[i] for i in range(NS - 1)]
    theirs = [w2n.at[i] for i in range(NS)]
    v_c = lambda n: Two(C, n, 1 - y, theirs[OWN], dev_y)
    v_b = lambda n: Two(B, n, y, mine[CORE], dev_c)
    v_e = lambda n: Two(D, n, y, mine[FAR], dev_x)
    v_d = lambda n: v_pass(C, n, theirs[OWN], theirs[CORE], dev_c)
    v_f = lambda n: v_pass(B, n, theirs[OWN], theirs[FAR], dev_x)
    v_g = lambda n: v_pass(D, n, mine[FAR], mine[FAR_CORE], dev_c)
    v_h = lambda n: v_pass(E, n, theirs[FAR], theirs[FAR_CORE], dev_c)

    def o_y(g, n):
        return remote(pb.at[rows_of(g), tile(n)], ry.at[rows_of(g), tile(n)], y_s, y_r.at[g, n], dev_y)

    def part_rows(k):
        return pl.ds(pl.multiple_of(k * HALF, HALF), HALF)

    def own_out(k):
        return pl.ds(pl.multiple_of(row0 + k * HALF, HALF), HALF)

    def o_x(k, n):
        at = out.at[own_out(k), tile(n)]
        return remote(at, at, x_s, x_r.at[k, n], dev_x)

    def o_c(k, n):
        at = out.at[own_out(k), tile(n)]
        return remote(at, at, o_s.at[0], o_r.at[0], dev_c)

    def o_f(k, n):
        at = out.at[pl.ds(pl.multiple_of(row0_x + k * HALF, HALF), HALF), tile(n)]
        return remote(at, at, o_s.at[1], o_r.at[1], dev_c)

    rows = WID // LANES
    few = DH // LANES
    my_units = mb.at[pl.ds(pl.multiple_of(y * rows, rows), rows)]
    small_far = [remote(src, raw.at[i], m_s.at[i], m_r.at[i], dev) for i, (src, dev) in enumerate((
        (lns, dev_y), (my_units, dev_c), (my_units, dev_x), (my_units, dev_d)))]
    small = [pltpu.make_async_copy(src, dst, csem.at[i]) for i, (src, dst) in enumerate((
        (lns, raw.at[NS]), (my_units, raw.at[NS + 1]), (ab, raw.at[NS + 2]), (bb, raw.at[NS + 3]), (qs, raw2.at[0]), (ks, raw2.at[1])))]

    def spread(src, dst, count):
        for i in range(count):
            dst[:, i * LANES:(i + 1) * LANES] = src[i:i + 1].astype(F32)

    loop(0, NS, lambda j: w_e(j).start())
    start_all(small_far)
    loop(0, NS, lambda k: t_dir(k).start())
    loop(0, NJ, lambda j: w_c(j).start())
    loop(NS, NK, lambda k: t_dir(k).start())
    loop(0, NN, lambda n: v_c(n).start())
    w_e(NS).start()
    w_e(NS + 1).start()
    loop(0, NJ, lambda j: w_b(j).start())
    loop(0, NN, lambda n: v_b(n).start())
    start_all(small)
    wait_all(small)
    for one in small_far:
        one.wait_recv()
    for i, dst in enumerate((sc.at[1], ub.at[CORE], ub.at[FAR], ub.at[FAR_CORE], sc.at[0], ub.at[OWN], ob.at[0], ob.at[1])):
        spread(raw.at[i], dst, rows)
    for i in range(2):
        spread(raw2.at[i], gains.at[i], few)

    def l_copies(g, i, slot):
        at = pl.multiple_of(g * M + i * LN, LN)
        return (
            pltpu.make_async_copy(tok.at[pl.ds(pl.multiple_of(row0 + at, LN), LN)], lbuf.at[slot, 0], lsem.at[slot, 0]),
            pltpu.make_async_copy(toth.at[pl.ds(at, LN)], lbuf.at[slot, 1], lsem.at[slot, 1]),
        )

    def layer_norm(g):
        steps = M // LN
        t_dir(2 * g).wait_recv()
        start_all(l_copies(g, 0, 0))

        def rows(i):
            slot = i % 2

            @pl.when(i == steps // 2 - 1)
            def _():
                t_dir(2 * g + 1).wait_recv()

            @pl.when(i + 1 < steps)
            def _():
                start_all(l_copies(g, i + 1, 1 - slot))

            wait_all(l_copies(g, i, slot))
            step = 64

            def part(k):
                at = pl.ds(pl.multiple_of(k * step, step), step)
                a, b = lbuf[slot, 0, at].astype(F32), lbuf[slot, 1, at].astype(F32)
                mean = (jnp.sum(a, -1, keepdims=True) + jnp.sum(b, -1, keepdims=True)) * (0.5 / WID)
                a, b = a - mean, b - mean
                var = (jnp.sum(a * a, -1, keepdims=True) + jnp.sum(b * b, -1, keepdims=True)) * (0.5 / WID)
                inv = lax.rsqrt(var + EPS)
                to = pl.ds(pl.multiple_of(i * LN + k * step, step), step)
                zj[g % 2, to, :WID] = (a * inv * sc[0]).astype(BF16)
                zj[g % 2, to, WID:2 * WID] = (b * inv * sc[1]).astype(BF16)

            loop(0, LN // step, part)

        loop(0, steps, rows)

    def w1_copies(slot, top, bottom):
        return (
            pltpu.make_async_copy(top, wbuf.at[slot, :WID], w1sem.at[slot, 0]),
            pltpu.make_async_copy(bottom, wbuf.at[slot, WID:2 * WID], w1sem.at[slot, 1]),
        )

    def fetch1(p, t):
        j, s = tile_of(t)
        slot = t % 2

        @pl.when(p == 0)
        def _():
            @pl.when(s == 0)
            def _():
                w_c(j).wait_recv()
                w_d(j).start()
                w_f(j).start()

                @pl.when(j == 2)
                def _():
                    w_e(NJ - 1).start()

                @pl.when(j == NJ - 1)
                def _():
                    v_e(0).start()
                    v_e(1).start()

            @pl.when(s == 1)
            def _():
                w_b(j).wait_recv()
                w_d(j).wait_recv()

            @pl.when(s == 2)
            def _():
                w_e(j).wait_recv()
                w_g(j).start()
                w_f(j).wait_recv()
                w_h(j).start()

            @pl.when(s == 3)
            def _():
                w_g(j).wait_recv()
                w_h(j).wait_recv()

        @pl.when(s == 0)
        def _():
            start_all(w1_copies(slot, w_in.at[:, in_col(j, y)], w1b.at[0, :, tile(j)]))

        @pl.when(s > 0)
        def _():
            start_all(w1_copies(slot, w1t.at[s - 1, :, tile(j)], w1b.at[s, :, tile(j)]))

    def h_store(slot, dst):
        return pltpu.make_async_copy(ptile.at[slot], dst, psem.at[slot])

    def h_done(slot):
        h_store(slot, pb.at[rows_of(0), tile(0)]).wait()

    def w1_tile(p, t):
        j, s = tile_of(t)
        wait_all(w1_copies(t % 2, w1t.at[0, :, tile(0)], w1b.at[0, :, tile(0)]))

        def one(gl):
            g = 2 * p + gl

            def project():
                h = (jnp.dot(zj[gl, :, :WID], wbuf[t % 2, :WID], preferred_element_type=F32)
                     + jnp.dot(zj[gl, :, WID:2 * WID], wbuf[t % 2, WID:2 * WID], preferred_element_type=F32))
                return h.astype(BF16)

            @pl.when((t > 0) & (t != 24))
            def _():
                h_done(gl)

            @pl.when(j < 2)
            def _():
                h = project().astype(F32)
                gain = gains[j]
                for k in range(2):
                    part = h[:, k * DH:(k + 1) * DH]
                    part = part - jnp.mean(part, -1, keepdims=True)
                    var = jnp.mean(part * part, -1, keepdims=True)
                    ptile[gl, :, k * DH:(k + 1) * DH] = (part * lax.rsqrt(var + EPS) * gain).astype(BF16)

            @pl.when(j == 2)
            def _():
                ptile[gl] = project()

            @pl.when(j > 2)
            def _():
                h = project().astype(F32) + ub[s, :, tile(j - 3)]
                ptile[gl] = (0.5 * h * (1.0 + lax.erf(h * 0.7071067811865476))).astype(BF16)

            @pl.when(j <= 2)
            def _():
                h_store(gl, qkv.at[j, s, rows_of(g)]).start()

            @pl.when(j > 2)
            def _():
                h_store(gl, jb.at[rows_of(g), pl.ds(pl.multiple_of(s * JB + (j - 2) * TN, TN), TN)]).start()

        loop(0, 2, one)

    def a_loads(p, w, slot):
        g, s = 2 * p + w // NS, w % NS
        return [pltpu.make_async_copy(qkv.at[i, s, rows_of(g)], abuf.at[slot, i], asem.at[slot, i]) for i in range(3)]

    def a_store(p, w, slot):
        g, s = 2 * p + w // NS, w % NS
        return h_store(slot, jb.at[rows_of(g), pl.ds(pl.multiple_of(s * JB, TN), TN)])

    def attention(p):
        units = 2 * NS
        start_all(a_loads(p, 0, 0))

        def unit(w):
            slot = w % 2

            @pl.when(w + 1 < units)
            def _():
                start_all(a_loads(p, w + 1, 1 - slot))

            wait_all(a_loads(p, w, slot))

            @pl.when(w >= 2)
            def _():
                a_store(p, w - 2, slot).wait()

            def images(i):
                for ii in range(2):
                    at = pl.ds(pl.multiple_of((2 * i + ii) * SEQ, SEQ), SEQ)
                    for k in range(2):
                        cols = slice(k * DH, (k + 1) * DH)
                        q, kk, v = abuf[slot, 0, at, cols], abuf[slot, 1, at, cols], abuf[slot, 2, at, cols]
                        lg = lax.dot_general(q, kk, (((1,), (1,)), ((), ())), preferred_element_type=F32) * (DH ** -0.5)
                        e = jnp.exp(lg - jnp.max(lg, -1, keepdims=True))
                        prob = (e / jnp.sum(e, -1, keepdims=True)).astype(BF16)
                        ptile[slot, at, cols] = jnp.dot(prob, v, preferred_element_type=F32).astype(BF16)

            loop(0, M // SEQ // 2, images)
            a_store(p, w, slot).start()

        loop(0, units, unit)
        a_store(p, units - 2, 0).wait()
        a_store(p, units - 1, 1).wait()

    def w2_slot(m, half):
        return 2 * ((m + 1) % 2) + half

    def w2_dst(m, s):
        return wbuf.at[w2_slot(m, s // 2), pl.ds((s % 2) * JB, JB)]

    def fetch2(m):
        n = m // 2
        e = m % 2

        @pl.when(e == 0)
        def _():
            v_d(n).wait_recv()
            v_h(n).wait_recv()
            for s in range(NS):
                pltpu.make_async_copy(w2n.at[s, :, tile(n)], w2_dst(m, s), w2sem.at[e, s]).start()

        @pl.when(e == 1)
        def _():
            v_b(n).wait_recv()
            v_g(n).wait_recv()
            for p in range(2):
                to = wbuf.at[w2_slot(m, 0), PART_ROWS[p]]
                pltpu.make_async_copy(w_out.at[out_row(p, y), tile(n)], to, w2sem.at[e, 4 * p]).start()
            for s in range(1, NS):
                pltpu.make_async_copy(w2y.at[s - 1, :, tile(n)], w2_dst(m, s), w2sem.at[e, s]).start()

    def arrive2(m):
        e = m % 2

        @pl.when(e == 0)
        def _():
            for s in range(NS):
                pltpu.make_async_copy(w2n.at[s, :, tile(0)], w2_dst(m, s), w2sem.at[e, s]).wait()

        @pl.when(e == 1)
        def _():
            for p in range(2):
                to = wbuf.at[w2_slot(m, 0), PART_ROWS[p]]
                pltpu.make_async_copy(w2n.at[0, PART_ROWS[p], tile(0)], to, w2sem.at[e, 4 * p]).wait()
            for s in range(1, NS):
                pltpu.make_async_copy(w2n.at[s, :, tile(0)], w2_dst(m, s), w2sem.at[e, s]).wait()

    def hand_c(n):
        v_c(n).wait_recv()
        v_d(n).start()
        v_f(n).start()

    def hand_e(n):
        v_e(n).wait_recv()
        v_g(n).start()

    def hand_f(n):
        v_f(n).wait_recv()
        v_h(n).start()

    hands = {5: [lambda: hand_c(0)], 8: [lambda: hand_e(0)], 11: [lambda: hand_c(1), lambda: v_e(2).start()],
             14: [lambda: hand_e(1), lambda: hand_f(0)], 17: [lambda: hand_c(2), lambda: v_e(3).start()],
             20: [lambda: hand_f(1)], 23: [lambda: hand_c(3)]}

    def w1_pass(p):
        layer_norm(2 * p)
        layer_norm(2 * p + 1)

        @pl.when(p == 0)
        def _():
            fetch1(p, 0)

        def step(t):
            @pl.when(t == 24)
            def _():
                h_done(0)
                h_done(1)
                attention(p)

            def fetch_next():
                @pl.when(t + 1 < NT)
                def _():
                    fetch1(p, t + 1)

                @pl.when((t + 1 == NT) & (p == 0))
                def _():
                    fetch1(1, 0)

                @pl.when((t + 1 == NT) & (p == 1))
                def _():
                    fetch2(0)

            @pl.when(p == 1)
            def _():
                fetch_next()

            w1_tile(p, t)

            @pl.when(p == 0)
            def _():
                fetch_next()

            for at, todo in hands.items():
                @pl.when((p == 1) & (t == at))
                def _(todo=todo):
                    for one in todo:
                        one()

        loop(0, NT, step)
        h_done(0)
        h_done(1)

    loop(0, 2, w1_pass)

    def load(e, i, src):
        return pltpu.make_async_copy(src, sv.at[e, i], vsem.at[e, i])

    def fin_loads(k, n, e):
        at = (part_rows(k), tile(n))
        return [load(e, 0, pa.at[at]), load(e, 1, ry.at[at]), load(e, 2, tok.at[own_out(k), tile(n)])]

    def fin_store(k, n, e):
        return pltpu.make_async_copy(sv.at[e, 3], out.at[own_out(k), tile(n)], vsem.at[e, 3])

    def tail_store(k, e):
        def to(ref):
            return pltpu.make_async_copy(sv.at[e, 3], ref, vsem.at[e, 4])

        @pl.when(k < NK - 1)
        def _():
            to(tail.at[part_rows(k - NL)]).start()

        @pl.when(k == NK - 1)
        def _():
            to(tail2).start()

    def is_tail(k, n):
        return (n == NN - 1) & (k >= NL)

    def fin_load(k, n, e):
        @pl.when(k % 2 == 0)
        def _():
            o_y(k // 2, n).wait_recv()

        start_all(fin_loads(k, n, e))

    def fin_do(k, n, e):
        wait_all(fin_loads(k, n, e))
        total = sv[e, 0].astype(F32) + sv[e, 1].astype(F32) + (ob[0, :, tile(n)] + ob[1, :, tile(n)]) + sv[e, 2].astype(F32)
        sv[e, 3] = total.astype(BF16)
        fin_store(k, n, e).start()

        @pl.when(is_tail(k, n))
        def _():
            tail_store(k, e)

    def fin_send(k, n, e):
        fin_store(k, n, e).wait()

        @pl.when(is_tail(k, n))
        def _():
            pltpu.make_async_copy(sv.at[e, 3], tail2, vsem.at[e, 4]).wait()

        @pl.when(jnp.logical_not(is_tail(k, n)))
        def _():
            o_x(k, n).start()

        o_c(k, n).start()

    def hand_out(k, n):
        o_x(k, n).wait_recv()
        o_f(k, n).start()

    STEPS = 2 * NN * NK

    def service(v):
        f = v - 11
        n, i = f // 16, f % 16

        @pl.when((f >= 0) & (i >= 2) & (i < NK + 2))
        def _():
            fin_send(i - 2, n, v % 2)

        @pl.when((f >= 0) & (i < NK))
        def _():
            fin_load(i, n, v % 2)

        @pl.when((f >= 0) & (i >= 1) & (i < NK + 1))
        def _():
            fin_do(i - 1, n, (v + 1) % 2)

        for n, at in enumerate((33, 49)):
            @pl.when((v >= at) & (v < at + NK))
            def _(n=n, at=at):
                hand_out(v - at, n)

    def j_copy(v):
        g, half = (v % 8) // 2, v % 2
        src = jb.at[rows_of(g), pl.ds(pl.multiple_of(half * KH, KH), KH)]
        return pltpu.make_async_copy(src, zj.at[half], jsem.at[half])

    def p_copy(m, g):
        n, slot = m // 2, g % 2
        return n, lambda ref: pltpu.make_async_copy(ptile.at[slot], ref.at[rows_of(g), tile(n)], psem.at[slot])

    def p_start(m, g):
        _, to = p_copy(m, g)

        @pl.when(m % 2 == 0)
        def _():
            to(pb).start()

        @pl.when(m % 2 == 1)
        def _():
            to(pa).start()

    def p_finish(m, g):
        n, to = p_copy(m, g)

        @pl.when(m % 2 == 0)
        def _():
            to(pb).wait()
            o_y(g, n).start()

        @pl.when(m % 2 == 1)
        def _():
            to(pa).wait()

    j_copy(0).start()

    def w2_tile(m):
        for at, todo in enumerate((lambda: hand_e(2), lambda: hand_f(2), lambda: hand_e(3), lambda: hand_f(3))):
            @pl.when(m == at)
            def _(todo=todo):
                todo()

        @pl.when(m + 1 < 2 * NN)
        def _():
            fetch2(m + 1)

        arrive2(m)

        def one(g):
            v = m * 2 * GROUPS + 2 * g
            j_copy(v + 1).start()
            j_copy(v).wait()
            acc[...] = jnp.dot(zj[0], wbuf[w2_slot(m, 0)], preferred_element_type=F32)

            @pl.when(g > 0)
            def _():
                p_finish(m, g - 1)

            service(v)

            @pl.when(v + 2 < STEPS)
            def _():
                j_copy(v + 2).start()

            j_copy(v + 1).wait()
            ptile[g % 2] = (acc[...] + jnp.dot(zj[1], wbuf[w2_slot(m, 1)], preferred_element_type=F32)).astype(BF16)
            p_start(m, g)
            service(v + 1)

        loop(0, GROUPS, one)
        p_finish(m, GROUPS - 1)

    loop(0, 2 * NN, w2_tile)

    loop(STEPS, STEPS + 5, service)
    loop(0, NK, lambda k: hand_out(k, 2))

    for one in small_far:
        one.wait_send()
    remote(toth, toth, t_s, t_s, dev_y).wait_send()
    for kind in range(C + NJ):
        remote(bots[OWN], bots[OWN], w_s.at[kind], w_s.at[kind], dev_y).wait_send()
    for kind in range(NS):
        remote(theirs[OWN], theirs[OWN], d_s.at[kind], d_s.at[kind], dev_y).wait_send()
    for kind in range(NS - 1):
        remote(theirs[OWN], theirs[OWN], e_s.at[kind], e_s.at[kind], dev_y).wait_send()
    remote(pb, pb, y_s, y_s, dev_y).wait_send()
    mine_out = out.at[pl.ds(pl.multiple_of(row0, ROWS), ROWS)]
    near_out = remote(mine_out, mine_out, o_s.at[0], o_r.at[0], dev_c)
    near_out.wait_send()
    near_out.wait_recv()

    loop(0, NK - NL, lambda k: hand_out(k, NN - 1))
    sent = out.at[pl.ds(pl.multiple_of(row0, ROWS), ROWS - (NK - NL) * HALF // NN)]
    remote(sent, sent, x_s, x_s, dev_x).wait_send()
    far_out = remote(sent, sent, o_s.at[1], o_r.at[1], dev_c)
    far_out.wait_send()
    far_out.wait_recv()


def copy_kernel(lo, hi, src, *rest):
    dst, buf, sem = rest[-3:]
    slots = buf.shape[0]
    x = lax.axis_index("mx") // 2

    def moves(i):
        first = (x + i // (2 * NK)) % 2
        rows = pl.ds(pl.multiple_of(first * 2 * ROWS + (i % (2 * NK)) * HALF, HALF), HALF)
        late = i >= 2 * NK and i % NK >= NL
        cols = pl.ds(0, WID - TN if late else WID)
        k = (i - lo) % slots
        return (pltpu.make_async_copy(src.at[rows, cols], buf.at[k, :, cols], sem.at[0, k]),
                pltpu.make_async_copy(buf.at[k, :, cols], dst.at[rows, cols], sem.at[1, k]))

    every = [moves(i) for i in range(lo, hi)]
    ahead, count = 12, hi - lo
    for i in range(count + ahead):
        if i < count:
            if i >= slots:
                every[i - slots][1].wait()
            every[i][0].start()
        if i >= ahead:
            every[i - ahead][0].wait()
            every[i - ahead][1].start()
    for _, store in every[-min(slots, count):]:
        store.wait()


def tail_kernel(lo, hi, other, base, src, out, sem):
    mi = lax.axis_index("mx")
    x, c = mi // 2, (mi + other) % 2
    at = pl.multiple_of((2 * (1 - x) + c) * ROWS + lo * HALF, HALF)
    move = pltpu.make_async_copy(src, out.at[pl.ds(at, (hi - lo) * HALF), pl.ds((NN - 1) * TN, TN)], sem)
    move.start()
    move.wait()


def solution(mesh):
    hbm = pl.BlockSpec(memory_space=pltpu.HBM)

    def dma(*shape):
        return pltpu.SemaphoreType.DMA(shape)

    def local_layer(tokens, ln_scale, w_in, mlp_bias, q_scale, k_scale, w_out, attn_out_bias, mlp_out_bias):
        tok = tokens.reshape(-1, WID)
        vecs = [v.reshape(-1, LANES) for v in (ln_scale, mlp_bias, q_scale, k_scale, attn_out_bias, mlp_out_bias)]
        of = lambda *shape: jax.ShapeDtypeStruct(shape, BF16)
        shapes = [of(*tok.shape), *[of((hi - lo) * HALF, TN) for lo, hi in TAILS], of(ROWS, WID), of(3, WID, NJ * TN), of(4, WID, NJ * TN), of(3, JB, WID), of(4, JB, WID),
                  of(3, NS, ROWS, TN), of(ROWS, NS * JB), of(ROWS, WID), of(ROWS, WID), of(ROWS, WID)]
        flops = 2 * ROWS * (2 * WID * NT * TN + NS * JB * 2 * WID)
        pairs = [(), (NK,), (7,), (7, NJ), (3,), (3, NN), (NS,), (NS, NN), (), (GROUPS, NN), (), (NK, NN), (2,), (2,), (NS,), (NS,)]
        res = pl.pallas_call(
            kernel,
            out_shape=shapes,
            in_specs=[hbm] * 9,
            out_specs=[hbm] * len(shapes),
            scratch_shapes=[
                pltpu.VMEM((2, M, KH), BF16),
                pltpu.VMEM((4, KH, TN), BF16),
                pltpu.VMEM((2, M, TN), BF16),
                pltpu.VMEM((M, TN), F32),
                pltpu.VMEM((2, 3, M, TN), BF16),
                pltpu.VMEM((2, 4, HALF, TN), BF16),
                pltpu.VMEM((2, 2, LN, WID), BF16),
                pltpu.VMEM((2, 1, WID), F32),
                pltpu.VMEM((NS, 1, UNITS // 2), F32),
                pltpu.VMEM((2, 1, DH), F32),
                pltpu.VMEM((2, 1, WID), F32),
                pltpu.VMEM((2 * NS, WID // LANES, LANES), BF16),
                pltpu.VMEM((2, DH // LANES, LANES), BF16),
                dma(2, 2), dma(2, 5), dma(2), dma(2), dma(2, 3), dma(2, 5), dma(2, 2), dma(6),
            ] + [dma(*shape) for shape in pairs],
            compiler_params=pltpu.CompilerParams(collective_id=0, has_side_effects=True, vmem_limit_bytes=63 * 2**20),
            cost_estimate=pl.CostEstimate(flops=flops, bytes_accessed=2**30, transcendentals=0),
            name="layer",
        )(tok, w_in, w_out, *vecs)
        base = res[0]
        over_x = [(0, 2), (1, 3), (2, 0), (3, 1)]
        over_core = [(0, 1), (1, 0), (2, 3), (3, 2)]
        far = []
        for own in res[1:3]:
            far.append(lax.ppermute(own, 'mx', over_x))

        def put(lo, hi, *arrays):
            return pl.pallas_call(
                functools.partial(copy_kernel, lo, hi),
                out_shape=of(*tok.shape),
                in_specs=[hbm] * len(arrays),
                out_specs=hbm,
                input_output_aliases={i: 0 for i in range(1, len(arrays))},
                scratch_shapes=[pltpu.VMEM((16, HALF, WID), BF16), dma(2, 16)],
                compiler_params=pltpu.CompilerParams(vmem_limit_bytes=40 * 2**20),
                cost_estimate=pl.CostEstimate(flops=(hi - lo) * 10**9, bytes_accessed=(hi - lo) * 4 * HALF * WID, transcendentals=0),
                name="place",
            )(*arrays)

        def put_last(base, piece, lo, hi, other):
            return pl.pallas_call(
                functools.partial(tail_kernel, lo, hi, other),
                out_shape=of(*tok.shape),
                in_specs=[hbm, pl.BlockSpec(memory_space=pltpu.VMEM)],
                out_specs=hbm,
                input_output_aliases={0: 0},
                scratch_shapes=[dma()],
                compiler_params=pltpu.CompilerParams(vmem_limit_bytes=8 * 2**20),
                cost_estimate=pl.CostEstimate(flops=10**9, bytes_accessed=4 * piece.size, transcendentals=0),
                name="place_last",
            )(base, piece)

        results = base
        base = put(0, SPLIT, results)
        for (lo, hi), piece in zip(TAILS, far):
            piece, base = lax.optimization_barrier((piece, base))
            farther = lax.ppermute(piece, 'mx', over_core)
            if lo == NL:
                base = put(SPLIT, 4 * NK, results, base)
            for other, part in enumerate((piece, farther)):
                base = put_last(base, part, lo, hi, other)
        return base.reshape(tokens.shape)

    specs_in = (P('dp', None, 'my'), P('my'), P('my', 'mx'), P('mx'), P(), P(), P('mx', 'my'), P('my'), P('my'))

    return jax.shard_map(local_layer, mesh=mesh, in_specs=specs_in, out_specs=P('dp', None, 'my'), check_vma=False)
```

```python
import functools

import jax
import jax.numpy as jnp
from jax import lax
from jax.experimental import pallas as pl
from jax.experimental.pallas import tpu as pltpu
from jax.sharding import PartitionSpec as P


MESH = pl.DeviceIdType.MESH
F32, BF16 = jnp.float32, jnp.bfloat16

SEQ, DH, WID = 256, 256, 2048
M, GROUPS = 1024, 4
ROWS = M * GROUPS
HALF = M // 2
TN = 512
QKV, UNITS = 1024, 4096
NS = 4
NJ = 7
NT = NS * NJ
NN = WID // TN
JB = 5 * TN
KH = 2 * JB
LANES = 128
LN = 128
EPS = 1e-6
NK = 2 * GROUPS
NL = NK // 2
TAILS = ((NL, NK - 1), (NK - 1, NK))
SPLIT = 3 * NK + NL


def in_col(j, side):
    mlp = (j + 1) // 4
    at = (1 - mlp) * (QKV * j + (QKV // 2) * side) + mlp * (3 * QKV + (UNITS // 2) * side + TN * (j - 3))
    return pl.ds(pl.multiple_of(at, TN), TN)


def out_row(part, side):
    if part == 0:
        return pl.ds(pl.multiple_of((QKV // 2) * side, QKV // 2), TN)
    return pl.ds(pl.multiple_of(QKV + (UNITS // 2) * side, QKV), UNITS // 2)


LAST = pl.ds((NN - 1) * TN, TN)
PART_ROWS = (pl.ds(0, TN), pl.ds(TN, JB - TN))


def first_row(x, c):
    return pl.multiple_of((2 * x + c) * ROWS, ROWS)


def cost(flops, size):
    return pl.CostEstimate(flops=flops, bytes_accessed=size, transcendentals=0)


def tile(n):
    return pl.ds(pl.multiple_of(n * TN, TN), TN)


def rows_of(g):
    return pl.ds(pl.multiple_of(g * M, M), M)


def tile_of(t):
    a, b = (t + 24) // 28, t // 24
    j = (1 - a) * (t // 2) + (a - b) * (t // 4 + 1 - 2 * ((t % 4) // 2)) + b * (t // 2 - 7)
    s = (1 - a) * (t % 2) + (a - b) * (t % 4) + b * (2 + t % 2)
    return j, s


def loop(lo, hi, body):
    def run(i, carry):
        body(i)
        return carry

    lax.fori_loop(lo, hi, run, 0)


def start_all(copies):
    for one in copies:
        one.start()


def wait_all(copies):
    for one in copies:
        one.wait()


def kernel(tok, w_in, w_out, lns, mb, qs, ks, ab, bb,
           out, tail, tail2, rec, toth, w1t, w1b, w2y, w2n, qkv, jb, pa, pb, ry,
           zj, wbuf, ptile, acc, abuf, sv, lbuf, sc, ub, gains, ob, raw, raw2,
           w1sem, w2sem, jsem, psem, asem, vsem, lsem, csem,
           t_s, t_r, w_s, w_r, e_s, e_r, d_s, d_r, y_s, y_r, x_s, x_r, o_s, o_r, m_s, m_r):
    y = lax.axis_index("my")
    mi = lax.axis_index("mx")
    x, c = mi // 2, mi % 2
    dev_y = {"my": 1 - y, "mx": mi}
    dev_x = {"my": y, "mx": 2 * (1 - x) + c}
    dev_c = {"my": y, "mx": 2 * x + 1 - c}
    dev_d = {"my": y, "mx": 2 * (1 - x) + 1 - c}
    row0, row0_x = first_row(x, c), first_row(1 - x, c)

    barrier = pltpu.get_barrier_semaphore()
    for dev in (dev_y, dev_x, dev_c, dev_d):
        pl.semaphore_signal(barrier, inc=1, device_id=dev, device_id_type=MESH)
    pl.semaphore_wait(barrier, 4)

    def remote(src, dst, ss, rs, dev):
        return pltpu.make_async_remote_copy(src_ref=src, dst_ref=dst, send_sem=ss, recv_sem=rs, device_id=dev, device_id_type=MESH)

    def t_dir(k):
        src = tok.at[pl.ds(pl.multiple_of(row0 + k * HALF, HALF), HALF)]
        return remote(src, toth.at[pl.ds(pl.multiple_of(k * HALF, HALF), HALF)], t_s, t_r.at[k], dev_y)

    C, B, D, E, F, G, H = range(7)

    def w_own(kind, j, side, dst, dev):
        return remote(w_in.at[:, in_col(j, side)], dst.at[:, tile(j)], w_s.at[kind], w_r.at[kind, j], dev)

    def w_pass(kind, j, src, dst, dev):
        return remote(src.at[:, tile(j)], dst.at[:, tile(j)], w_s.at[kind], w_r.at[kind, j], dev)

    tops = [None] + [w1t.at[i] for i in range(NS - 1)]
    bots = [w1b.at[i] for i in range(NS)]
    OWN, CORE, FAR, FAR_CORE = range(NS)
    w_c = lambda j: w_own(C, j, 1 - y, bots[OWN], dev_y)
    w_b = lambda j: w_own(B, j, y, tops[CORE], dev_c)
    w_d = lambda j: w_pass(D, j, bots[OWN], bots[CORE], dev_c)
    w_e = lambda j: w_own(E, j, y, tops[FAR], dev_x)
    w_f = lambda j: w_pass(F, j, bots[OWN], bots[FAR], dev_x)
    w_g = lambda j: w_pass(G, j, tops[FAR], tops[FAR_CORE], dev_c)
    w_h = lambda j: w_pass(H, j, bots[FAR], bots[FAR_CORE], dev_c)

    class Two:
        def __init__(self, kind, n, side, dst, dev):
            self.copies = [remote(w_out.at[out_row(p, side), tile(n)], dst.at[rows, tile(n)], e_s.at[kind], e_r.at[kind, n], dev)
                           for p, rows in enumerate(PART_ROWS)]
            self.both = remote(dst.at[:, tile(n)], dst.at[:, tile(n)], e_s.at[kind], e_r.at[kind, n], dev)

        def start(self):
            start_all(self.copies)

        def wait_recv(self):
            self.both.wait_recv()

    def v_pass(kind, n, src, dst, dev):
        return remote(src.at[:, tile(n)], dst.at[:, tile(n)], d_s.at[kind], d_r.at[kind, n], dev)

    mine = [None] + [w2y.at[i] for i in range(NS - 1)]
    theirs = [w2n.at[i] for i in range(NS)]
    v_c = lambda n: Two(C, n, 1 - y, theirs[OWN], dev_y)
    v_b = lambda n: Two(B, n, y, mine[CORE], dev_c)
    v_e = lambda n: Two(D, n, y, mine[FAR], dev_x)
    v_d = lambda n: v_pass(C, n, theirs[OWN], theirs[CORE], dev_c)
    v_f = lambda n: v_pass(B, n, theirs[OWN], theirs[FAR], dev_x)
    v_g = lambda n: v_pass(D, n, mine[FAR], mine[FAR_CORE], dev_c)
    v_h = lambda n: v_pass(E, n, theirs[FAR], theirs[FAR_CORE], dev_c)

    def o_y(g, n):
        return remote(pb.at[rows_of(g), tile(n)], ry.at[rows_of(g), tile(n)], y_s, y_r.at[g, n], dev_y)

    def part_rows(k):
        return pl.ds(pl.multiple_of(k * HALF, HALF), HALF)

    def own_out(k):
        return pl.ds(pl.multiple_of(row0 + k * HALF, HALF), HALF)

    def o_x(k, n):
        at = out.at[own_out(k), tile(n)]
        return remote(at, at, x_s, x_r.at[k, n], dev_x)

    def o_c(k, n):
        at = out.at[own_out(k), tile(n)]
        return remote(at, at, o_s.at[0], o_r.at[0], dev_c)

    def o_f(k, n):
        at = out.at[pl.ds(pl.multiple_of(row0_x + k * HALF, HALF), HALF), tile(n)]
        return remote(at, at, o_s.at[1], o_r.at[1], dev_c)

    rows = WID // LANES
    few = DH // LANES
    my_units = mb.at[pl.ds(pl.multiple_of(y * rows, rows), rows)]
    small_far = [remote(src, raw.at[i], m_s.at[i], m_r.at[i], dev) for i, (src, dev) in enumerate((
        (lns, dev_y), (my_units, dev_c), (my_units, dev_x), (my_units, dev_d)))]
    small = [pltpu.make_async_copy(src, dst, csem.at[i]) for i, (src, dst) in enumerate((
        (lns, raw.at[NS]), (my_units, raw.at[NS + 1]), (ab, raw.at[NS + 2]), (bb, raw.at[NS + 3]), (qs, raw2.at[0]), (ks, raw2.at[1])))]

    def spread(src, dst, count):
        for i in range(count):
            dst[:, i * LANES:(i + 1) * LANES] = src[i:i + 1].astype(F32)

    loop(0, NS, lambda j: w_e(j).start())
    start_all(small_far)
    loop(0, NS, lambda k: t_dir(k).start())
    loop(0, NJ, lambda j: w_c(j).start())
    loop(NS, NK, lambda k: t_dir(k).start())
    loop(0, NN, lambda n: v_c(n).start())
    w_e(NS).start()
    w_e(NS + 1).start()
    loop(0, NJ, lambda j: w_b(j).start())
    loop(0, NN, lambda n: v_b(n).start())
    start_all(small)
    wait_all(small)
    for one in small_far:
        one.wait_recv()
    for i, dst in enumerate((sc.at[1], ub.at[CORE], ub.at[FAR], ub.at[FAR_CORE], sc.at[0], ub.at[OWN], ob.at[0], ob.at[1])):
        spread(raw.at[i], dst, rows)
    for i in range(2):
        spread(raw2.at[i], gains.at[i], few)

    def l_copies(g, i, slot):
        at = pl.multiple_of(g * M + i * LN, LN)
        return (
            pltpu.make_async_copy(tok.at[pl.ds(pl.multiple_of(row0 + at, LN), LN)], lbuf.at[slot, 0], lsem.at[slot, 0]),
            pltpu.make_async_copy(toth.at[pl.ds(at, LN)], lbuf.at[slot, 1], lsem.at[slot, 1]),
        )

    def layer_norm(g):
        steps = M // LN
        t_dir(2 * g).wait_recv()
        start_all(l_copies(g, 0, 0))

        def rows(i):
            slot = i % 2

            @pl.when(i == steps // 2 - 1)
            def _():
                t_dir(2 * g + 1).wait_recv()

            @pl.when(i + 1 < steps)
            def _():
                start_all(l_copies(g, i + 1, 1 - slot))

            wait_all(l_copies(g, i, slot))
            step = 64

            def part(k):
                at = pl.ds(pl.multiple_of(k * step, step), step)
                a, b = lbuf[slot, 0, at].astype(F32), lbuf[slot, 1, at].astype(F32)
                mean = (jnp.sum(a, -1, keepdims=True) + jnp.sum(b, -1, keepdims=True)) * (0.5 / WID)
                a, b = a - mean, b - mean
                var = (jnp.sum(a * a, -1, keepdims=True) + jnp.sum(b * b, -1, keepdims=True)) * (0.5 / WID)
                inv = lax.rsqrt(var + EPS)
                to = pl.ds(pl.multiple_of(i * LN + k * step, step), step)
                zj[g % 2, to, :WID] = (a * inv * sc[0]).astype(BF16)
                zj[g % 2, to, WID:2 * WID] = (b * inv * sc[1]).astype(BF16)

            loop(0, LN // step, part)

        loop(0, steps, rows)

    def w1_copies(slot, top, bottom):
        return (
            pltpu.make_async_copy(top, wbuf.at[slot, :WID], w1sem.at[slot, 0]),
            pltpu.make_async_copy(bottom, wbuf.at[slot, WID:2 * WID], w1sem.at[slot, 1]),
        )

    def fetch1(p, t):
        j, s = tile_of(t)
        slot = t % 2

        @pl.when(p == 0)
        def _():
            @pl.when(s == 0)
            def _():
                w_c(j).wait_recv()
                w_d(j).start()
                w_f(j).start()

                @pl.when(j == 2)
                def _():
                    w_e(NJ - 1).start()

                @pl.when(j == NJ - 1)
                def _():
                    v_e(0).start()
                    v_e(1).start()

            @pl.when(s == 1)
            def _():
                w_b(j).wait_recv()
                w_d(j).wait_recv()

            @pl.when(s == 2)
            def _():
                w_e(j).wait_recv()
                w_g(j).start()
                w_f(j).wait_recv()
                w_h(j).start()

            @pl.when(s == 3)
            def _():
                w_g(j).wait_recv()
                w_h(j).wait_recv()

        @pl.when(s == 0)
        def _():
            start_all(w1_copies(slot, w_in.at[:, in_col(j, y)], w1b.at[0, :, tile(j)]))

        @pl.when(s > 0)
        def _():
            start_all(w1_copies(slot, w1t.at[s - 1, :, tile(j)], w1b.at[s, :, tile(j)]))

    def h_store(slot, dst):
        return pltpu.make_async_copy(ptile.at[slot], dst, psem.at[slot])

    def h_done(slot):
        h_store(slot, pb.at[rows_of(0), tile(0)]).wait()

    def w1_tile(p, t):
        j, s = tile_of(t)
        wait_all(w1_copies(t % 2, w1t.at[0, :, tile(0)], w1b.at[0, :, tile(0)]))

        def one(gl):
            g = 2 * p + gl

            def project():
                h = (jnp.dot(zj[gl, :, :WID], wbuf[t % 2, :WID], preferred_element_type=F32)
                     + jnp.dot(zj[gl, :, WID:2 * WID], wbuf[t % 2, WID:2 * WID], preferred_element_type=F32))
                return h.astype(BF16)

            @pl.when((t > 0) & (t != 24))
            def _():
                h_done(gl)

            @pl.when(j < 2)
            def _():
                h = project().astype(F32)
                gain = gains[j]
                for k in range(2):
                    part = h[:, k * DH:(k + 1) * DH]
                    part = part - jnp.mean(part, -1, keepdims=True)
                    var = jnp.mean(part * part, -1, keepdims=True)
                    ptile[gl, :, k * DH:(k + 1) * DH] = (part * lax.rsqrt(var + EPS) * gain).astype(BF16)

            @pl.when(j == 2)
            def _():
                ptile[gl] = project()

            @pl.when(j > 2)
            def _():
                h = project().astype(F32) + ub[s, :, tile(j - 3)]
                ptile[gl] = (0.5 * h * (1.0 + lax.erf(h * 0.7071067811865476))).astype(BF16)

            @pl.when(j <= 2)
            def _():
                h_store(gl, qkv.at[j, s, rows_of(g)]).start()

            @pl.when(j > 2)
            def _():
                h_store(gl, jb.at[rows_of(g), pl.ds(pl.multiple_of(s * JB + (j - 2) * TN, TN), TN)]).start()

        loop(0, 2, one)

    def a_loads(p, w, slot):
        g, s = 2 * p + w // NS, w % NS
        return [pltpu.make_async_copy(qkv.at[i, s, rows_of(g)], abuf.at[slot, i], asem.at[slot, i]) for i in range(3)]

    def a_store(p, w, slot):
        g, s = 2 * p + w // NS, w % NS
        return h_store(slot, jb.at[rows_of(g), pl.ds(pl.multiple_of(s * JB, TN), TN)])

    def attention(p):
        units = 2 * NS
        start_all(a_loads(p, 0, 0))

        def unit(w):
            slot = w % 2

            @pl.when(w + 1 < units)
            def _():
                start_all(a_loads(p, w + 1, 1 - slot))

            wait_all(a_loads(p, w, slot))

            @pl.when(w >= 2)
            def _():
                a_store(p, w - 2, slot).wait()

            def images(i):
                for ii in range(2):
                    at = pl.ds(pl.multiple_of((2 * i + ii) * SEQ, SEQ), SEQ)
                    for k in range(2):
                        cols = slice(k * DH, (k + 1) * DH)
                        q, kk, v = abuf[slot, 0, at, cols], abuf[slot, 1, at, cols], abuf[slot, 2, at, cols]
                        lg = lax.dot_general(q, kk, (((1,), (1,)), ((), ())), preferred_element_type=F32) * (DH ** -0.5)
                        e = jnp.exp(lg - jnp.max(lg, -1, keepdims=True))
                        prob = (e / jnp.sum(e, -1, keepdims=True)).astype(BF16)
                        ptile[slot, at, cols] = jnp.dot(prob, v, preferred_element_type=F32).astype(BF16)

            loop(0, M // SEQ // 2, images)
            a_store(p, w, slot).start()

        loop(0, units, unit)
        a_store(p, units - 2, 0).wait()
        a_store(p, units - 1, 1).wait()

    def w2_slot(m, half):
        return 2 * ((m + 1) % 2) + half

    def w2_dst(m, s):
        return wbuf.at[w2_slot(m, s // 2), pl.ds((s % 2) * JB, JB)]

    def fetch2(m):
        n = m // 2
        e = m % 2

        @pl.when(e == 0)
        def _():
            v_d(n).wait_recv()
            v_h(n).wait_recv()
            for s in range(NS):
                pltpu.make_async_copy(w2n.at[s, :, tile(n)], w2_dst(m, s), w2sem.at[e, s]).start()

        @pl.when(e == 1)
        def _():
            v_b(n).wait_recv()
            v_g(n).wait_recv()
            for p in range(2):
                to = wbuf.at[w2_slot(m, 0), PART_ROWS[p]]
                pltpu.make_async_copy(w_out.at[out_row(p, y), tile(n)], to, w2sem.at[e, 4 * p]).start()
            for s in range(1, NS):
                pltpu.make_async_copy(w2y.at[s - 1, :, tile(n)], w2_dst(m, s), w2sem.at[e, s]).start()

    def arrive2(m):
        e = m % 2

        @pl.when(e == 0)
        def _():
            for s in range(NS):
                pltpu.make_async_copy(w2n.at[s, :, tile(0)], w2_dst(m, s), w2sem.at[e, s]).wait()

        @pl.when(e == 1)
        def _():
            for p in range(2):
                to = wbuf.at[w2_slot(m, 0), PART_ROWS[p]]
                pltpu.make_async_copy(w2n.at[0, PART_ROWS[p], tile(0)], to, w2sem.at[e, 4 * p]).wait()
            for s in range(1, NS):
                pltpu.make_async_copy(w2n.at[s, :, tile(0)], w2_dst(m, s), w2sem.at[e, s]).wait()

    def hand_c(n):
        v_c(n).wait_recv()
        v_d(n).start()
        v_f(n).start()

    def hand_e(n):
        v_e(n).wait_recv()
        v_g(n).start()

    def hand_f(n):
        v_f(n).wait_recv()
        v_h(n).start()

    hands = {5: [lambda: hand_c(0)], 8: [lambda: hand_e(0)], 11: [lambda: hand_c(1), lambda: v_e(2).start()],
             14: [lambda: hand_e(1), lambda: hand_f(0)], 17: [lambda: hand_c(2), lambda: v_e(3).start()],
             20: [lambda: hand_f(1)], 23: [lambda: hand_c(3)]}

    def w1_pass(p):
        layer_norm(2 * p)
        layer_norm(2 * p + 1)

        @pl.when(p == 0)
        def _():
            fetch1(p, 0)

        def step(t):
            @pl.when(t == 24)
            def _():
                h_done(0)
                h_done(1)
                attention(p)

            def fetch_next():
                @pl.when(t + 1 < NT)
                def _():
                    fetch1(p, t + 1)

                @pl.when((t + 1 == NT) & (p == 0))
                def _():
                    fetch1(1, 0)

                @pl.when((t + 1 == NT) & (p == 1))
                def _():
                    fetch2(0)

            @pl.when(p == 1)
            def _():
                fetch_next()

            w1_tile(p, t)

            @pl.when(p == 0)
            def _():
                fetch_next()

            for at, todo in hands.items():
                @pl.when((p == 1) & (t == at))
                def _(todo=todo):
                    for one in todo:
                        one()

        loop(0, NT, step)
        h_done(0)
        h_done(1)

    loop(0, 2, w1_pass)

    def load(e, i, src):
        return pltpu.make_async_copy(src, sv.at[e, i], vsem.at[e, i])

    def fin_loads(k, n, e):
        at = (part_rows(k), tile(n))
        return [load(e, 0, pa.at[at]), load(e, 1, ry.at[at]), load(e, 2, tok.at[own_out(k), tile(n)])]

    def fin_store(k, n, e):
        return pltpu.make_async_copy(sv.at[e, 3], out.at[own_out(k), tile(n)], vsem.at[e, 3])

    def tail_store(k, e):
        def to(ref):
            return pltpu.make_async_copy(sv.at[e, 3], ref, vsem.at[e, 4])

        @pl.when(k < NK - 1)
        def _():
            to(tail.at[part_rows(k - NL)]).start()

        @pl.when(k == NK - 1)
        def _():
            to(tail2).start()

    def is_last(k, n):
        return (n == NN - 1) & (k == NL - 1)

    def o_rec():
        at = out.at[own_out(NL - 1), LAST]
        return remote(at, rec, x_s, x_r.at[NL - 1, NN - 1], dev_x)

    def is_tail(k, n):
        return (n == NN - 1) & (k >= NL)

    def fin_load(k, n, e):
        @pl.when(k % 2 == 0)
        def _():
            o_y(k // 2, n).wait_recv()

        start_all(fin_loads(k, n, e))

    def fin_do(k, n, e):
        wait_all(fin_loads(k, n, e))
        total = sv[e, 0].astype(F32) + sv[e, 1].astype(F32) + (ob[0, :, tile(n)] + ob[1, :, tile(n)]) + sv[e, 2].astype(F32)
        sv[e, 3] = total.astype(BF16)
        fin_store(k, n, e).start()

        @pl.when(is_tail(k, n))
        def _():
            tail_store(k, e)

    def fin_send(k, n, e):
        fin_store(k, n, e).wait()

        @pl.when(is_tail(k, n))
        def _():
            pltpu.make_async_copy(sv.at[e, 3], tail2, vsem.at[e, 4]).wait()

        @pl.when(is_last(k, n))
        def _():
            o_rec().start()

        @pl.when(jnp.logical_not(is_tail(k, n) | is_last(k, n)))
        def _():
            o_x(k, n).start()

        o_c(k, n).start()

    def hand_out(k, n):
        o_x(k, n).wait_recv()
        o_f(k, n).start()

    STEPS = 2 * NN * NK

    def service(v):
        f = v - 11
        n, i = f // 16, f % 16

        @pl.when((f >= 0) & (i >= 2) & (i < NK + 2))
        def _():
            fin_send(i - 2, n, v % 2)

        @pl.when((f >= 0) & (i < NK))
        def _():
            fin_load(i, n, v % 2)

        @pl.when((f >= 0) & (i >= 1) & (i < NK + 1))
        def _():
            fin_do(i - 1, n, (v + 1) % 2)

        for n, at in enumerate((33, 49)):
            @pl.when((v >= at) & (v < at + NK))
            def _(n=n, at=at):
                hand_out(v - at, n)

    def j_copy(v):
        g, half = (v % 8) // 2, v % 2
        src = jb.at[rows_of(g), pl.ds(pl.multiple_of(half * KH, KH), KH)]
        return pltpu.make_async_copy(src, zj.at[half], jsem.at[half])

    def p_copy(m, g):
        n, slot = m // 2, g % 2
        return n, lambda ref: pltpu.make_async_copy(ptile.at[slot], ref.at[rows_of(g), tile(n)], psem.at[slot])

    def p_start(m, g):
        _, to = p_copy(m, g)

        @pl.when(m % 2 == 0)
        def _():
            to(pb).start()

        @pl.when(m % 2 == 1)
        def _():
            to(pa).start()

    def p_finish(m, g):
        n, to = p_copy(m, g)

        @pl.when(m % 2 == 0)
        def _():
            to(pb).wait()
            o_y(g, n).start()

        @pl.when(m % 2 == 1)
        def _():
            to(pa).wait()

    j_copy(0).start()

    def w2_tile(m):
        for at, todo in enumerate((lambda: hand_e(2), lambda: hand_f(2), lambda: hand_e(3), lambda: hand_f(3))):
            @pl.when(m == at)
            def _(todo=todo):
                todo()

        @pl.when(m + 1 < 2 * NN)
        def _():
            fetch2(m + 1)

        arrive2(m)

        def one(g):
            v = m * 2 * GROUPS + 2 * g
            j_copy(v + 1).start()
            j_copy(v).wait()
            acc[...] = jnp.dot(zj[0], wbuf[w2_slot(m, 0)], preferred_element_type=F32)

            @pl.when(g > 0)
            def _():
                p_finish(m, g - 1)

            service(v)

            @pl.when(v + 2 < STEPS)
            def _():
                j_copy(v + 2).start()

            j_copy(v + 1).wait()
            ptile[g % 2] = (acc[...] + jnp.dot(zj[1], wbuf[w2_slot(m, 1)], preferred_element_type=F32)).astype(BF16)
            p_start(m, g)
            service(v + 1)

        loop(0, GROUPS, one)
        p_finish(m, GROUPS - 1)

    loop(0, 2 * NN, w2_tile)

    loop(STEPS, STEPS + 5, service)
    loop(0, NK, lambda k: hand_out(k, 2))

    for one in small_far:
        one.wait_send()
    remote(toth, toth, t_s, t_s, dev_y).wait_send()
    for kind in range(C + NJ):
        remote(bots[OWN], bots[OWN], w_s.at[kind], w_s.at[kind], dev_y).wait_send()
    for kind in range(NS):
        remote(theirs[OWN], theirs[OWN], d_s.at[kind], d_s.at[kind], dev_y).wait_send()
    for kind in range(NS - 1):
        remote(theirs[OWN], theirs[OWN], e_s.at[kind], e_s.at[kind], dev_y).wait_send()
    remote(pb, pb, y_s, y_s, dev_y).wait_send()
    mine_out = out.at[pl.ds(row0, ROWS)]
    near_out = remote(mine_out, mine_out, o_s.at[0], o_r.at[0], dev_c)
    near_out.wait_send()
    near_out.wait_recv()

    loop(0, NL - 1, lambda k: hand_out(k, NN - 1))
    crossed = ROWS - (NK - NL) * HALF // NN
    handed = out.at[pl.ds(row0, crossed - HALF // NN)]
    sent = out.at[pl.ds(row0, crossed)]
    far_out = remote(handed, handed, o_s.at[1], o_r.at[1], dev_c)
    far_out.wait_send()
    far_out.wait_recv()
    o_rec().wait_recv()
    remote(sent, sent, x_s, x_s, dev_x).wait_send()


def copy_kernel(lo, hi, src, *rest):
    more, (dst, buf, sem) = rest[1:-3], rest[-3:]
    slots = buf.shape[0]
    x = lax.axis_index("mx") // 2

    def moves(i):
        first = (x + i // (2 * NK)) % 2
        rows = pl.ds(pl.multiple_of(first_row(first, (i // NK) % 2) + (i % NK) * HALF, HALF), HALF)
        late = i >= 2 * NK and i % NK >= NL
        cols = pl.ds(0, WID - TN if late else WID)
        k = (i - lo) % slots
        return (pltpu.make_async_copy(src.at[rows, cols], buf.at[k, :, cols], sem.at[0, k]),
                pltpu.make_async_copy(buf.at[k, :, cols], dst.at[rows, cols], sem.at[1, k]))

    def one_more(i, ref):
        c = (lax.axis_index("mx") + i) % 2
        rows = pl.ds(pl.multiple_of(first_row(1 - x, c) + (NL - 1) * HALF, HALF), HALF)
        cols = LAST
        k = (hi - lo + i) % slots
        return (pltpu.make_async_copy(ref, buf.at[k, :, cols], sem.at[0, k]),
                pltpu.make_async_copy(buf.at[k, :, cols], dst.at[rows, cols], sem.at[1, k]))

    every = [moves(i) for i in range(lo, hi)] + [one_more(i, ref) for i, ref in enumerate(more)]
    ahead, count = 12, len(every)
    for i in range(count + ahead):
        if i < count:
            if i >= slots:
                every[i - slots][1].wait()
            every[i][0].start()
        if i >= ahead:
            every[i - ahead][0].wait()
            every[i - ahead][1].start()
    for _, store in every[-min(slots, count):]:
        store.wait()


def tail_kernel(lo, hi, others, base, *rest):
    pieces, (out, sem) = rest[:-2], rest[-2:]
    mi = lax.axis_index("mx")
    moves = []
    for i, (other, piece) in enumerate(zip(others, pieces)):
        at = pl.multiple_of(first_row(1 - mi // 2, (mi + other) % 2) + lo * HALF, HALF)
        moves.append(pltpu.make_async_copy(piece, out.at[pl.ds(at, (hi - lo) * HALF), LAST], sem.at[i]))
    start_all(moves)
    wait_all(moves)


def solution(mesh):
    hbm = pl.BlockSpec(memory_space=pltpu.HBM)

    def dma(*shape):
        return pltpu.SemaphoreType.DMA(shape)

    def local_layer(tokens, ln_scale, w_in, mlp_bias, q_scale, k_scale, w_out, attn_out_bias, mlp_out_bias):
        tok = tokens.reshape(-1, WID)
        vecs = [v.reshape(-1, LANES) for v in (ln_scale, mlp_bias, q_scale, k_scale, attn_out_bias, mlp_out_bias)]
        of = lambda *shape: jax.ShapeDtypeStruct(shape, BF16)
        shapes = [of(*tok.shape), *[of((hi - lo) * HALF, TN) for lo, hi in TAILS], of(HALF, TN), of(ROWS, WID), of(3, WID, NJ * TN), of(4, WID, NJ * TN), of(3, JB, WID), of(4, JB, WID),
                  of(3, NS, ROWS, TN), of(ROWS, NS * JB), of(ROWS, WID), of(ROWS, WID), of(ROWS, WID)]
        flops = 2 * ROWS * (2 * WID * NT * TN + NS * JB * 2 * WID)
        pairs = [(), (NK,), (7,), (7, NJ), (3,), (3, NN), (NS,), (NS, NN), (), (GROUPS, NN), (), (NK, NN), (2,), (2,), (NS,), (NS,)]
        res = pl.pallas_call(
            kernel,
            out_shape=shapes,
            in_specs=[hbm] * 9,
            out_specs=[hbm] * len(shapes),
            scratch_shapes=[
                pltpu.VMEM((2, M, KH), BF16),
                pltpu.VMEM((4, KH, TN), BF16),
                pltpu.VMEM((2, M, TN), BF16),
                pltpu.VMEM((M, TN), F32),
                pltpu.VMEM((2, 3, M, TN), BF16),
                pltpu.VMEM((2, 4, HALF, TN), BF16),
                pltpu.VMEM((2, 2, LN, WID), BF16),
                pltpu.VMEM((2, 1, WID), F32),
                pltpu.VMEM((NS, 1, UNITS // 2), F32),
                pltpu.VMEM((2, 1, DH), F32),
                pltpu.VMEM((2, 1, WID), F32),
                pltpu.VMEM((2 * NS, WID // LANES, LANES), BF16),
                pltpu.VMEM((2, DH // LANES, LANES), BF16),
                dma(2, 2), dma(2, 5), dma(2), dma(2), dma(2, 3), dma(2, 5), dma(2, 2), dma(6),
            ] + [dma(*shape) for shape in pairs],
            compiler_params=pltpu.CompilerParams(collective_id=0, has_side_effects=True, vmem_limit_bytes=63 * 2**20),
            cost_estimate=cost(flops, 2**30),
            name="layer",
        )(tok, w_in, w_out, *vecs)
        base = res[0]
        over_x = [(i, i ^ 2) for i in range(NS)]
        over_core = [(i, i ^ 1) for i in range(NS)]
        far = []
        for own in res[1:3]:
            far.append(lax.ppermute(own, 'mx', over_x))

        def put(lo, hi, *arrays):
            return pl.pallas_call(
                functools.partial(copy_kernel, lo, hi),
                out_shape=of(*tok.shape),
                in_specs=[hbm] * len(arrays),
                out_specs=hbm,
                input_output_aliases={i: 0 for i in range(1, min(2, len(arrays)))},
                scratch_shapes=[pltpu.VMEM((16, HALF, WID), BF16), dma(2, 16)],
                compiler_params=pltpu.CompilerParams(vmem_limit_bytes=40 * 2**20),
                cost_estimate=cost((hi - lo) * 10**9, (hi - lo) * 4 * HALF * WID),
                name="place",
            )(*arrays)

        def put_last(base, lo, hi, others, *pieces):
            return pl.pallas_call(
                functools.partial(tail_kernel, lo, hi, others),
                out_shape=of(*tok.shape),
                in_specs=[hbm] + [pl.BlockSpec(memory_space=pltpu.VMEM)] * len(pieces),
                out_specs=hbm,
                input_output_aliases={0: 0},
                scratch_shapes=[dma(2)],
                compiler_params=pltpu.CompilerParams(vmem_limit_bytes=8 * 2**20),
                cost_estimate=cost(10**9, 8 * pieces[0].size),
                name="place_last",
            )(base, *pieces)

        results, rec = base, res[3]
        rec_near = lax.ppermute(rec, 'mx', over_core)
        base = put(0, SPLIT, results)
        for (lo, hi), piece in zip(TAILS, far):
            piece, base = lax.optimization_barrier((piece, base))
            farther = lax.ppermute(piece, 'mx', over_core)
            if lo == NL:
                base = put(SPLIT, 4 * NK, results, base, rec, rec_near)
                base = put_last(base, lo, hi, (0, 1), piece, farther)
            else:
                base = put_last(base, lo, hi, (0,), piece)
                base = put_last(base, lo, hi, (1,), farther)
        return base.reshape(tokens.shape)

    specs_in = (P('dp', None, 'my'), P('my'), P('my', 'mx'), P('mx'), P(), P(), P('mx', 'my'), P('my'), P('my'))

    return jax.shard_map(local_layer, mesh=mesh, in_specs=specs_in, out_specs=P('dp', None, 'my'), check_vma=False)
```

```python
import functools

import jax
import jax.numpy as jnp
from jax import lax
from jax.experimental import pallas as pl
from jax.experimental.pallas import tpu as pltpu
from jax.sharding import PartitionSpec as P


MESH = pl.DeviceIdType.MESH
F32, BF16 = jnp.float32, jnp.bfloat16

SEQ, DH, WID = 256, 256, 2048
M, GROUPS = 1024, 4
ROWS = M * GROUPS
HALF = M // 2
TN = 512
QKV, UNITS = 1024, 4096
NS = 4
NJ = 7
NT = NS * NJ
NN = WID // TN
JB = 5 * TN
KH = 2 * JB
LANES = 128
LN = 128
EPS = 1e-6
NK = 2 * GROUPS
NL = NK // 2
TAILS = ((NL, NK - 1), (NK - 1, NK))
SPLIT = 4 * NK - 2


def in_col(j, side):
    mlp = (j + 1) // 4
    at = (1 - mlp) * (QKV * j + (QKV // 2) * side) + mlp * (3 * QKV + (UNITS // 2) * side + TN * (j - 3))
    return pl.ds(pl.multiple_of(at, TN), TN)


def out_row(part, side):
    if part == 0:
        return pl.ds(pl.multiple_of((QKV // 2) * side, QKV // 2), TN)
    return pl.ds(pl.multiple_of(QKV + (UNITS // 2) * side, QKV), UNITS // 2)


LAST = pl.ds((NN - 1) * TN, TN)
PART_ROWS = (pl.ds(0, TN), pl.ds(TN, JB - TN))


def first_row(x, c):
    return pl.multiple_of((2 * x + c) * ROWS, ROWS)


def cost(flops, size):
    return pl.CostEstimate(flops=flops, bytes_accessed=size, transcendentals=0)


def tile(n):
    return pl.ds(pl.multiple_of(n * TN, TN), TN)


def rows_of(g):
    return pl.ds(pl.multiple_of(g * M, M), M)


def tile_of(t):
    a, b = (t + 24) // 28, t // 24
    j = (1 - a) * (t // 2) + (a - b) * (t // 4 + 1 - 2 * ((t % 4) // 2)) + b * (t // 2 - 7)
    s = (1 - a) * (t % 2) + (a - b) * (t % 4) + b * (2 + t % 2)
    return j, s


def loop(lo, hi, body):
    def run(i, carry):
        body(i)
        return carry

    lax.fori_loop(lo, hi, run, 0)


def start_all(copies):
    for one in copies:
        one.start()


def wait_all(copies):
    for one in copies:
        one.wait()


def kernel(tok, w_in, w_out, lns, mb, qs, ks, ab, bb,
           out, tail, tail2, rec, toth, w1t, w1b, w2y, w2n, qkv, jb, pa, pb, ry,
           zj, wbuf, ptile, acc, abuf, sv, lbuf, sc, ub, gains, ob, raw, raw2,
           w1sem, w2sem, jsem, psem, asem, vsem, lsem, csem,
           t_s, t_r, w_s, w_r, e_s, e_r, d_s, d_r, y_s, y_r, x_s, x_r, o_s, o_r, m_s, m_r):
    y = lax.axis_index("my")
    mi = lax.axis_index("mx")
    x, c = mi // 2, mi % 2
    dev_y = {"my": 1 - y, "mx": mi}
    dev_x = {"my": y, "mx": 2 * (1 - x) + c}
    dev_c = {"my": y, "mx": 2 * x + 1 - c}
    dev_d = {"my": y, "mx": 2 * (1 - x) + 1 - c}
    row0, row0_x = first_row(x, c), first_row(1 - x, c)

    barrier = pltpu.get_barrier_semaphore()
    for dev in (dev_y, dev_x, dev_c, dev_d):
        pl.semaphore_signal(barrier, inc=1, device_id=dev, device_id_type=MESH)
    pl.semaphore_wait(barrier, 4)

    def remote(src, dst, ss, rs, dev):
        return pltpu.make_async_remote_copy(src_ref=src, dst_ref=dst, send_sem=ss, recv_sem=rs, device_id=dev, device_id_type=MESH)

    def t_dir(k):
        src = tok.at[pl.ds(pl.multiple_of(row0 + k * HALF, HALF), HALF)]
        return remote(src, toth.at[pl.ds(pl.multiple_of(k * HALF, HALF), HALF)], t_s, t_r.at[k], dev_y)

    C, B, D, E, F, G, H = range(7)

    def w_own(kind, j, side, dst, dev):
        return remote(w_in.at[:, in_col(j, side)], dst.at[:, tile(j)], w_s.at[kind], w_r.at[kind, j], dev)

    def w_pass(kind, j, src, dst, dev):
        return remote(src.at[:, tile(j)], dst.at[:, tile(j)], w_s.at[kind], w_r.at[kind, j], dev)

    tops = [None] + [w1t.at[i] for i in range(NS - 1)]
    bots = [w1b.at[i] for i in range(NS)]
    OWN, CORE, FAR, FAR_CORE = range(NS)
    w_c = lambda j: w_own(C, j, 1 - y, bots[OWN], dev_y)
    w_b = lambda j: w_own(B, j, y, tops[CORE], dev_c)
    w_d = lambda j: w_pass(D, j, bots[OWN], bots[CORE], dev_c)
    w_e = lambda j: w_own(E, j, y, tops[FAR], dev_x)
    w_f = lambda j: w_pass(F, j, bots[OWN], bots[FAR], dev_x)
    w_g = lambda j: w_pass(G, j, tops[FAR], tops[FAR_CORE], dev_c)
    w_h = lambda j: w_pass(H, j, bots[FAR], bots[FAR_CORE], dev_c)

    class Two:
        def __init__(self, kind, n, side, dst, dev):
            self.copies = [remote(w_out.at[out_row(p, side), tile(n)], dst.at[rows, tile(n)], e_s.at[kind], e_r.at[kind, n], dev)
                           for p, rows in enumerate(PART_ROWS)]
            self.both = remote(dst.at[:, tile(n)], dst.at[:, tile(n)], e_s.at[kind], e_r.at[kind, n], dev)

        def start(self):
            start_all(self.copies)

        def wait_recv(self):
            self.both.wait_recv()

    def v_pass(kind, n, src, dst, dev):
        return remote(src.at[:, tile(n)], dst.at[:, tile(n)], d_s.at[kind], d_r.at[kind, n], dev)

    mine = [None] + [w2y.at[i] for i in range(NS - 1)]
    theirs = [w2n.at[i] for i in range(NS)]
    v_c = lambda n: Two(C, n, 1 - y, theirs[OWN], dev_y)
    v_b = lambda n: Two(B, n, y, mine[CORE], dev_c)
    v_e = lambda n: Two(D, n, y, mine[FAR], dev_x)
    v_d = lambda n: v_pass(C, n, theirs[OWN], theirs[CORE], dev_c)
    v_f = lambda n: v_pass(B, n, theirs[OWN], theirs[FAR], dev_x)
    v_g = lambda n: v_pass(D, n, mine[FAR], mine[FAR_CORE], dev_c)
    v_h = lambda n: v_pass(E, n, theirs[FAR], theirs[FAR_CORE], dev_c)

    def o_y(g, n):
        return remote(pb.at[rows_of(g), tile(n)], ry.at[rows_of(g), tile(n)], y_s, y_r.at[g, n], dev_y)

    def part_rows(k):
        return pl.ds(pl.multiple_of(k * HALF, HALF), HALF)

    def own_out(k):
        return pl.ds(pl.multiple_of(row0 + k * HALF, HALF), HALF)

    def o_x(k, n):
        at = out.at[own_out(k), tile(n)]
        return remote(at, at, x_s, x_r.at[k, n], dev_x)

    def o_c(k, n):
        at = out.at[own_out(k), tile(n)]
        return remote(at, at, o_s.at[0], o_r.at[0], dev_c)

    def o_f(k, n):
        at = out.at[pl.ds(pl.multiple_of(row0_x + k * HALF, HALF), HALF), tile(n)]
        return remote(at, at, o_s.at[1], o_r.at[1], dev_c)

    rows = WID // LANES
    few = DH // LANES
    my_units = mb.at[pl.ds(pl.multiple_of(y * rows, rows), rows)]
    small_far = [remote(src, raw.at[i], m_s.at[i], m_r.at[i], dev) for i, (src, dev) in enumerate((
        (lns, dev_y), (my_units, dev_c), (my_units, dev_x), (my_units, dev_d)))]
    small = [pltpu.make_async_copy(src, dst, csem.at[i]) for i, (src, dst) in enumerate((
        (lns, raw.at[NS]), (my_units, raw.at[NS + 1]), (ab, raw.at[NS + 2]), (bb, raw.at[NS + 3]), (qs, raw2.at[0]), (ks, raw2.at[1])))]

    def spread(src, dst, count):
        for i in range(count):
            dst[:, i * LANES:(i + 1) * LANES] = src[i:i + 1].astype(F32)

    loop(0, NS, lambda j: w_e(j).start())
    start_all(small_far)
    loop(0, NS, lambda k: t_dir(k).start())
    loop(0, NJ, lambda j: w_c(j).start())
    loop(NS, NK, lambda k: t_dir(k).start())
    loop(0, NN, lambda n: v_c(n).start())
    w_e(NS).start()
    w_e(NS + 1).start()
    loop(0, NJ, lambda j: w_b(j).start())
    loop(0, NN, lambda n: v_b(n).start())
    start_all(small)
    wait_all(small)
    for one in small_far:
        one.wait_recv()
    for i, dst in enumerate((sc.at[1], ub.at[CORE], ub.at[FAR], ub.at[FAR_CORE], sc.at[0], ub.at[OWN], ob.at[0], ob.at[1])):
        spread(raw.at[i], dst, rows)
    for i in range(2):
        spread(raw2.at[i], gains.at[i], few)

    def l_copies(g, i, slot):
        at = pl.multiple_of(g * M + i * LN, LN)
        return (
            pltpu.make_async_copy(tok.at[pl.ds(pl.multiple_of(row0 + at, LN), LN)], lbuf.at[slot, 0], lsem.at[slot, 0]),
            pltpu.make_async_copy(toth.at[pl.ds(at, LN)], lbuf.at[slot, 1], lsem.at[slot, 1]),
        )

    def layer_norm(g):
        steps = M // LN
        t_dir(2 * g).wait_recv()
        start_all(l_copies(g, 0, 0))

        def rows(i):
            slot = i % 2

            @pl.when(i == steps // 2 - 1)
            def _():
                t_dir(2 * g + 1).wait_recv()

            @pl.when(i + 1 < steps)
            def _():
                start_all(l_copies(g, i + 1, 1 - slot))

            wait_all(l_copies(g, i, slot))
            step = 64

            def part(k):
                at = pl.ds(pl.multiple_of(k * step, step), step)
                a, b = lbuf[slot, 0, at].astype(F32), lbuf[slot, 1, at].astype(F32)
                mean = (jnp.sum(a, -1, keepdims=True) + jnp.sum(b, -1, keepdims=True)) * (0.5 / WID)
                a, b = a - mean, b - mean
                var = (jnp.sum(a * a, -1, keepdims=True) + jnp.sum(b * b, -1, keepdims=True)) * (0.5 / WID)
                inv = lax.rsqrt(var + EPS)
                to = pl.ds(pl.multiple_of(i * LN + k * step, step), step)
                zj[g % 2, to, :WID] = (a * inv * sc[0]).astype(BF16)
                zj[g % 2, to, WID:2 * WID] = (b * inv * sc[1]).astype(BF16)

            loop(0, LN // step, part)

        loop(0, steps, rows)

    def w1_copies(slot, top, bottom):
        return (
            pltpu.make_async_copy(top, wbuf.at[slot, :WID], w1sem.at[slot, 0]),
            pltpu.make_async_copy(bottom, wbuf.at[slot, WID:2 * WID], w1sem.at[slot, 1]),
        )

    def fetch1(p, t):
        j, s = tile_of(t)
        slot = t % 2

        @pl.when(p == 0)
        def _():
            @pl.when(s == 0)
            def _():
                w_c(j).wait_recv()
                w_d(j).start()
                w_f(j).start()

                @pl.when(j == 2)
                def _():
                    w_e(NJ - 1).start()

                @pl.when(j == NJ - 1)
                def _():
                    v_e(0).start()
                    v_e(1).start()

            @pl.when(s == 1)
            def _():
                w_b(j).wait_recv()
                w_d(j).wait_recv()

            @pl.when(s == 2)
            def _():
                w_e(j).wait_recv()
                w_g(j).start()
                w_f(j).wait_recv()
                w_h(j).start()

            @pl.when(s == 3)
            def _():
                w_g(j).wait_recv()
                w_h(j).wait_recv()

        @pl.when(s == 0)
        def _():
            start_all(w1_copies(slot, w_in.at[:, in_col(j, y)], w1b.at[0, :, tile(j)]))

        @pl.when(s > 0)
        def _():
            start_all(w1_copies(slot, w1t.at[s - 1, :, tile(j)], w1b.at[s, :, tile(j)]))

    def h_store(slot, dst):
        return pltpu.make_async_copy(ptile.at[slot], dst, psem.at[slot])

    def h_done(slot):
        h_store(slot, pb.at[rows_of(0), tile(0)]).wait()

    def w1_tile(p, t):
        j, s = tile_of(t)
        wait_all(w1_copies(t % 2, w1t.at[0, :, tile(0)], w1b.at[0, :, tile(0)]))

        def one(gl):
            g = 2 * p + gl

            def project():
                h = (jnp.dot(zj[gl, :, :WID], wbuf[t % 2, :WID], preferred_element_type=F32)
                     + jnp.dot(zj[gl, :, WID:2 * WID], wbuf[t % 2, WID:2 * WID], preferred_element_type=F32))
                return h.astype(BF16)

            @pl.when((t > 0) & (t != 24))
            def _():
                h_done(gl)

            @pl.when(j < 2)
            def _():
                h = project().astype(F32)
                gain = gains[j]
                for k in range(2):
                    part = h[:, k * DH:(k + 1) * DH]
                    part = part - jnp.mean(part, -1, keepdims=True)
                    var = jnp.mean(part * part, -1, keepdims=True)
                    ptile[gl, :, k * DH:(k + 1) * DH] = (part * lax.rsqrt(var + EPS) * gain).astype(BF16)

            @pl.when(j == 2)
            def _():
                ptile[gl] = project()

            @pl.when(j > 2)
            def _():
                h = project().astype(F32) + ub[s, :, tile(j - 3)]
                ptile[gl] = (0.5 * h * (1.0 + lax.erf(h * 0.7071067811865476))).astype(BF16)

            @pl.when(j <= 2)
            def _():
                h_store(gl, qkv.at[j, s, rows_of(g)]).start()

            @pl.when(j > 2)
            def _():
                h_store(gl, jb.at[rows_of(g), pl.ds(pl.multiple_of(s * JB + (j - 2) * TN, TN), TN)]).start()

        loop(0, 2, one)

    def a_loads(p, w, slot):
        g, s = 2 * p + w // NS, w % NS
        return [pltpu.make_async_copy(qkv.at[i, s, rows_of(g)], abuf.at[slot, i], asem.at[slot, i]) for i in range(3)]

    def a_store(p, w, slot):
        g, s = 2 * p + w // NS, w % NS
        return h_store(slot, jb.at[rows_of(g), pl.ds(pl.multiple_of(s * JB, TN), TN)])

    def attention(p):
        units = 2 * NS
        start_all(a_loads(p, 0, 0))

        def unit(w):
            slot = w % 2

            @pl.when(w + 1 < units)
            def _():
                start_all(a_loads(p, w + 1, 1 - slot))

            wait_all(a_loads(p, w, slot))

            @pl.when(w >= 2)
            def _():
                a_store(p, w - 2, slot).wait()

            def images(i):
                for ii in range(2):
                    at = pl.ds(pl.multiple_of((2 * i + ii) * SEQ, SEQ), SEQ)
                    for k in range(2):
                        cols = slice(k * DH, (k + 1) * DH)
                        q, kk, v = abuf[slot, 0, at, cols], abuf[slot, 1, at, cols], abuf[slot, 2, at, cols]
                        lg = lax.dot_general(q, kk, (((1,), (1,)), ((), ())), preferred_element_type=F32) * (DH ** -0.5)
                        e = jnp.exp(lg - jnp.max(lg, -1, keepdims=True))
                        prob = (e / jnp.sum(e, -1, keepdims=True)).astype(BF16)
                        ptile[slot, at, cols] = jnp.dot(prob, v, preferred_element_type=F32).astype(BF16)

            loop(0, M // SEQ // 2, images)
            a_store(p, w, slot).start()

        loop(0, units, unit)
        a_store(p, units - 2, 0).wait()
        a_store(p, units - 1, 1).wait()

    def w2_slot(m, half):
        return 2 * ((m + 1) % 2) + half

    def w2_dst(m, s):
        return wbuf.at[w2_slot(m, s // 2), pl.ds((s % 2) * JB, JB)]

    def fetch2(m):
        n = m // 2
        e = m % 2

        @pl.when(e == 0)
        def _():
            v_d(n).wait_recv()
            v_h(n).wait_recv()
            for s in range(NS):
                pltpu.make_async_copy(w2n.at[s, :, tile(n)], w2_dst(m, s), w2sem.at[e, s]).start()

        @pl.when(e == 1)
        def _():
            v_b(n).wait_recv()
            v_g(n).wait_recv()
            for p in range(2):
                to = wbuf.at[w2_slot(m, 0), PART_ROWS[p]]
                pltpu.make_async_copy(w_out.at[out_row(p, y), tile(n)], to, w2sem.at[e, 4 * p]).start()
            for s in range(1, NS):
                pltpu.make_async_copy(w2y.at[s - 1, :, tile(n)], w2_dst(m, s), w2sem.at[e, s]).start()

    def arrive2(m):
        e = m % 2

        @pl.when(e == 0)
        def _():
            for s in range(NS):
                pltpu.make_async_copy(w2n.at[s, :, tile(0)], w2_dst(m, s), w2sem.at[e, s]).wait()

        @pl.when(e == 1)
        def _():
            for p in range(2):
                to = wbuf.at[w2_slot(m, 0), PART_ROWS[p]]
                pltpu.make_async_copy(w2n.at[0, PART_ROWS[p], tile(0)], to, w2sem.at[e, 4 * p]).wait()
            for s in range(1, NS):
                pltpu.make_async_copy(w2n.at[s, :, tile(0)], w2_dst(m, s), w2sem.at[e, s]).wait()

    def hand_c(n):
        v_c(n).wait_recv()
        v_d(n).start()
        v_f(n).start()

    def hand_e(n):
        v_e(n).wait_recv()
        v_g(n).start()

    def hand_f(n):
        v_f(n).wait_recv()
        v_h(n).start()

    hands = {5: [lambda: hand_c(0)], 8: [lambda: hand_e(0)], 11: [lambda: hand_c(1), lambda: v_e(2).start()],
             14: [lambda: hand_e(1), lambda: hand_f(0)], 17: [lambda: hand_c(2), lambda: v_e(3).start()],
             20: [lambda: hand_f(1)], 23: [lambda: hand_c(3)]}

    def w1_pass(p):
        layer_norm(2 * p)
        layer_norm(2 * p + 1)

        @pl.when(p == 0)
        def _():
            fetch1(p, 0)

        def step(t):
            @pl.when(t == 24)
            def _():
                h_done(0)
                h_done(1)
                attention(p)

            def fetch_next():
                @pl.when(t + 1 < NT)
                def _():
                    fetch1(p, t + 1)

                @pl.when((t + 1 == NT) & (p == 0))
                def _():
                    fetch1(1, 0)

                @pl.when((t + 1 == NT) & (p == 1))
                def _():
                    fetch2(0)

            @pl.when(p == 1)
            def _():
                fetch_next()

            w1_tile(p, t)

            @pl.when(p == 0)
            def _():
                fetch_next()

            for at, todo in hands.items():
                @pl.when((p == 1) & (t == at))
                def _(todo=todo):
                    for one in todo:
                        one()

        loop(0, NT, step)
        h_done(0)
        h_done(1)

    loop(0, 2, w1_pass)

    def load(e, i, src):
        return pltpu.make_async_copy(src, sv.at[e, i], vsem.at[e, i])

    def fin_loads(k, n, e):
        at = (part_rows(k), tile(n))
        return [load(e, 0, pa.at[at]), load(e, 1, ry.at[at]), load(e, 2, tok.at[own_out(k), tile(n)])]

    def fin_store(k, n, e):
        return pltpu.make_async_copy(sv.at[e, 3], out.at[own_out(k), tile(n)], vsem.at[e, 3])

    def tail_store(k, e):
        def to(ref):
            return pltpu.make_async_copy(sv.at[e, 3], ref, vsem.at[e, 4])

        @pl.when(k < NK - 1)
        def _():
            to(tail.at[part_rows(k - NL)]).start()

        @pl.when(k == NK - 1)
        def _():
            to(tail2).start()

    def is_last(k, n):
        return (n == NN - 1) & (k == NL - 1)

    def o_rec():
        at = out.at[own_out(NL - 1), LAST]
        return remote(at, rec, x_s, x_r.at[NL - 1, NN - 1], dev_x)

    def is_tail(k, n):
        return (n == NN - 1) & (k >= NL)

    def fin_load(k, n, e):
        @pl.when(k % 2 == 0)
        def _():
            o_y(k // 2, n).wait_recv()

        start_all(fin_loads(k, n, e))

    def fin_do(k, n, e):
        wait_all(fin_loads(k, n, e))
        total = sv[e, 0].astype(F32) + sv[e, 1].astype(F32) + (ob[0, :, tile(n)] + ob[1, :, tile(n)]) + sv[e, 2].astype(F32)
        sv[e, 3] = total.astype(BF16)
        fin_store(k, n, e).start()

        @pl.when(is_tail(k, n))
        def _():
            tail_store(k, e)

    def fin_send(k, n, e):
        fin_store(k, n, e).wait()

        @pl.when(is_tail(k, n))
        def _():
            pltpu.make_async_copy(sv.at[e, 3], tail2, vsem.at[e, 4]).wait()

        @pl.when(is_last(k, n))
        def _():
            o_rec().start()

        @pl.when(jnp.logical_not(is_tail(k, n) | is_last(k, n)))
        def _():
            o_x(k, n).start()

        o_c(k, n).start()

    def hand_out(k, n):
        o_x(k, n).wait_recv()
        o_f(k, n).start()

    STEPS = 2 * NN * NK

    def service(v):
        f = v - 11
        n, i = f // 16, f % 16

        @pl.when((f >= 0) & (i >= 2) & (i < NK + 2))
        def _():
            fin_send(i - 2, n, v % 2)

        @pl.when((f >= 0) & (i < NK))
        def _():
            fin_load(i, n, v % 2)

        @pl.when((f >= 0) & (i >= 1) & (i < NK + 1))
        def _():
            fin_do(i - 1, n, (v + 1) % 2)

        for n, at in enumerate((33, 49)):
            @pl.when((v >= at) & (v < at + NK))
            def _(n=n, at=at):
                hand_out(v - at, n)

    def j_copy(v):
        g, half = (v % 8) // 2, v % 2
        src = jb.at[rows_of(g), pl.ds(pl.multiple_of(half * KH, KH), KH)]
        return pltpu.make_async_copy(src, zj.at[half], jsem.at[half])

    def p_copy(m, g):
        n, slot = m // 2, g % 2
        return n, lambda ref: pltpu.make_async_copy(ptile.at[slot], ref.at[rows_of(g), tile(n)], psem.at[slot])

    def p_start(m, g):
        _, to = p_copy(m, g)

        @pl.when(m % 2 == 0)
        def _():
            to(pb).start()

        @pl.when(m % 2 == 1)
        def _():
            to(pa).start()

    def p_finish(m, g):
        n, to = p_copy(m, g)

        @pl.when(m % 2 == 0)
        def _():
            to(pb).wait()
            o_y(g, n).start()

        @pl.when(m % 2 == 1)
        def _():
            to(pa).wait()

    j_copy(0).start()

    def w2_tile(m):
        for at, todo in enumerate((lambda: hand_e(2), lambda: hand_f(2), lambda: hand_e(3), lambda: hand_f(3))):
            @pl.when(m == at)
            def _(todo=todo):
                todo()

        @pl.when(m + 1 < 2 * NN)
        def _():
            fetch2(m + 1)

        arrive2(m)

        def one(g):
            v = m * 2 * GROUPS + 2 * g
            j_copy(v + 1).start()
            j_copy(v).wait()
            acc[...] = jnp.dot(zj[0], wbuf[w2_slot(m, 0)], preferred_element_type=F32)

            @pl.when(g > 0)
            def _():
                p_finish(m, g - 1)

            service(v)

            @pl.when(v + 2 < STEPS)
            def _():
                j_copy(v + 2).start()

            j_copy(v + 1).wait()
            ptile[g % 2] = (acc[...] + jnp.dot(zj[1], wbuf[w2_slot(m, 1)], preferred_element_type=F32)).astype(BF16)
            p_start(m, g)
            service(v + 1)

        loop(0, GROUPS, one)
        p_finish(m, GROUPS - 1)

    loop(0, 2 * NN, w2_tile)

    loop(STEPS, STEPS + 5, service)
    loop(0, NK, lambda k: hand_out(k, 2))

    for one in small_far:
        one.wait_send()
    remote(toth, toth, t_s, t_s, dev_y).wait_send()
    for kind in range(C + NJ):
        remote(bots[OWN], bots[OWN], w_s.at[kind], w_s.at[kind], dev_y).wait_send()
    for kind in range(NS):
        remote(theirs[OWN], theirs[OWN], d_s.at[kind], d_s.at[kind], dev_y).wait_send()
    for kind in range(NS - 1):
        remote(theirs[OWN], theirs[OWN], e_s.at[kind], e_s.at[kind], dev_y).wait_send()
    remote(pb, pb, y_s, y_s, dev_y).wait_send()
    mine_out = out.at[pl.ds(row0, ROWS)]
    near_out = remote(mine_out, mine_out, o_s.at[0], o_r.at[0], dev_c)
    near_out.wait_send()
    near_out.wait_recv()

    loop(0, NL - 1, lambda k: hand_out(k, NN - 1))
    crossed = ROWS - (NK - NL) * HALF // NN
    handed = out.at[pl.ds(row0, crossed - HALF // NN)]
    sent = out.at[pl.ds(row0, crossed)]
    far_out = remote(handed, handed, o_s.at[1], o_r.at[1], dev_c)
    far_out.wait_send()
    far_out.wait_recv()
    o_rec().wait_recv()
    remote(sent, sent, x_s, x_s, dev_x).wait_send()


def copy_kernel(lo, hi, src, *rest):
    more, (dst, buf, sem) = rest[1:-3], rest[-3:]
    slots = buf.shape[0]
    x = lax.axis_index("mx") // 2

    def moves(i):
        first = (x + i // (2 * NK)) % 2
        rows = pl.ds(pl.multiple_of(first_row(first, (i // NK) % 2) + (i % NK) * HALF, HALF), HALF)
        late = i >= 2 * NK and i % NK >= NL
        cols = pl.ds(0, WID - TN if late else WID)
        k = (i - lo) % slots
        return (pltpu.make_async_copy(src.at[rows, cols], buf.at[k, :, cols], sem.at[0, k]),
                pltpu.make_async_copy(buf.at[k, :, cols], dst.at[rows, cols], sem.at[1, k]))

    def one_more(i, ref):
        c = (lax.axis_index("mx") + i) % 2
        rows = pl.ds(pl.multiple_of(first_row(1 - x, c) + (NL - 1) * HALF, HALF), HALF)
        cols = LAST
        k = (hi - lo + i) % slots
        return (pltpu.make_async_copy(ref, buf.at[k, :, cols], sem.at[0, k]),
                pltpu.make_async_copy(buf.at[k, :, cols], dst.at[rows, cols], sem.at[1, k]))

    every = [moves(i) for i in range(lo, hi)] + [one_more(i, ref) for i, ref in enumerate(more)]
    ahead, count = 12, len(every)
    for i in range(count + ahead):
        if i < count:
            if i >= slots:
                every[i - slots][1].wait()
            every[i][0].start()
        if i >= ahead:
            every[i - ahead][0].wait()
            every[i - ahead][1].start()
    for _, store in every[-min(slots, count):]:
        store.wait()


def tail_kernel(lo, hi, others, base, *rest):
    pieces, (out, sem) = rest[:-2], rest[-2:]
    mi = lax.axis_index("mx")
    moves = []
    for i, (other, piece) in enumerate(zip(others, pieces)):
        at = pl.multiple_of(first_row(1 - mi // 2, (mi + other) % 2) + lo * HALF, HALF)
        moves.append(pltpu.make_async_copy(piece, out.at[pl.ds(at, (hi - lo) * HALF), LAST], sem.at[i]))
    start_all(moves)
    wait_all(moves)


def solution(mesh):
    hbm = pl.BlockSpec(memory_space=pltpu.HBM)

    def dma(*shape):
        return pltpu.SemaphoreType.DMA(shape)

    def local_layer(tokens, ln_scale, w_in, mlp_bias, q_scale, k_scale, w_out, attn_out_bias, mlp_out_bias):
        tok = tokens.reshape(-1, WID)
        vecs = [v.reshape(-1, LANES) for v in (ln_scale, mlp_bias, q_scale, k_scale, attn_out_bias, mlp_out_bias)]
        of = lambda *shape: jax.ShapeDtypeStruct(shape, BF16)
        shapes = [of(*tok.shape), *[of((hi - lo) * HALF, TN) for lo, hi in TAILS], of(HALF, TN), of(ROWS, WID), of(3, WID, NJ * TN), of(4, WID, NJ * TN), of(3, JB, WID), of(4, JB, WID),
                  of(3, NS, ROWS, TN), of(ROWS, NS * JB), of(ROWS, WID), of(ROWS, WID), of(ROWS, WID)]
        flops = 2 * ROWS * (2 * WID * NT * TN + NS * JB * 2 * WID)
        pairs = [(), (NK,), (7,), (7, NJ), (3,), (3, NN), (NS,), (NS, NN), (), (GROUPS, NN), (), (NK, NN), (2,), (2,), (NS,), (NS,)]
        res = pl.pallas_call(
            kernel,
            out_shape=shapes,
            in_specs=[hbm] * 9,
            out_specs=[hbm] * len(shapes),
            scratch_shapes=[
                pltpu.VMEM((2, M, KH), BF16),
                pltpu.VMEM((4, KH, TN), BF16),
                pltpu.VMEM((2, M, TN), BF16),
                pltpu.VMEM((M, TN), F32),
                pltpu.VMEM((2, 3, M, TN), BF16),
                pltpu.VMEM((2, 4, HALF, TN), BF16),
                pltpu.VMEM((2, 2, LN, WID), BF16),
                pltpu.VMEM((2, 1, WID), F32),
                pltpu.VMEM((NS, 1, UNITS // 2), F32),
                pltpu.VMEM((2, 1, DH), F32),
                pltpu.VMEM((2, 1, WID), F32),
                pltpu.VMEM((2 * NS, WID // LANES, LANES), BF16),
                pltpu.VMEM((2, DH // LANES, LANES), BF16),
                dma(2, 2), dma(2, 5), dma(2), dma(2), dma(2, 3), dma(2, 5), dma(2, 2), dma(6),
            ] + [dma(*shape) for shape in pairs],
            compiler_params=pltpu.CompilerParams(collective_id=0, has_side_effects=True, vmem_limit_bytes=63 * 2**20),
            cost_estimate=cost(flops, 2**30),
            name="layer",
        )(tok, w_in, w_out, *vecs)
        base = res[0]
        over_x = [(i, i ^ 2) for i in range(NS)]
        over_core = [(i, i ^ 1) for i in range(NS)]
        far = []
        for own in res[1:3]:
            far.append(lax.ppermute(own, 'mx', over_x))

        def put(lo, hi, *arrays):
            return pl.pallas_call(
                functools.partial(copy_kernel, lo, hi),
                out_shape=of(*tok.shape),
                in_specs=[hbm] * len(arrays),
                out_specs=hbm,
                input_output_aliases={i: 0 for i in range(1, min(2, len(arrays)))},
                scratch_shapes=[pltpu.VMEM((16, HALF, WID), BF16), dma(2, 16)],
                compiler_params=pltpu.CompilerParams(vmem_limit_bytes=40 * 2**20),
                cost_estimate=cost((hi - lo) * 10**9, (hi - lo) * 4 * HALF * WID),
                name="place",
            )(*arrays)

        def put_last(base, lo, hi, others, *pieces):
            return pl.pallas_call(
                functools.partial(tail_kernel, lo, hi, others),
                out_shape=of(*tok.shape),
                in_specs=[hbm] + [pl.BlockSpec(memory_space=pltpu.VMEM)] * len(pieces),
                out_specs=hbm,
                input_output_aliases={0: 0},
                scratch_shapes=[dma(2)],
                compiler_params=pltpu.CompilerParams(vmem_limit_bytes=8 * 2**20),
                cost_estimate=cost(10**9, 8 * pieces[0].size),
                name="place_last",
            )(base, *pieces)

        results, rec = base, res[3]
        rec_near = lax.ppermute(rec, 'mx', over_core)
        base = put(0, SPLIT, results)
        first, base = lax.optimization_barrier((far[0], base))
        first_near = lax.ppermute(first, 'mx', over_core)
        base = put(SPLIT, 4 * NK, results, base, rec, rec_near)
        second, first_near, base = lax.optimization_barrier((far[1], first_near, base))
        second_near = lax.ppermute(second, 'mx', over_core)
        for (lo, hi), pieces in zip(TAILS, ((first, first_near), (second, second_near))):
            base = put_last(base, lo, hi, range(2), *pieces)
        return base.reshape(tokens.shape)

    specs_in = (P('dp', None, 'my'), P('my'), P('my', 'mx'), P('mx'), P(), P(), P('mx', 'my'), P('my'), P('my'))

    return jax.shard_map(local_layer, mesh=mesh, in_specs=specs_in, out_specs=P('dp', None, 'my'), check_vma=False)
```

```python
import functools

import jax
import jax.numpy as jnp
from jax import lax
from jax.experimental import pallas as pl
from jax.experimental.pallas import tpu as pltpu
from jax.sharding import PartitionSpec as P


MESH = pl.DeviceIdType.MESH
F32, BF16 = jnp.float32, jnp.bfloat16

SEQ, DH, WID = 256, 256, 2048
M, GROUPS = 1024, 4
ROWS = M * GROUPS
HALF = M // 2
TN = 512
QKV, UNITS = 1024, 4096
NS = 4
NJ = 7
NT = NS * NJ
NN = WID // TN
JB = 5 * TN
KH = 2 * JB
LANES = 128
LN = 128
EPS = 1e-6
NK = 2 * GROUPS
NL = NK // 2
TAILS = ((NL, NK - 1), (NK - 1, NK))
SPLIT = 4 * NK - 2


def in_col(j, side):
    mlp = (j + 1) // 4
    at = (1 - mlp) * (QKV * j + (QKV // 2) * side) + mlp * (3 * QKV + (UNITS // 2) * side + TN * (j - 3))
    return pl.ds(pl.multiple_of(at, TN), TN)


def out_row(part, side):
    if part == 0:
        return pl.ds(pl.multiple_of((QKV // 2) * side, QKV // 2), TN)
    return pl.ds(pl.multiple_of(QKV + (UNITS // 2) * side, QKV), UNITS // 2)


LAST = pl.ds((NN - 1) * TN, TN)
PART_ROWS = (pl.ds(0, TN), pl.ds(TN, JB - TN))


def first_row(x, c):
    return pl.multiple_of((2 * x + c) * ROWS, ROWS)


def cost(flops, size):
    return pl.CostEstimate(flops=flops, bytes_accessed=size, transcendentals=0)


def tile(n):
    return pl.ds(pl.multiple_of(n * TN, TN), TN)


def rows_of(g):
    return pl.ds(pl.multiple_of(g * M, M), M)


def tile_of(t):
    a, b = (t + 24) // 28, t // 24
    j = (1 - a) * (t // 2) + (a - b) * (t // 4 + 1 - 2 * ((t % 4) // 2)) + b * (t // 2 - 7)
    s = (1 - a) * (t % 2) + (a - b) * (t % 4) + b * (2 + t % 2)
    return j, s


def loop(lo, hi, body):
    def run(i, carry):
        body(i)
        return carry

    lax.fori_loop(lo, hi, run, 0)


def start_all(copies):
    for one in copies:
        one.start()


def wait_all(copies):
    for one in copies:
        one.wait()


def kernel(tok, w_in, w_out, lns, mb, qs, ks, ab, bb,
           out, tail, tail2, rec, toth, w1t, w1b, w2y, w2n, qkv, jb, pa, pb, ry,
           zj, wbuf, ptile, acc, abuf, sv, lbuf, sc, ub, gains, ob, raw, raw2,
           w1sem, w2sem, jsem, psem, asem, vsem, lsem, csem,
           t_s, t_r, w_s, w_r, e_s, e_r, d_s, d_r, y_s, y_r, x_s, x_r, o_s, o_r, m_s, m_r):
    y = lax.axis_index("my")
    mi = lax.axis_index("mx")
    x, c = mi // 2, mi % 2
    dev_y = {"my": 1 - y, "mx": mi}
    dev_x = {"my": y, "mx": 2 * (1 - x) + c}
    dev_c = {"my": y, "mx": 2 * x + 1 - c}
    dev_d = {"my": y, "mx": 2 * (1 - x) + 1 - c}
    row0, row0_x = first_row(x, c), first_row(1 - x, c)

    barrier = pltpu.get_barrier_semaphore()
    for dev in (dev_y, dev_x, dev_c, dev_d):
        pl.semaphore_signal(barrier, inc=1, device_id=dev, device_id_type=MESH)
    pl.semaphore_wait(barrier, 4)

    def remote(src, dst, ss, rs, dev):
        return pltpu.make_async_remote_copy(src_ref=src, dst_ref=dst, send_sem=ss, recv_sem=rs, device_id=dev, device_id_type=MESH)

    def t_dir(k):
        src = tok.at[pl.ds(pl.multiple_of(row0 + k * HALF, HALF), HALF)]
        return remote(src, toth.at[pl.ds(pl.multiple_of(k * HALF, HALF), HALF)], t_s, t_r.at[k], dev_y)

    C, B, D, E, F, G, H = range(7)

    def w_own(kind, j, side, dst, dev):
        return remote(w_in.at[:, in_col(j, side)], dst.at[:, tile(j)], w_s.at[kind], w_r.at[kind, j], dev)

    def w_pass(kind, j, src, dst, dev):
        return remote(src.at[:, tile(j)], dst.at[:, tile(j)], w_s.at[kind], w_r.at[kind, j], dev)

    tops = [None] + [w1t.at[i] for i in range(NS - 1)]
    bots = [w1b.at[i] for i in range(NS)]
    OWN, CORE, FAR, FAR_CORE = range(NS)
    w_c = lambda j: w_own(C, j, 1 - y, bots[OWN], dev_y)
    w_b = lambda j: w_own(B, j, y, tops[CORE], dev_c)
    w_d = lambda j: w_pass(D, j, bots[OWN], bots[CORE], dev_c)
    w_e = lambda j: w_own(E, j, y, tops[FAR], dev_x)
    w_f = lambda j: w_pass(F, j, bots[OWN], bots[FAR], dev_x)
    w_g = lambda j: w_pass(G, j, tops[FAR], tops[FAR_CORE], dev_c)
    w_h = lambda j: w_pass(H, j, bots[FAR], bots[FAR_CORE], dev_c)

    class Two:
        def __init__(self, kind, n, side, dst, dev):
            self.copies = [remote(w_out.at[out_row(p, side), tile(n)], dst.at[rows, tile(n)], e_s.at[kind], e_r.at[kind, n], dev)
                           for p, rows in enumerate(PART_ROWS)]
            self.both = remote(dst.at[:, tile(n)], dst.at[:, tile(n)], e_s.at[kind], e_r.at[kind, n], dev)

        def start(self):
            start_all(self.copies)

        def wait_recv(self):
            self.both.wait_recv()

    def v_pass(kind, n, src, dst, dev):
        return remote(src.at[:, tile(n)], dst.at[:, tile(n)], d_s.at[kind], d_r.at[kind, n], dev)

    mine = [None] + [w2y.at[i] for i in range(NS - 1)]
    theirs = [w2n.at[i] for i in range(NS)]
    v_c = lambda n: Two(C, n, 1 - y, theirs[OWN], dev_y)
    v_b = lambda n: Two(B, n, y, mine[CORE], dev_c)
    v_e = lambda n: Two(D, n, y, mine[FAR], dev_x)
    v_d = lambda n: v_pass(C, n, theirs[OWN], theirs[CORE], dev_c)
    v_f = lambda n: v_pass(B, n, theirs[OWN], theirs[FAR], dev_x)
    v_g = lambda n: v_pass(D, n, mine[FAR], mine[FAR_CORE], dev_c)
    v_h = lambda n: v_pass(E, n, theirs[FAR], theirs[FAR_CORE], dev_c)

    def o_y(g, n):
        return remote(pb.at[rows_of(g), tile(n)], ry.at[rows_of(g), tile(n)], y_s, y_r.at[g, n], dev_y)

    def part_rows(k):
        return pl.ds(pl.multiple_of(k * HALF, HALF), HALF)

    def own_out(k):
        return pl.ds(pl.multiple_of(row0 + k * HALF, HALF), HALF)

    def o_x(k, n):
        at = out.at[own_out(k), tile(n)]
        return remote(at, at, x_s, x_r.at[k, n], dev_x)

    def o_c(k, n):
        at = out.at[own_out(k), tile(n)]
        return remote(at, at, o_s.at[0], o_r.at[0], dev_c)

    def o_f(k, n):
        at = out.at[pl.ds(pl.multiple_of(row0_x + k * HALF, HALF), HALF), tile(n)]
        return remote(at, at, o_s.at[1], o_r.at[1], dev_c)

    rows = WID // LANES
    few = DH // LANES
    my_units = mb.at[pl.ds(pl.multiple_of(y * rows, rows), rows)]
    small_far = [remote(src, raw.at[i], m_s.at[i], m_r.at[i], dev) for i, (src, dev) in enumerate((
        (lns, dev_y), (my_units, dev_c), (my_units, dev_x), (my_units, dev_d)))]
    small = [pltpu.make_async_copy(src, dst, csem.at[i]) for i, (src, dst) in enumerate((
        (lns, raw.at[NS]), (my_units, raw.at[NS + 1]), (ab, raw.at[NS + 2]), (bb, raw.at[NS + 3]), (qs, raw2.at[0]), (ks, raw2.at[1])))]

    def spread(src, dst, count):
        for i in range(count):
            dst[:, i * LANES:(i + 1) * LANES] = src[i:i + 1].astype(F32)

    loop(0, NS, lambda j: w_e(j).start())
    start_all(small_far)
    loop(0, NS, lambda k: t_dir(k).start())
    loop(0, NJ, lambda j: w_c(j).start())
    loop(NS, NK, lambda k: t_dir(k).start())
    loop(0, NN, lambda n: v_c(n).start())
    w_e(NS).start()
    w_e(NS + 1).start()
    loop(0, NJ, lambda j: w_b(j).start())
    loop(0, NN, lambda n: v_b(n).start())
    start_all(small)
    wait_all(small)
    for one in small_far:
        one.wait_recv()
    for i, dst in enumerate((sc.at[1], ub.at[CORE], ub.at[FAR], ub.at[FAR_CORE], sc.at[0], ub.at[OWN], ob.at[0], ob.at[1])):
        spread(raw.at[i], dst, rows)
    for i in range(2):
        spread(raw2.at[i], gains.at[i], few)

    def l_copies(g, i, slot):
        at = pl.multiple_of(g * M + i * LN, LN)
        return (
            pltpu.make_async_copy(tok.at[pl.ds(pl.multiple_of(row0 + at, LN), LN)], lbuf.at[slot, 0], lsem.at[slot, 0]),
            pltpu.make_async_copy(toth.at[pl.ds(at, LN)], lbuf.at[slot, 1], lsem.at[slot, 1]),
        )

    def layer_norm(g):
        steps = M // LN
        t_dir(2 * g).wait_recv()
        start_all(l_copies(g, 0, 0))

        def rows(i):
            slot = i % 2

            @pl.when(i == steps // 2 - 1)
            def _():
                t_dir(2 * g + 1).wait_recv()

            @pl.when(i + 1 < steps)
            def _():
                start_all(l_copies(g, i + 1, 1 - slot))

            wait_all(l_copies(g, i, slot))
            step = 64

            def part(k):
                at = pl.ds(pl.multiple_of(k * step, step), step)
                a, b = lbuf[slot, 0, at].astype(F32), lbuf[slot, 1, at].astype(F32)
                mean = (jnp.sum(a, -1, keepdims=True) + jnp.sum(b, -1, keepdims=True)) * (0.5 / WID)
                a, b = a - mean, b - mean
                var = (jnp.sum(a * a, -1, keepdims=True) + jnp.sum(b * b, -1, keepdims=True)) * (0.5 / WID)
                inv = lax.rsqrt(var + EPS)
                to = pl.ds(pl.multiple_of(i * LN + k * step, step), step)
                zj[g % 2, to, :WID] = (a * inv * sc[0]).astype(BF16)
                zj[g % 2, to, WID:2 * WID] = (b * inv * sc[1]).astype(BF16)

            loop(0, LN // step, part)

        loop(0, steps, rows)

    def w1_copies(slot, top, bottom):
        return (
            pltpu.make_async_copy(top, wbuf.at[slot, :WID], w1sem.at[slot, 0]),
            pltpu.make_async_copy(bottom, wbuf.at[slot, WID:2 * WID], w1sem.at[slot, 1]),
        )

    def fetch1(p, t):
        j, s = tile_of(t)
        slot = t % 2

        @pl.when(p == 0)
        def _():
            @pl.when(s == 0)
            def _():
                w_c(j).wait_recv()
                w_d(j).start()
                w_f(j).start()

                @pl.when(j == 2)
                def _():
                    w_e(NJ - 1).start()

                @pl.when(j == NJ - 1)
                def _():
                    v_e(0).start()
                    v_e(1).start()

            @pl.when(s == 1)
            def _():
                w_b(j).wait_recv()
                w_d(j).wait_recv()

            @pl.when(s == 2)
            def _():
                w_e(j).wait_recv()
                w_g(j).start()
                w_f(j).wait_recv()
                w_h(j).start()

            @pl.when(s == 3)
            def _():
                w_g(j).wait_recv()
                w_h(j).wait_recv()

        @pl.when(s == 0)
        def _():
            start_all(w1_copies(slot, w_in.at[:, in_col(j, y)], w1b.at[0, :, tile(j)]))

        @pl.when(s > 0)
        def _():
            start_all(w1_copies(slot, w1t.at[s - 1, :, tile(j)], w1b.at[s, :, tile(j)]))

    def h_store(slot, dst):
        return pltpu.make_async_copy(ptile.at[slot], dst, psem.at[slot])

    def h_done(slot):
        h_store(slot, pb.at[rows_of(0), tile(0)]).wait()

    def w1_tile(p, t):
        j, s = tile_of(t)
        wait_all(w1_copies(t % 2, w1t.at[0, :, tile(0)], w1b.at[0, :, tile(0)]))

        def one(gl):
            g = 2 * p + gl

            def project():
                h = (jnp.dot(zj[gl, :, :WID], wbuf[t % 2, :WID], preferred_element_type=F32)
                     + jnp.dot(zj[gl, :, WID:2 * WID], wbuf[t % 2, WID:2 * WID], preferred_element_type=F32))
                return h.astype(BF16)

            @pl.when((t > 0) & (t != 24))
            def _():
                h_done(gl)

            @pl.when(j < 2)
            def _():
                h = project().astype(F32)
                gain = gains[j]
                for k in range(2):
                    part = h[:, k * DH:(k + 1) * DH]
                    part = part - jnp.mean(part, -1, keepdims=True)
                    var = jnp.mean(part * part, -1, keepdims=True)
                    ptile[gl, :, k * DH:(k + 1) * DH] = (part * lax.rsqrt(var + EPS) * gain).astype(BF16)

            @pl.when(j == 2)
            def _():
                ptile[gl] = project()

            @pl.when(j > 2)
            def _():
                h = project().astype(F32) + ub[s, :, tile(j - 3)]
                ptile[gl] = (0.5 * h * (1.0 + lax.erf(h * 0.7071067811865476))).astype(BF16)

            @pl.when(j <= 2)
            def _():
                h_store(gl, qkv.at[j, s, rows_of(g)]).start()

            @pl.when(j > 2)
            def _():
                h_store(gl, jb.at[rows_of(g), pl.ds(pl.multiple_of(s * JB + (j - 2) * TN, TN), TN)]).start()

        loop(0, 2, one)

    def a_loads(p, w, slot):
        g, s = 2 * p + w // NS, w % NS
        return [pltpu.make_async_copy(qkv.at[i, s, rows_of(g)], abuf.at[slot, i], asem.at[slot, i]) for i in range(3)]

    def a_store(p, w, slot):
        g, s = 2 * p + w // NS, w % NS
        return h_store(slot, jb.at[rows_of(g), pl.ds(pl.multiple_of(s * JB, TN), TN)])

    def attention(p):
        units = 2 * NS
        start_all(a_loads(p, 0, 0))

        def unit(w):
            slot = w % 2

            @pl.when(w + 1 < units)
            def _():
                start_all(a_loads(p, w + 1, 1 - slot))

            wait_all(a_loads(p, w, slot))

            @pl.when(w >= 2)
            def _():
                a_store(p, w - 2, slot).wait()

            def images(i):
                for ii in range(2):
                    at = pl.ds(pl.multiple_of((2 * i + ii) * SEQ, SEQ), SEQ)
                    for k in range(2):
                        cols = slice(k * DH, (k + 1) * DH)
                        q, kk, v = abuf[slot, 0, at, cols], abuf[slot, 1, at, cols], abuf[slot, 2, at, cols]
                        lg = lax.dot_general(q, kk, (((1,), (1,)), ((), ())), preferred_element_type=F32) * (DH ** -0.5)
                        e = jnp.exp(lg - jnp.max(lg, -1, keepdims=True))
                        prob = (e / jnp.sum(e, -1, keepdims=True)).astype(BF16)
                        ptile[slot, at, cols] = jnp.dot(prob, v, preferred_element_type=F32).astype(BF16)

            loop(0, M // SEQ // 2, images)
            a_store(p, w, slot).start()

        loop(0, units, unit)
        a_store(p, units - 2, 0).wait()
        a_store(p, units - 1, 1).wait()

    def w2_slot(m, half):
        return 2 * ((m + 1) % 2) + half

    def w2_dst(m, s):
        return wbuf.at[w2_slot(m, s // 2), pl.ds((s % 2) * JB, JB)]

    def fetch2(m):
        n = m // 2
        e = m % 2

        @pl.when(e == 0)
        def _():
            v_d(n).wait_recv()
            v_h(n).wait_recv()
            for s in range(NS):
                pltpu.make_async_copy(w2n.at[s, :, tile(n)], w2_dst(m, s), w2sem.at[e, s]).start()

        @pl.when(e == 1)
        def _():
            v_b(n).wait_recv()
            v_g(n).wait_recv()
            for p in range(2):
                to = wbuf.at[w2_slot(m, 0), PART_ROWS[p]]
                pltpu.make_async_copy(w_out.at[out_row(p, y), tile(n)], to, w2sem.at[e, 4 * p]).start()
            for s in range(1, NS):
                pltpu.make_async_copy(w2y.at[s - 1, :, tile(n)], w2_dst(m, s), w2sem.at[e, s]).start()

    def arrive2(m):
        e = m % 2

        @pl.when(e == 0)
        def _():
            for s in range(NS):
                pltpu.make_async_copy(w2n.at[s, :, tile(0)], w2_dst(m, s), w2sem.at[e, s]).wait()

        @pl.when(e == 1)
        def _():
            for p in range(2):
                to = wbuf.at[w2_slot(m, 0), PART_ROWS[p]]
                pltpu.make_async_copy(w2n.at[0, PART_ROWS[p], tile(0)], to, w2sem.at[e, 4 * p]).wait()
            for s in range(1, NS):
                pltpu.make_async_copy(w2n.at[s, :, tile(0)], w2_dst(m, s), w2sem.at[e, s]).wait()

    def hand_c(n):
        v_c(n).wait_recv()
        v_d(n).start()
        v_f(n).start()

    def hand_e(n):
        v_e(n).wait_recv()
        v_g(n).start()

    def hand_f(n):
        v_f(n).wait_recv()
        v_h(n).start()

    hands = {5: [lambda: hand_c(0)], 8: [lambda: hand_e(0)], 11: [lambda: hand_c(1), lambda: v_e(2).start()],
             14: [lambda: hand_e(1), lambda: hand_f(0)], 17: [lambda: hand_c(2), lambda: v_e(3).start()],
             20: [lambda: hand_f(1)], 23: [lambda: hand_c(3)]}

    def w1_pass(p):
        layer_norm(2 * p)
        layer_norm(2 * p + 1)

        @pl.when(p == 0)
        def _():
            fetch1(p, 0)

        def step(t):
            @pl.when(t == 24)
            def _():
                h_done(0)
                h_done(1)
                attention(p)

            def fetch_next():
                @pl.when(t + 1 < NT)
                def _():
                    fetch1(p, t + 1)

                @pl.when((t + 1 == NT) & (p == 0))
                def _():
                    fetch1(1, 0)

                @pl.when((t + 1 == NT) & (p == 1))
                def _():
                    fetch2(0)

            @pl.when(p == 1)
            def _():
                fetch_next()

            w1_tile(p, t)

            @pl.when(p == 0)
            def _():
                fetch_next()

            for at, todo in hands.items():
                @pl.when((p == 1) & (t == at))
                def _(todo=todo):
                    for one in todo:
                        one()

        loop(0, NT, step)
        h_done(0)
        h_done(1)

    loop(0, 2, w1_pass)

    def load(e, i, src):
        return pltpu.make_async_copy(src, sv.at[e, i], vsem.at[e, i])

    def fin_loads(k, n, e):
        at = (part_rows(k), tile(n))
        return [load(e, 0, pa.at[at]), load(e, 1, ry.at[at]), load(e, 2, tok.at[own_out(k), tile(n)])]

    def fin_store(k, n, e):
        return pltpu.make_async_copy(sv.at[e, 3], out.at[own_out(k), tile(n)], vsem.at[e, 3])

    def tail_store(k, e):
        def to(ref):
            return pltpu.make_async_copy(sv.at[e, 3], ref, vsem.at[e, 4])

        @pl.when(k < NK - 1)
        def _():
            to(tail.at[part_rows(k - NL)]).start()

        @pl.when(k == NK - 1)
        def _():
            to(tail2).start()

    def is_last(k, n):
        return (n == NN - 1) & (k == NL - 1)

    def o_rec():
        at = out.at[own_out(NL - 1), LAST]
        return remote(at, rec, x_s, x_r.at[NL - 1, NN - 1], dev_x)

    def is_tail(k, n):
        return (n == NN - 1) & (k >= NL)

    def fin_load(k, n, e):
        @pl.when(k % 2 == 0)
        def _():
            o_y(k // 2, n).wait_recv()

        start_all(fin_loads(k, n, e))

    def fin_do(k, n, e):
        wait_all(fin_loads(k, n, e))
        total = sv[e, 0].astype(F32) + sv[e, 1].astype(F32) + (ob[0, :, tile(n)] + ob[1, :, tile(n)]) + sv[e, 2].astype(F32)
        sv[e, 3] = total.astype(BF16)
        fin_store(k, n, e).start()

        @pl.when(is_tail(k, n))
        def _():
            tail_store(k, e)

    def fin_send(k, n, e):
        fin_store(k, n, e).wait()

        @pl.when(is_tail(k, n))
        def _():
            pltpu.make_async_copy(sv.at[e, 3], tail2, vsem.at[e, 4]).wait()

        @pl.when(is_last(k, n))
        def _():
            o_rec().start()

        @pl.when(jnp.logical_not(is_tail(k, n) | is_last(k, n)))
        def _():
            o_x(k, n).start()

        o_c(k, n).start()

    def hand_out(k, n):
        o_x(k, n).wait_recv()
        o_f(k, n).start()

    STEPS = 2 * NN * NK

    def service(v):
        f = v - 11
        n, i = f // 16, f % 16

        @pl.when((f >= 0) & (i >= 2) & (i < NK + 2))
        def _():
            fin_send(i - 2, n, v % 2)

        @pl.when((f >= 0) & (i < NK))
        def _():
            fin_load(i, n, v % 2)

        @pl.when((f >= 0) & (i >= 1) & (i < NK + 1))
        def _():
            fin_do(i - 1, n, (v + 1) % 2)

        for n, at in enumerate((33, 49)):
            @pl.when((v >= at) & (v < at + NK))
            def _(n=n, at=at):
                hand_out(v - at, n)

    def j_copy(v):
        g, half = (v % 8) // 2, v % 2
        src = jb.at[rows_of(g), pl.ds(pl.multiple_of(half * KH, KH), KH)]
        return pltpu.make_async_copy(src, zj.at[half], jsem.at[half])

    def p_copy(m, g):
        n, slot = m // 2, g % 2
        return n, lambda ref: pltpu.make_async_copy(ptile.at[slot], ref.at[rows_of(g), tile(n)], psem.at[slot])

    def p_start(m, g):
        _, to = p_copy(m, g)

        @pl.when(m % 2 == 0)
        def _():
            to(pb).start()

        @pl.when(m % 2 == 1)
        def _():
            to(pa).start()

    def p_finish(m, g):
        n, to = p_copy(m, g)

        @pl.when(m % 2 == 0)
        def _():
            to(pb).wait()
            o_y(g, n).start()

        @pl.when(m % 2 == 1)
        def _():
            to(pa).wait()

    j_copy(0).start()

    def w2_tile(m):
        for at, todo in enumerate((lambda: hand_e(2), lambda: hand_f(2), lambda: hand_e(3), lambda: hand_f(3))):
            @pl.when(m == at)
            def _(todo=todo):
                todo()

        @pl.when(m + 1 < 2 * NN)
        def _():
            fetch2(m + 1)

        arrive2(m)

        def one(g):
            v = m * 2 * GROUPS + 2 * g
            j_copy(v + 1).start()
            j_copy(v).wait()
            acc[...] = jnp.dot(zj[0], wbuf[w2_slot(m, 0)], preferred_element_type=F32)

            @pl.when(g > 0)
            def _():
                p_finish(m, g - 1)

            service(v)

            @pl.when(v + 2 < STEPS)
            def _():
                j_copy(v + 2).start()

            j_copy(v + 1).wait()
            ptile[g % 2] = (acc[...] + jnp.dot(zj[1], wbuf[w2_slot(m, 1)], preferred_element_type=F32)).astype(BF16)
            p_start(m, g)
            service(v + 1)

        loop(0, GROUPS, one)
        p_finish(m, GROUPS - 1)

    loop(0, 2 * NN, w2_tile)

    loop(STEPS, STEPS + 5, service)
    loop(0, NK, lambda k: hand_out(k, 2))

    for one in small_far:
        one.wait_send()
    remote(toth, toth, t_s, t_s, dev_y).wait_send()
    for kind in range(C + NJ):
        remote(bots[OWN], bots[OWN], w_s.at[kind], w_s.at[kind], dev_y).wait_send()
    for kind in range(NS):
        remote(theirs[OWN], theirs[OWN], d_s.at[kind], d_s.at[kind], dev_y).wait_send()
    for kind in range(NS - 1):
        remote(theirs[OWN], theirs[OWN], e_s.at[kind], e_s.at[kind], dev_y).wait_send()
    remote(pb, pb, y_s, y_s, dev_y).wait_send()
    mine_out = out.at[pl.ds(row0, ROWS)]
    near_out = remote(mine_out, mine_out, o_s.at[0], o_r.at[0], dev_c)
    near_out.wait_send()
    near_out.wait_recv()

    loop(0, NL - 1, lambda k: hand_out(k, NN - 1))
    crossed = ROWS - (NK - NL) * HALF // NN
    handed = out.at[pl.ds(row0, crossed - HALF // NN)]
    sent = out.at[pl.ds(row0, crossed)]
    far_out = remote(handed, handed, o_s.at[1], o_r.at[1], dev_c)
    far_out.wait_send()
    far_out.wait_recv()
    o_rec().wait_recv()
    remote(sent, sent, x_s, x_s, dev_x).wait_send()


def copy_kernel(lo, hi, src, *rest):
    more, (dst, buf, sem) = rest[1:-3], rest[-3:]
    slots = buf.shape[0]
    x = lax.axis_index("mx") // 2

    def moves(i):
        first = (x + i // (2 * NK)) % 2
        rows = pl.ds(pl.multiple_of(first_row(first, (i // NK) % 2) + (i % NK) * HALF, HALF), HALF)
        late = i >= 2 * NK and i % NK >= NL
        cols = pl.ds(0, WID - TN if late else WID)
        k = (i - lo) % slots
        return (pltpu.make_async_copy(src.at[rows, cols], buf.at[k, :, cols], sem.at[0, k]),
                pltpu.make_async_copy(buf.at[k, :, cols], dst.at[rows, cols], sem.at[1, k]))

    def one_more(i, ref):
        c = (lax.axis_index("mx") + i) % 2
        rows = pl.ds(pl.multiple_of(first_row(1 - x, c) + (NL - 1) * HALF, HALF), HALF)
        cols = LAST
        k = (hi - lo + i) % slots
        return (pltpu.make_async_copy(ref, buf.at[k, :, cols], sem.at[0, k]),
                pltpu.make_async_copy(buf.at[k, :, cols], dst.at[rows, cols], sem.at[1, k]))

    every = [moves(i) for i in range(lo, hi)] + [one_more(i, ref) for i, ref in enumerate(more)]
    ahead, count = 6, len(every)
    for i in range(count + ahead):
        if i < count:
            if i >= slots:
                every[i - slots][1].wait()
            every[i][0].start()
        if i >= ahead:
            every[i - ahead][0].wait()
            every[i - ahead][1].start()
    for _, store in every[-min(slots, count):]:
        store.wait()


def tail_kernel(lo, hi, others, base, *rest):
    pieces, (out, sem) = rest[:-2], rest[-2:]
    mi = lax.axis_index("mx")
    moves = []
    for i, (other, piece) in enumerate(zip(others, pieces)):
        at = pl.multiple_of(first_row(1 - mi // 2, (mi + other) % 2) + lo * HALF, HALF)
        moves.append(pltpu.make_async_copy(piece, out.at[pl.ds(at, (hi - lo) * HALF), LAST], sem.at[i]))
    start_all(moves)
    wait_all(moves)


def solution(mesh):
    hbm = pl.BlockSpec(memory_space=pltpu.HBM)

    def dma(*shape):
        return pltpu.SemaphoreType.DMA(shape)

    def local_layer(tokens, ln_scale, w_in, mlp_bias, q_scale, k_scale, w_out, attn_out_bias, mlp_out_bias):
        tok = tokens.reshape(-1, WID)
        vecs = [v.reshape(-1, LANES) for v in (ln_scale, mlp_bias, q_scale, k_scale, attn_out_bias, mlp_out_bias)]
        of = lambda *shape: jax.ShapeDtypeStruct(shape, BF16)
        shapes = [of(*tok.shape), *[of((hi - lo) * HALF, TN) for lo, hi in TAILS], of(HALF, TN), of(ROWS, WID), of(3, WID, NJ * TN), of(4, WID, NJ * TN), of(3, JB, WID), of(4, JB, WID),
                  of(3, NS, ROWS, TN), of(ROWS, NS * JB), of(ROWS, WID), of(ROWS, WID), of(ROWS, WID)]
        flops = 2 * ROWS * (2 * WID * NT * TN + NS * JB * 2 * WID)
        pairs = [(), (NK,), (7,), (7, NJ), (3,), (3, NN), (NS,), (NS, NN), (), (GROUPS, NN), (), (NK, NN), (2,), (2,), (NS,), (NS,)]
        res = pl.pallas_call(
            kernel,
            out_shape=shapes,
            in_specs=[hbm] * 9,
            out_specs=[hbm] * len(shapes),
            scratch_shapes=[
                pltpu.VMEM((2, M, KH), BF16),
                pltpu.VMEM((4, KH, TN), BF16),
                pltpu.VMEM((2, M, TN), BF16),
                pltpu.VMEM((M, TN), F32),
                pltpu.VMEM((2, 3, M, TN), BF16),
                pltpu.VMEM((2, 4, HALF, TN), BF16),
                pltpu.VMEM((2, 2, LN, WID), BF16),
                pltpu.VMEM((2, 1, WID), F32),
                pltpu.VMEM((NS, 1, UNITS // 2), F32),
                pltpu.VMEM((2, 1, DH), F32),
                pltpu.VMEM((2, 1, WID), F32),
                pltpu.VMEM((2 * NS, WID // LANES, LANES), BF16),
                pltpu.VMEM((2, DH // LANES, LANES), BF16),
                dma(2, 2), dma(2, 5), dma(2), dma(2), dma(2, 3), dma(2, 5), dma(2, 2), dma(6),
            ] + [dma(*shape) for shape in pairs],
            compiler_params=pltpu.CompilerParams(collective_id=0, has_side_effects=True, vmem_limit_bytes=63 * 2**20),
            cost_estimate=cost(flops, 2**30),
            name="layer",
        )(tok, w_in, w_out, *vecs)
        base = res[0]
        over_x = [(i, i ^ 2) for i in range(NS)]
        over_core = [(i, i ^ 1) for i in range(NS)]
        far = []
        for own in res[1:3]:
            far.append(lax.ppermute(own, 'mx', over_x))

        def put(lo, hi, *arrays):
            return pl.pallas_call(
                functools.partial(copy_kernel, lo, hi),
                out_shape=of(*tok.shape),
                in_specs=[hbm] * len(arrays),
                out_specs=hbm,
                input_output_aliases={i: 0 for i in range(1, min(2, len(arrays)))},
                scratch_shapes=[pltpu.VMEM((8, HALF, WID), BF16), dma(2, 8)],
                compiler_params=pltpu.CompilerParams(vmem_limit_bytes=20 * 2**20),
                cost_estimate=cost((hi - lo) * 10**9, (hi - lo) * 4 * HALF * WID),
                name="place",
            )(*arrays)

        def put_last(base, lo, hi, others, *pieces):
            return pl.pallas_call(
                functools.partial(tail_kernel, lo, hi, others),
                out_shape=of(*tok.shape),
                in_specs=[hbm] + [pl.BlockSpec(memory_space=pltpu.VMEM)] * len(pieces),
                out_specs=hbm,
                input_output_aliases={0: 0},
                scratch_shapes=[dma(2)],
                compiler_params=pltpu.CompilerParams(vmem_limit_bytes=8 * 2**20),
                cost_estimate=cost(10**9, 8 * pieces[0].size),
                name="place_last",
            )(base, *pieces)

        results, rec = base, res[3]
        rec_near = lax.ppermute(rec, 'mx', over_core)
        base = put(0, SPLIT, results)
        first, base = lax.optimization_barrier((far[0], base))
        first_near = lax.ppermute(first, 'mx', over_core)
        base = put(SPLIT, 4 * NK, results, base, rec, rec_near)
        second, first_near, base = lax.optimization_barrier((far[1], first_near, base))
        second_near = lax.ppermute(second, 'mx', over_core)
        for (lo, hi), pieces in zip(TAILS, ((first, first_near), (second, second_near))):
            base = put_last(base, lo, hi, range(2), *pieces)
        return base.reshape(tokens.shape)

    specs_in = (P('dp', None, 'my'), P('my'), P('my', 'mx'), P('mx'), P(), P(), P('mx', 'my'), P('my'), P('my'))

    return jax.shard_map(local_layer, mesh=mesh, in_specs=specs_in, out_specs=P('dp', None, 'my'), check_vma=False)
```
